128 devices in a mesh: dp: 32 (over x, y, core), mp: 4 (over z).
Axes of the slice: x: 4, y: 4, z: 4, core: 2. Of those that a mesh axis runs over, the one named last changes fastest.
Arguments:
- slab_values: bfloat16 [128, 128, 2048], P(('dp', 'mp')), may hold values from -6 to 6
- row_ids: int32 [128, 128, 32], P(('dp', 'mp')), may hold values from 0 to 4095, as said below
- peer_counts: int32 [128, 128], P(('dp', 'mp')), may hold values from 1 to 32, as said below
- lookup_slots: int32 [32768, 16], P(('dp', 'mp')), may hold values from 0 to 4095, as said below
- labels: int32 [32768], P('dp'), may hold values 0 or 1
- sample_weight: float32 [32768], P('dp'), may hold values from 0.3 to 9
- weight_in: bfloat16 [1024, 8192], P(None, 'mp'), may hold values from -0.1875 to 0.1875
- bias_in: float32 [8192], P('mp'), may hold values from -3 to 3
- weight_out: bfloat16 [8192], P('mp'), may hold values from -0.0625 to 0.0625
- dense_accum: float32 [1024, 8192], P('dp', 'mp'), may hold values from 1e-08 to 1e-06
- table_rows: float32 [524288, 64], P(('dp', 'mp')), may hold values from -0.12 to 0.12
- table_accum: float32 [524288], P(('dp', 'mp')), may hold values from 1e-12 to 1e-05
Outputs:
- weight_new: bfloat16 [1024, 8192], P(None, 'mp')
- accum_new: float32 [1024, 8192], P('dp', 'mp')
- table_new: float32 [524288, 64], P(('dp', 'mp'))
- table_accum_new: float32 [524288], P(('dp', 'mp'))
The draws below stay inside these ranges and needn't reach their ends.
Inputs may be any that keep to these rules, and one draw needn't show every extreme that they name: `row_ids`: the first peer_counts entries of each device's list for an owner are distinct rows of that owner's shard. `peer_counts`: some owner has 32 touched rows on every device, and some device has 32 touched rows of every owner. `lookup_slots`: below the sum of that device's peer_counts; every device has a lookup of its last touched row.
All inputs are finite; a program needn't handle non-finite values. No bound on the sum of `labels` on one device may be relied on, other than what follows from the above.
Results may differ from the reference program's by a relative error of at most 0.0034.
Values may be sent and summed in bfloat16 or wider, within the bound.
No kernel may reach another device: no remote copies, remote signals or barrier semaphores. Data moves between devices by JAX's collectives and lax.ppermute only.
A program may use at most 128 MiB of HBM per device.

```python
import math
import jax
import jax.numpy as jnp
from jax import lax

D_EMB = 64
NF = 16
H = 8192
B_DEV = 256
CAP = 32
ROWS_OWN = 4096
K = 1024
PEERS = 128
SAMPLES = 32768
TABLE_ROWS = 524288
N_DP = 32
N_MP = 4


def count_table(key):
    base = jax.random.fold_in(key, 7)
    counts = jax.random.randint(jax.random.fold_in(base, 1), (PEERS, PEERS), max(1, CAP // 4), CAP + 1)
    hot_owner = jax.random.randint(jax.random.fold_in(base, 2), (), 0, PEERS)
    full_device = jax.random.randint(jax.random.fold_in(base, 3), (), 0, PEERS)
    column = jnp.arange(PEERS)[None, :]
    row_number = jnp.arange(PEERS)[:, None]
    counts = jnp.where(column == hot_owner, CAP, counts)
    counts = jnp.where(row_number == full_device, CAP, counts)
    return counts.astype(jnp.int32)


def draw_peer_counts(key, part):
    return count_table(key)


def draw_lookup_slots(key, part):
    counts = count_table(key)
    live = jnp.sum(counts, axis=1)
    raw_draw = jax.random.randint(jax.random.fold_in(key, 11), (SAMPLES, NF), 0, 2 ** 30)
    device = jnp.arange(SAMPLES) // B_DEV
    within = jnp.arange(SAMPLES) % B_DEV
    drawn = raw_draw % live[device][:, None]
    chosen_sample = jax.random.randint(jax.random.fold_in(key, 19), (PEERS,), 0, B_DEV)
    chosen_feature = jax.random.randint(jax.random.fold_in(key, 23), (PEERS,), 0, NF)
    marked = (within == chosen_sample[device])[:, None] & (jnp.arange(NF)[None, :] == chosen_feature[device][:, None])
    return jnp.where(marked, live[device][:, None] - 1, drawn).astype(jnp.int32)


def draw_row_ids(key, part):
    stride = ROWS_OWN // CAP
    offsets = jax.random.randint(jax.random.fold_in(key, 13), (PEERS, PEERS, CAP), 0, stride)
    return (jnp.arange(CAP)[None, None, :] * stride + offsets).astype(jnp.int32)


def draw_sample_weight(key, part):
    position = jnp.arange(SAMPLES).astype(jnp.float32) / SAMPLES
    rising = 1.0 + 2.0 * position
    level = jax.random.uniform(jax.random.fold_in(key, 17), (SAMPLES,), jnp.float32, 0.5, 1.5)
    return (rising * level).astype(jnp.float32)


def with_ends(values, own_key, low, largest):
    spot = [jax.random.randint(jax.random.fold_in(own_key, axis), (), 0, length) for axis, length in enumerate(values.shape)]
    longest = values.shape.index(max(values.shape))
    beside = spot[:longest] + [(spot[longest] + 1) % values.shape[longest]] + spot[longest + 1:]
    return values.at[tuple(spot)].set(low).at[tuple(beside)].set(largest)


def shard_levels(key, dims, split, smallest, high):
    level = 1.0
    for dim, blocks in split:
        steps = jax.random.uniform(jax.random.fold_in(jax.random.fold_in(key, 6), dim), (blocks,), jnp.float32, smallest / len(split), high / len(split))
        level = level * jnp.repeat(jnp.exp(steps), dims[dim] // blocks).reshape((-1,) + (1,) * (len(dims) - 1 - dim))
    return level


def gaussian(key, extent, deviation, reach, split=(), kind=jnp.bfloat16):
    loudness = shard_levels(key, extent, split, -0.22, 0.18) if split else 1.0
    result = jax.random.normal(key, extent, jnp.float32) * deviation * loudness
    return jnp.minimum(jnp.maximum(result, -reach), reach).astype(kind)


def setup_inputs(seed: int = 0) -> dict:
    seeds = jax.random.split(jax.random.key(seed), 13)
    return {
        "slab_values": gaussian(seeds[0], (PEERS, PEERS, CAP * D_EMB), 1.0, 6.0, ((0, 128),)),
        "row_ids": draw_row_ids(jax.random.fold_in(seeds[12], 71), 0),
        "peer_counts": draw_peer_counts(jax.random.fold_in(seeds[12], 71), 0),
        "lookup_slots": draw_lookup_slots(jax.random.fold_in(seeds[12], 71), 0),
        "labels": with_ends((jax.random.randint(seeds[4], (SAMPLES,), 0, 4) < 1).astype(jnp.int32), jax.random.fold_in(seeds[4], 1), 0, 1),
        "sample_weight": draw_sample_weight(jax.random.fold_in(seeds[12], 71), 0),
        "weight_in": gaussian(seeds[6], (K, H), K ** -0.5, 0.1875, ((1, 4),)),
        "bias_in": gaussian(seeds[7], (H,), 0.5, 3.0, ((0, 4),), jnp.float32),
        "weight_out": gaussian(seeds[8], (H,), H ** -0.5, 0.0625, ((0, 4),)),
        "dense_accum": jnp.clip(jnp.exp(math.log(9.999999974752427e-07) - 4.6051702 * jax.random.uniform(seeds[9], (K, H), jnp.float32) ** shard_levels(seeds[9], (K, H), ((0, 32), (1, 4)), -0.2, 0.2)), 9.99999993922529e-09, 9.999999974752427e-07),
        "table_rows": gaussian(seeds[10], (TABLE_ROWS, D_EMB), 0.02, 0.12, ((0, 128),), jnp.float32),
        "table_accum": jnp.clip(jnp.exp(math.log(9.999999747378752e-06) - 16.118096 * jax.random.uniform(seeds[11], (TABLE_ROWS,), jnp.float32) ** shard_levels(seeds[11], (TABLE_ROWS,), ((0, 128),), -0.2, 0.2)), 9.999999960041972e-13, 9.999999747378752e-06),
    }


clip_norm = 1.0
dense_rate = 0.02
table_rate = 0.5
adagrad_eps = 1e-10

def slot_index(compact, counts, capacity):
    slot_ends = jnp.cumsum(counts)
    owner_index = lax.optimization_barrier(jnp.sum((compact[..., None] >= slot_ends).astype(jnp.int32), axis=-1))
    slot_starts = slot_ends - counts
    owner_match = owner_index[..., None] == jnp.arange(counts.shape[0], dtype=jnp.int32)
    owner_begin = lax.optimization_barrier(jnp.sum(jnp.where(owner_match, slot_starts, 0), axis=-1))
    return (owner_index * capacity + compact - owner_begin).astype(jnp.int32)

def reference(slab_values, row_ids, peer_counts, lookup_slots, labels, sample_weight, weight_in, bias_in, weight_out, dense_accum, table_rows, table_accum):
    group_rows = N_MP * B_DEV
    slabs = slab_values.reshape(N_DP, N_MP, PEERS * CAP, D_EMB)
    counts = peer_counts.reshape(N_DP, N_MP, PEERS)
    slots = lookup_slots.reshape(N_DP, N_MP, B_DEV, NF)
    targets = labels.astype(jnp.float32).reshape(N_DP, group_rows)
    weights = sample_weight.reshape(N_DP, group_rows)

    def group_step(carry, inputs):
        grad_in, grad_bias, grad_out = carry
        slab, count, slot, target, weight = inputs

        def pool(one_slab, one_count, one_slot):
            index = slot_index(one_slot, one_count, CAP)
            return (one_slab[index].reshape(B_DEV, K), index)
        pooled, index = jax.vmap(pool)(slab, count, slot)
        pooled = pooled.reshape(group_rows, K)
        act = jnp.dot(pooled, weight_in, preferred_element_type=jnp.float32) + bias_in
        hidden = jax.nn.silu(act).astype(jnp.bfloat16)
        logit = jnp.dot(hidden, weight_out, preferred_element_type=jnp.float32)
        dlogit = weight * (jax.nn.sigmoid(logit) - target)
        sigma = jax.nn.sigmoid(act)
        dact = (dlogit[:, None] * weight_out.astype(jnp.float32)[None, :] * sigma * (1.0 + act * (1.0 - sigma))).astype(jnp.bfloat16)
        grad_in = grad_in + lax.dot_general(pooled, dact, (((0,), (0,)), ((), ())), preferred_element_type=jnp.float32)
        grad_bias = grad_bias + lax.optimization_barrier(jnp.sum(dact.astype(jnp.float32), axis=0))
        grad_out = grad_out + jnp.dot(dlogit, hidden.astype(jnp.float32), precision=lax.Precision.HIGHEST)
        dpooled = lax.dot_general(dact, weight_in, (((1,), (1,)), ((), ())), preferred_element_type=jnp.float32)
        pieces = dpooled.reshape(N_MP, B_DEV * NF, D_EMB)

        def gather_slots(piece, one_index):
            return jax.ops.segment_sum(piece, one_index.reshape(-1), num_segments=PEERS * CAP)
        slot_grad = jax.vmap(gather_slots)(pieces, index)
        return ((grad_in, grad_bias, grad_out), slot_grad)
    start = (jnp.zeros((K, H), jnp.float32), jnp.zeros((H,), jnp.float32), jnp.zeros((H,), jnp.float32))
    (grad_in, grad_bias, grad_out), slot_grad = lax.scan(group_step, start, (slabs, counts, slots, targets, weights))
    slot_grad = slot_grad.reshape(PEERS, PEERS * CAP, D_EMB)
    total = jnp.sum(grad_in * grad_in) + jnp.sum(grad_bias * grad_bias) + jnp.sum(grad_out * grad_out) + jnp.sum(slot_grad * slot_grad)
    scale = clip_norm / jnp.maximum(jnp.sqrt(total), clip_norm)
    clipped = scale * grad_in
    accum_new = dense_accum + clipped * clipped
    weight_new = (weight_in.astype(jnp.float32) - dense_rate * clipped / (jnp.sqrt(accum_new) + adagrad_eps)).astype(jnp.bfloat16)
    owners = jnp.arange(PEERS, dtype=jnp.int32)[None, :, None]
    global_rows = (owners * ROWS_OWN + row_ids).reshape(-1)
    received = scale * jax.ops.segment_sum(slot_grad.reshape(-1, D_EMB), global_rows, num_segments=TABLE_ROWS)
    table_accum_new = table_accum + lax.optimization_barrier(jnp.mean(received * received, axis=1))
    table_new = table_rows - table_rate * received / (jnp.sqrt(table_accum_new)[:, None] + adagrad_eps)
    return (weight_new, accum_new, table_new, table_accum_new)
```

```python
import functools

import jax
import jax.numpy as jnp
from jax import lax
from jax.experimental import pallas as pl
from jax.experimental.pallas import tpu as pltpu
from jax.sharding import Mesh
from jax.sharding import PartitionSpec as P

DP = ("dp_0", "dp_1", "dp_2")
DP_MP = ("dp_0", "dp_1", "dp_2", "mp")

clip_norm = 1.0
dense_rate = 0.02
table_rate = 0.5
adagrad_eps = 1e-10

F32 = jnp.float32
BF16 = jnp.bfloat16
VM = pl.BlockSpec(memory_space=pltpu.VMEM)


def iota(shape, dim):
    return lax.broadcasted_iota(jnp.int32, shape, dim)


def dot_f32(a, b, dims=(((1,), (0,)), ((), ()))):
    return lax.dot_general(a, b, dims, preferred_element_type=F32)


def gather_kernel(counts_ref, lookups_ref, slab_ref, out_ref):
    owners = counts_ref.shape[1]
    features, batch = lookups_ref.shape
    row_bytes = slab_ref.shape[1] // 2
    counts = counts_ref[...].astype(F32)
    spread = jnp.broadcast_to(counts, (owners, owners)).T
    before = iota((owners, owners), 0) <= iota((owners, owners), 1)
    ends = jnp.sum(jnp.where(before, spread, 0.0), axis=0, keepdims=True)
    starts = ends - counts
    lookups = lookups_ref[...].astype(F32).T
    halves = jnp.concatenate([slab_ref[:, :row_bytes], slab_ref[:, row_bytes:]], axis=0)
    low_lane = iota((batch, 128), 1) < 64
    for pair in range(features // 2):
        both = []
        for parity in range(2):
            f = 2 * pair + parity
            q = lookups[:, f : f + 1]
            match = (q >= starts) & (q < ends)
            begin = jnp.sum(jnp.where(match, starts, 0.0), axis=1, keepdims=True)
            slot = q - begin
            upper = slot >= 16.0
            chosen = jnp.where(match, 1.0, 0.0)
            hot = jnp.concatenate(
                [jnp.where(upper, 0.0, chosen), jnp.where(upper, chosen, 0.0)], axis=1
            ).astype(BF16)
            rows = dot_f32(hot, halves)
            inner = jnp.where(upper, slot - 16.0, slot)
            block = jnp.floor(inner * 0.5)
            odd = inner - 2.0 * block
            block = jnp.broadcast_to(block, (batch, 128))
            found = rows[:, :128]
            for k in range(1, 8):
                found = jnp.where(block == float(k), rows[:, 128 * k : 128 * (k + 1)], found)
            swap = jnp.broadcast_to(odd, (batch, 128)) != float(parity)
            both.append(jnp.where(swap, pltpu.roll(found, 64, 1), found))
        out_ref[:, 128 * pair : 128 * (pair + 1)] = jnp.where(low_lane, both[0], both[1]).astype(BF16)


def gather_rows(counts, lookups_t, slab):
    features, batch = lookups_t.shape
    return pl.pallas_call(
        gather_kernel,
        out_shape=jax.ShapeDtypeStruct((batch, features * 64), BF16),
        in_specs=[VM, VM, VM],
        out_specs=VM,
        name="gather_rows",
        cost_estimate=pl.CostEstimate(flops=6 * 10**9, transcendentals=0, bytes_accessed=2 * 10**6),
    )(counts, lookups_t, slab)


def slot_kernel(counts_ref, lookups_ref, ids_ref, own_ref, a_ref, b_ref, c_ref, dense_ref, out_ref, acc_ref):
    owners = counts_ref.shape[1]
    features, batch = lookups_ref.shape
    width = out_ref.shape[1] - 128
    half_width = width // 2
    counts = counts_ref[...].astype(F32)
    lower = iota((owners, owners), 1) <= iota((owners, owners), 0)
    spread = jnp.broadcast_to(counts, (owners, owners))
    ends = jnp.sum(jnp.where(lower, spread, 0.0), axis=1, keepdims=True)
    starts = ends - jnp.sum(
        jnp.where(iota((owners, owners), 1) == iota((owners, owners), 0), spread, 0.0), axis=1, keepdims=True
    )
    hots, inners = [], []
    for f in range(features):
        q = lookups_ref[f : f + 1, :].astype(F32)
        match = (q >= starts) & (q < ends)
        begin = jnp.sum(jnp.where(match, starts, 0.0), axis=0, keepdims=True)
        slot = q - begin
        upper = slot >= 16.0
        chosen = jnp.where(match, 1.0, 0.0)
        hots.append(
            jnp.concatenate([jnp.where(upper, 0.0, chosen), jnp.where(upper, chosen, 0.0)], axis=0).astype(BF16)
        )
        inners.append(jnp.where(upper, slot - 16.0, slot))
    inner = jnp.concatenate(inners, axis=0).T
    lane = iota((batch, 128), 1)
    low_lane = lane < 64
    offset = jnp.where(low_lane, 0.0, 1.0)
    for pair in range(features // 2):
        cols = slice(128 * pair, 128 * (pair + 1))
        total = own_ref[:, cols] + a_ref[:, cols].astype(F32) + b_ref[:, cols].astype(F32) + c_ref[:, cols].astype(F32)
        turned = pltpu.roll(total, 64, 1)
        for parity in range(2):
            f = 2 * pair + parity
            rows = jnp.where(low_lane, total, turned) if parity == 0 else jnp.where(low_lane, turned, total)
            target = jnp.broadcast_to(inner[:, f : f + 1], (batch, 128)) - offset
            high = rows.astype(BF16).astype(F32)
            low = rows - high
            spread_high, spread_low = [], []
            for k in range(8):
                mask = target == float(2 * k)
                spread_high.append(jnp.where(mask, high, 0.0).astype(BF16))
                spread_low.append(jnp.where(mask, low, 0.0).astype(BF16))
            values = jnp.concatenate(
                [jnp.concatenate(spread_high, axis=1), jnp.concatenate(spread_low, axis=1)], axis=0
            )
            hot = jnp.concatenate([hots[f], hots[f]], axis=1)
            part = dot_f32(hot, values)
            if f == 0:
                acc_ref[...] = part
            else:
                acc_ref[...] = acc_ref[...] + part
    acc = acc_ref[...]
    out_ref[:, :half_width] = acc[:owners].astype(BF16)
    out_ref[:, half_width:width] = acc[owners:].astype(BF16)
    square = jnp.sum(jnp.sum(acc * acc, axis=1, keepdims=True), axis=0, keepdims=True)
    square = square + dense_ref[0:1, 0:1]
    top = square.astype(BF16).astype(F32)
    mid = (square - top).astype(BF16).astype(F32)
    end = square - top - mid
    ids = ids_ref[...]
    block = ids >> 8
    inside = ids & 255
    tail_lane = iota((owners, 128 - 2 * ids.shape[1]), 1)
    tail = jnp.where(tail_lane == 0, top, jnp.where(tail_lane == 1, mid, jnp.where(tail_lane == 2, end, 0.0)))
    out_ref[:, width:] = jnp.concatenate([block.astype(F32), inside.astype(F32), tail], axis=1).astype(BF16)


def slot_sums(counts, lookups_t, ids, own, pieces, dense_square):
    owners, capacity = ids.shape
    return pl.pallas_call(
        slot_kernel,
        out_shape=jax.ShapeDtypeStruct((owners, capacity * 64 + 128), BF16),
        in_specs=[VM] * 8,
        out_specs=VM,
        scratch_shapes=[pltpu.VMEM((2 * owners, capacity * 32), F32)],
        name="slot_sums",
        cost_estimate=pl.CostEstimate(flops=8 * 10**9, transcendentals=0, bytes_accessed=3 * 10**6),
    )(counts, lookups_t, ids, own, *pieces, dense_square)


def table_kernel(rate, eps, clip, arrived_ref, table_ref, accum_ref, table_out, accum_out, scale_out, acc_ref):
    sources = arrived_ref.shape[0]
    width = arrived_ref.shape[1] - 128
    capacity = width // 64
    rows = table_ref.shape[1]
    blocks = rows // 256
    info = arrived_ref[:, width:].astype(F32).T
    squares = info[2 * capacity : 2 * capacity + 8, :]
    squares = jnp.sum(squares[0:3, :], axis=0, keepdims=True)
    total = jnp.sum(squares, axis=1, keepdims=True)
    scale = clip / jnp.maximum(jnp.sqrt(total), clip)
    scale_out[...] = jnp.broadcast_to(scale, scale_out.shape)
    inside_at = iota((256, sources), 0).astype(F32)
    for pair in range(capacity // 2):
        turned = arrived_ref[:, 128 * pair : 128 * (pair + 1)].astype(F32).T
        spread, hots = [], []
        for parity in range(2):
            c = 2 * pair + parity
            piece = turned[64 * parity : 64 * (parity + 1), :]
            block = info[c : c + 1, :]
            inside = info[capacity + c : capacity + c + 1, :]
            hots.append(jnp.where(inside_at == inside, 1.0, 0.0).astype(BF16))
            spread.append(
                jnp.concatenate([jnp.where(block == float(k), piece, 0.0).astype(BF16) for k in range(blocks)], axis=0)
            )
        part = dot_f32(
            jnp.concatenate(spread, axis=1), jnp.concatenate(hots, axis=1), (((1,), (1,)), ((), ()))
        )
        if pair == 0:
            acc_ref[...] = part
        else:
            acc_ref[...] = acc_ref[...] + part
    for k in range(blocks):
        received = scale * acc_ref[64 * k : 64 * (k + 1), :]
        cols = slice(256 * k, 256 * (k + 1))
        accum = accum_ref[:, cols] + jnp.sum(received * received, axis=0, keepdims=True) * (1.0 / 64.0)
        accum_out[:, cols] = accum
        table_out[:, cols] = table_ref[:, cols] - rate * received / (jnp.sqrt(accum) + eps)


def table_update(arrived, table_t, accum, rate, eps, clip):
    width, rows = table_t.shape
    return pl.pallas_call(
        functools.partial(table_kernel, rate, eps, clip),
        out_shape=(
            jax.ShapeDtypeStruct((width, rows), F32),
            jax.ShapeDtypeStruct((1, rows), F32),
            jax.ShapeDtypeStruct((8, 128), F32),
        ),
        in_specs=[VM] * 3,
        out_specs=(VM, VM, VM),
        scratch_shapes=[pltpu.VMEM((rows // 4, 256), F32)],
        name="table_update",
        cost_estimate=pl.CostEstimate(flops=6 * 10**9, transcendentals=0, bytes_accessed=3 * 10**6),
    )(arrived, table_t, accum)


def call(kernel, outs, name, flops, args, scratch=()):
    shapes = tuple(jax.ShapeDtypeStruct(s, t) for s, t in outs)
    return pl.pallas_call(
        kernel,
        out_shape=shapes,
        in_specs=[VM] * len(args),
        out_specs=tuple(VM for _ in shapes),
        scratch_shapes=list(scratch),
        name=name,
        cost_estimate=pl.CostEstimate(flops=flops, transcendentals=0, bytes_accessed=2 * 10**6),
    )(*args)


SHIFTS = (1, 3, 2)


def spot(axis, shift):
    return lax.rem(lax.axis_index(axis) + shift, 4)


def forward_kernel(chunks, *refs):
    ins, (w_ref, bias_ref, out_w_ref) = refs[:chunks], refs[chunks : chunks + 3]
    slope_refs = refs[chunks + 3 : 2 * chunks + 3]
    hidden_ref, logit_ref, turned_ref = refs[2 * chunks + 3 :]
    rows = ins[0].shape[0]
    width = w_ref.shape[1]
    for k in range(chunks):
        turned_ref[:, rows * k : rows * (k + 1)] = ins[k][...].T
    for n in range(width // 256):
        cols = slice(256 * n, 256 * (n + 1))
        w = w_ref[:, cols]
        out_w = out_w_ref[:, cols].astype(F32)
        for k in range(chunks):
            act = dot_f32(ins[k][...], w) + bias_ref[:, cols]
            sigma = 1.0 / (1.0 + jnp.exp(-act))
            hidden_ref[rows * k : rows * (k + 1), cols] = (act * sigma).astype(BF16)
            slope_refs[k][:, cols] = out_w * sigma * (1.0 + act * (1.0 - sigma))
    out_w = jnp.broadcast_to(out_w_ref[...], (16, width))
    for k in range(chunks):
        part = dot_f32(out_w, hidden_ref[rows * k : rows * (k + 1), :], (((1,), (1,)), ((), ())))
        logit_ref[k : k + 1, :] = part[0:1, :]


def forward(chunks, w, bias, out_w):
    rows, depth = chunks[0].shape
    width = w.shape[1]
    n = len(chunks)
    outs = [((rows, width), F32)] * n + [((n * rows, width), BF16), ((n, rows), F32), ((depth, n * rows), BF16)]
    res = call(
        functools.partial(forward_kernel, n), outs, f"forward_{n}", n * 2 * 10**9, (*chunks, w, bias, out_w)
    )
    return list(res[:n]), res[n], res[n + 1], res[n + 2]


ORDER = (0, 3, 1, 2)
PARTNERS = ((0, 1, 2, 3), (2, 0, 3, 1), (1, 3, 0, 2), (3, 2, 1, 0))


def slope_kernel(*refs):
    slopes, hiddens = refs[0:4], refs[4:7]
    own_ref, prev_ref, next_ref, far_ref, labels_ref, weight_ref = refs[7:13]
    dact_ref, other_ref, sums_mine_ref, sums_other_ref, sums_ref = refs[13:]
    rows, width = slopes[0].shape
    half = width // 2
    core = lax.axis_index("dp_2")
    dlogits = []
    for k in range(4):
        at = spot("mp", ORDER[k])
        logit = (own_ref[k : k + 1, :] + far_ref[PARTNERS[3][k] : PARTNERS[3][k] + 1, :]) + (
            prev_ref[PARTNERS[1][k] : PARTNERS[1][k] + 1, :] + next_ref[PARTNERS[2][k] : PARTNERS[2][k] + 1, :]
        )
        label = labels_ref[pl.ds(at, 1), :].astype(F32)
        dlogits.append(weight_ref[pl.ds(at, 1), :] * (1.0 / (1.0 + jnp.exp(-logit)) - label))
    rows_form = jnp.concatenate(dlogits + [jnp.zeros((4, rows), F32)], axis=0)
    cols_form = rows_form.T
    for k in range(4):
        col = cols_form[:, k : k + 1]
        dact_ref[rows * k : rows * (k + 1), :] = (slopes[k][...] * col).astype(BF16)
    other_ref[...] = dact_ref[:, pl.ds(pl.multiple_of((1 - core) * half, half), half)]
    ones = jnp.ones((16, rows), BF16)
    bias_sum = jnp.zeros((16, width), F32)
    out_sum = jnp.zeros((16, width), F32)
    spans = ((0, 0), (1, 0), (1, rows), (2, 0))
    for k in range(4):
        bias_sum = bias_sum + dot_f32(ones, dact_ref[rows * k : rows * (k + 1), :])
        d = dlogits[k]
        top = d.astype(BF16)
        rest = (d - top.astype(F32)).astype(BF16)
        pick = iota((16, rows), 0)
        left = jnp.where(pick == 0, top.astype(F32), jnp.where(pick == 1, rest.astype(F32), 0.0)).astype(BF16)
        which, start = spans[k]
        out_sum = out_sum + dot_f32(left, hiddens[which][start : start + rows, :])
    pick = iota((16, width), 0)
    total = jnp.sum(out_sum, axis=0, keepdims=True)
    sums_ref[...] = jnp.where(pick == 0, bias_sum, jnp.where(pick == 1, total, 0.0))
    sums_mine_ref[...] = sums_ref[:, pl.ds(pl.multiple_of(core * half, half), half)]
    sums_other_ref[...] = sums_ref[:, pl.ds(pl.multiple_of((1 - core) * half, half), half)]


def grad_kernel(second, *refs):
    turned, (dact_ref, far_dact_ref, sums_a_ref, sums_b_ref) = refs[0:6], refs[6:10]
    outs, own_ref, acc_ref = refs[10:13], refs[13], refs[14]
    depth = turned[0].shape[0]
    half = far_dact_ref.shape[1]
    quarter = half // 2
    core = lax.axis_index("dp_2")
    spans = ((0, 256), (256, 512), (768, 256))
    start = pl.multiple_of(core * half + second * quarter, quarter)
    local = dact_ref[:, pl.ds(start, quarter)]
    remote = far_dact_ref[:, second * quarter : (second + 1) * quarter]
    extra = sums_a_ref[:, second * quarter : (second + 1) * quarter] + sums_b_ref[:, second * quarter : (second + 1) * quarter]

    def block(row):
        part = None
        for i, (s, n) in enumerate(spans):
            for source, d in ((turned[i], local), (turned[i + 3], remote)):
                p = dot_f32(source[pl.ds(row, 256), :], d[s : s + n, :])
                part = p if part is None else part + p
        return part

    if not second:
        for k, shift in enumerate(SHIFTS):
            outs[k][0:256, :] = block(pl.multiple_of(spot("dp_0", shift) * 256, 256)).astype(BF16)
        own_ref[0:256, :] = block(pl.multiple_of(spot("dp_0", 0) * 256, 256))
    else:
        for x in range(4):
            acc_ref[256 * x : 256 * (x + 1), :] = block(256 * x)
        for x in range(4):
            for k, shift in enumerate(SHIFTS):
                at = pl.multiple_of(spot("dp_1", shift) * 64 + 256 * x, 64)
                outs[k][64 * x : 64 * (x + 1), :] = acc_ref[pl.ds(at, 64), :].astype(BF16)
            at = pl.multiple_of(spot("dp_1", 0) * 64 + 256 * x, 64)
            own_ref[64 * x : 64 * (x + 1), :] = acc_ref[pl.ds(at, 64), :]
    for k in range(3):
        outs[k][256:272, :] = extra.astype(BF16)
    own_ref[256:272, :] = extra


def middle_kernel(*refs):
    ins, outs = refs[:8], refs[8:16]
    acc_ref = refs[16]
    for part, axis in enumerate(("dp_1", "dp_0")):
        own, a, b, c = ins[4 * part : 4 * part + 4]
        send, keep = outs[4 * part : 4 * part + 3], outs[4 * part + 3]
        acc_ref[...] = own[...] + a[...].astype(F32) + b[...].astype(F32) + c[...].astype(F32)
        extra = acc_ref[256:272, :]
        for k, shift in enumerate(SHIFTS):
            send[k][0:64, :] = acc_ref[pl.ds(pl.multiple_of(spot(axis, shift) * 64, 64), 64), :].astype(BF16)
            send[k][64:80, :] = extra.astype(BF16)
        keep[0:64, :] = acc_ref[pl.ds(pl.multiple_of(spot(axis, 0) * 64, 64), 64), :]
        keep[64:80, :] = extra


def last_kernel(*refs):
    ins = refs[:8]
    first_ref, second_ref, mine_ref, other_ref, square_ref, full_ref = refs[8:]
    core = lax.axis_index("dp_2")
    lead = jnp.where((lax.axis_index("dp_0") == 0) & (lax.axis_index("dp_1") == 0), 1.0, 0.0)
    square = jnp.zeros((1, 1), F32)
    for part in range(2):
        own, a, b, c = ins[4 * part : 4 * part + 4]
        total = own[...] + a[...].astype(F32) + b[...].astype(F32) + c[...].astype(F32)
        grad = total[0:64, :]
        extra = total[64:80, :]
        (first_ref, second_ref)[part][...] = grad.astype(BF16)
        full_ref[:, 512 * part : 512 * (part + 1)] = grad
        square = square + jnp.sum(jnp.sum(grad * grad, axis=1, keepdims=True), axis=0, keepdims=True)
        square = square + lead * jnp.sum(jnp.sum(extra * extra, axis=1, keepdims=True), axis=0, keepdims=True)
    mine_ref[...] = full_ref[pl.ds(pl.multiple_of(core * 32, 32), 32), :]
    other_ref[...] = full_ref[pl.ds(pl.multiple_of((1 - core) * 32, 32), 32), :]
    square_ref[...] = jnp.broadcast_to(square, square_ref.shape)


def weight_kernel(*refs):
    scale_ref, w_ref, accum_ref, rows_accum_ref, mine_ref, theirs_ref = refs[:6]
    stacks = refs[6:22]
    w_out_ref, accum_out_ref = refs[22:]
    core = lax.axis_index("dp_2")
    scale = scale_ref[0:1, 0:1]
    half = mine_ref.shape[1]
    quarter = half // 2
    for side in range(2):
        shift = pl.multiple_of((core if side == 0 else 1 - core) * half, half)
        for part in range(2):
            axes = ("dp_0", "dp_1") if part == 0 else ("dp_1", "dp_0")
            start = pl.multiple_of(shift + part * quarter, quarter)
            for i in range(4):
                stack = stacks[8 * side + 4 * part + i]
                outer = spot(axes[0], ORDER[i])
                for j in range(4):
                    inner = spot(axes[1], ORDER[j])
                    at = outer * 4 + inner if part == 0 else inner * 4 + outer
                    where = (pl.ds(pl.multiple_of(at * 64, 64), 64), pl.ds(start, quarter))
                    grad = scale * stack[64 * j : 64 * (j + 1), :].astype(F32)
                    accum = accum_ref[where].astype(F32) + grad * grad
                    w = w_ref[where].astype(F32)
                    w_out_ref[where] = (w - dense_rate * grad / (jnp.sqrt(accum) + adagrad_eps)).astype(BF16)
        grad = scale * (mine_ref if side == 0 else theirs_ref)[...]
        where = (slice(None), pl.ds(shift, half))
        accum_out_ref[where] = rows_accum_ref[where] + grad * grad


def send(x, axis, shift):
    n = lax.axis_size(axis)
    return lax.ppermute(x, axis, [(i, (i + shift) % n) for i in range(n)])


def exchange(pieces, axis):
    return [send(p, axis, s) for p, s in zip(pieces, SHIFTS)]


def around(x, axis):
    return [send(x, axis, s) for s in SHIFTS]


def body(
    slab_values,
    row_ids,
    peer_counts,
    lookup_slots,
    labels,
    sample_weight,
    weight_in,
    bias_in,
    weight_out,
    dense_accum,
    table_rows,
    table_accum,
):
    batch, features = lookup_slots.shape
    depth, width = weight_in.shape
    half = width // 2
    quarter = half // 2
    lookups_t = lookup_slots.T
    narrow = dense_accum.astype(BF16)
    everyone = lax.all_to_all(jnp.broadcast_to(narrow[None], (32, *narrow.shape)), DP, 0, 0, tiled=True)
    accum_full = everyone.reshape(depth, width)

    pooled = gather_rows(peer_counts, lookups_t, slab_values[0])
    before, after, far = around(pooled, "mp")
    bias = bias_in.reshape(1, width)
    out_w = weight_out.reshape(1, width)
    slope_0, hidden_0, logit_0, turned_0 = forward([pooled], weight_in, bias, out_w)
    slope_1, hidden_1, logit_1, turned_1 = forward([before, after], weight_in, bias, out_w)
    slope_2, hidden_2, logit_2, turned_2 = forward([far], weight_in, bias, out_w)
    turned = [turned_0, turned_1, turned_2]
    turned = turned + [send(t, "dp_2", 1) for t in turned]
    logits = jnp.concatenate([logit_0, logit_1, logit_2], axis=0)
    logit_before, logit_after, logit_far = around(logits, "mp")
    dact, other, sums_mine, sums_other = call(
        slope_kernel,
        [((4 * batch, width), BF16), ((4 * batch, half), BF16), ((16, half), F32), ((16, half), F32)],
        "slopes",
        2 * 10**9,
        (
            *slope_0,
            *slope_1,
            *slope_2,
            hidden_0,
            hidden_1,
            hidden_2,
            logits,
            logit_before,
            logit_after,
            logit_far,
            labels.reshape(4, batch),
            sample_weight.reshape(4, batch),
        ),
        [pltpu.VMEM((16, width), F32)],
    )
    far_dact = send(other, "dp_2", 1)
    far_sums = send(sums_other, "dp_2", 1)

    def back(k):
        return lax.dot_general(
            dact[k * batch : (k + 1) * batch], weight_in, (((1,), (1,)), ((), ())), preferred_element_type=F32
        )

    to_far = back(3).astype(BF16)
    from_far = send(to_far, "mp", 2)
    to_before = back(1).astype(BF16)
    from_after = send(to_before, "mp", 3)
    to_after = back(2).astype(BF16)
    from_before = send(to_after, "mp", 1)
    stage = [((272, quarter), BF16)] * 3 + [((272, quarter), F32)]
    common = (*turned, dact, far_dact, sums_mine, far_sums)
    scratch = [pltpu.VMEM((depth, quarter), F32)]
    a = call(functools.partial(grad_kernel, 0), stage, "grad_a", 4 * 10**9, common, scratch)
    a_in = exchange(a[:3], "dp_0")
    b = call(functools.partial(grad_kernel, 1), stage, "grad_b", 4 * 10**9, common, scratch)
    b_in = exchange(b[:3], "dp_1")
    own = back(0)
    stage = [((80, quarter), BF16)] * 3 + [((80, quarter), F32)]
    m = call(
        middle_kernel, stage + stage, "middle", 10**8, (a[3], *a_in, b[3], *b_in), [pltpu.VMEM((272, quarter), F32)]
    )
    a_in = exchange(m[0:3], "dp_1")
    b_in = exchange(m[4:7], "dp_0")
    first, second, mine, others, square = call(
        last_kernel,
        [((64, quarter), BF16)] * 2 + [((32, half), F32)] * 2 + [((8, 128), F32)],
        "last",
        10**8,
        (m[3], *a_in, m[7], *b_in),
        [pltpu.VMEM((64, half), F32)],
    )
    theirs = send(others, "dp_2", 1)
    a_stack = jnp.concatenate([first, *around(first, "dp_1")], axis=0)
    b_stack = jnp.concatenate([second, *around(second, "dp_0")], axis=0)
    stacks = [a_stack, *around(a_stack, "dp_0"), b_stack, *around(b_stack, "dp_1")]
    stacks = stacks + [send(s, "dp_2", 1) for s in stacks]

    outgoing = slot_sums(peer_counts, lookups_t, row_ids[0], own, [from_before, from_after, from_far], square)
    arrived = lax.all_to_all(outgoing, DP_MP, 0, 0, tiled=True)
    table_t, accum_t, scale = table_update(
        arrived, table_rows.T, table_accum.reshape(1, -1), table_rate, adagrad_eps, clip_norm
    )
    weight_new, accum_new = call(
        weight_kernel,
        [((depth, width), BF16), (dense_accum.shape, F32)],
        "weights",
        10**9,
        (scale, weight_in, accum_full, dense_accum, mine, theirs, *stacks),
    )
    return (weight_new, accum_new, table_t.T, accum_t.reshape(-1))


def solution(mesh):
    torus = Mesh(mesh.devices.reshape(4, 4, 2, mesh.shape["mp"]), ("dp_0", "dp_1", "dp_2", "mp"))
    placed = (
        P(DP_MP, None, None),
        P(DP_MP, None, None),
        P(DP_MP, None),
        P(DP_MP, None),
        P(DP),
        P(DP),
        P(None, "mp"),
        P("mp"),
        P("mp"),
        P(DP, "mp"),
        P(DP_MP, None),
        P(DP_MP),
    )
    return jax.shard_map(
        body,
        mesh=torus,
        in_specs=placed,
        out_specs=(P(None, "mp"), P(DP, "mp"), P(DP_MP, None), P(DP_MP)),
        check_vma=False,
    )
```

```python
import functools
import math

import jax
import jax.numpy as jnp
from jax import lax
from jax.experimental import pallas as pl
from jax.experimental.pallas import tpu as pltpu
from jax.sharding import Mesh
from jax.sharding import PartitionSpec as P


DP = ("dp_0", "dp_1", "dp_2")
DP_MP = ("dp_0", "dp_1", "dp_2", "mp")

clip_norm = 1.0
dense_rate = 0.02
table_rate = 0.5
adagrad_eps = 1e-10

F32 = jnp.float32
BF16 = jnp.bfloat16
VM = pl.BlockSpec(memory_space=pltpu.VMEM)


def iota(shape, dim):
    return lax.broadcasted_iota(jnp.int32, shape, dim)


def dot_f32(a, b, dims=(((1,), (0,)), ((), ()))):
    return lax.dot_general(a, b, dims, preferred_element_type=F32)


def hot_rows(counts_ref, lookups_ref):
    owners = counts_ref.shape[1]
    features = lookups_ref.shape[0]
    spread = jnp.broadcast_to(counts_ref[...].astype(F32), (owners, owners))
    at, of = iota((owners, owners), 0), iota((owners, owners), 1)
    ends = jnp.sum(jnp.where(of <= at, spread, 0.0), axis=1, keepdims=True)
    starts = ends - jnp.sum(jnp.where(of == at, spread, 0.0), axis=1, keepdims=True)
    hots, slots = [], []
    for f in range(features):
        q = lookups_ref[f : f + 1, :].astype(F32)
        match = (q >= starts) & (q < ends)
        hots.append(jnp.where(match, 1.0, 0.0))
        slots.append(q - jnp.sum(jnp.where(match, starts, 0.0), axis=0, keepdims=True))
    return hots, slots


def gather_kernel(counts_ref, lookups_ref, slab_ref, out_ref):
    features, batch = lookups_ref.shape
    halfway = slab_ref.shape[1] // 2
    hots, slots = hot_rows(counts_ref, lookups_ref)
    inner = jnp.concatenate([jnp.where(s >= 16.0, s - 16.0, s) for s in slots], axis=0).T
    halves = jnp.concatenate([slab_ref[:, :halfway], slab_ref[:, halfway:]], axis=0)
    low_lane = iota((batch, 128), 1) < 64
    for pair in range(features // 2):
        both = []
        for parity in range(2):
            f = 2 * pair + parity
            upper = slots[f] >= 16.0
            hot = jnp.concatenate(
                [jnp.where(upper, 0.0, hots[f]), jnp.where(upper, hots[f], 0.0)], axis=0
            ).astype(BF16)
            rows = dot_f32(hot, halves, (((0,), (0,)), ((), ())))
            place = jnp.broadcast_to(inner[:, f : f + 1], (batch, 128))
            block = jnp.floor(place * 0.5)
            found = rows[:, :128]
            for k in range(1, 8):
                found = jnp.where(block == float(k), rows[:, 128 * k : 128 * (k + 1)], found)
            swap = place - 2.0 * block != float(parity)
            both.append(jnp.where(swap, pltpu.roll(found, 64, 1), found))
        out_ref[:, 128 * pair : 128 * (pair + 1)] = jnp.where(low_lane, both[0], both[1]).astype(BF16)


def gather_rows(counts, lookups_t, slab):
    features, batch = lookups_t.shape
    return pl.pallas_call(
        gather_kernel,
        out_shape=jax.ShapeDtypeStruct((batch, features * 64), BF16),
        in_specs=[VM, VM, VM],
        out_specs=VM,
        name="gather_rows",
        compiler_params=pltpu.CompilerParams(vmem_limit_bytes=16 * 2**20),
        cost_estimate=pl.CostEstimate(flops=6 * 10**9, transcendentals=0, bytes_accessed=2 * 10**6),
    )(counts, lookups_t, slab)


def slot_kernel(counts_ref, lookups_ref, ids_ref, own_ref, a_ref, b_ref, c_ref, dense_ref, out_ref, acc_ref):
    owners = counts_ref.shape[1]
    features, batch = lookups_ref.shape
    width = out_ref.shape[1] - 128
    half_width = width // 2
    counts = counts_ref[...].astype(F32)
    lower = iota((owners, owners), 1) <= iota((owners, owners), 0)
    spread = jnp.broadcast_to(counts, (owners, owners))
    ends = jnp.sum(jnp.where(lower, spread, 0.0), axis=1, keepdims=True)
    starts = ends - jnp.sum(
        jnp.where(iota((owners, owners), 1) == iota((owners, owners), 0), spread, 0.0), axis=1, keepdims=True
    )
    hots, inners = [], []
    for f in range(features):
        q = lookups_ref[f : f + 1, :].astype(F32)
        match = (q >= starts) & (q < ends)
        begin = jnp.sum(jnp.where(match, starts, 0.0), axis=0, keepdims=True)
        slot = q - begin
        upper = slot >= 16.0
        chosen = jnp.where(match, 1.0, 0.0)
        hots.append(
            jnp.concatenate([jnp.where(upper, 0.0, chosen), jnp.where(upper, chosen, 0.0)], axis=0).astype(BF16)
        )
        inners.append(jnp.where(upper, slot - 16.0, slot))
    inner = jnp.concatenate(inners, axis=0).T
    lane = iota((batch, 128), 1)
    low_lane = lane < 64
    offset = jnp.where(low_lane, 0.0, 1.0)
    for pair in range(features // 2):
        cols = slice(128 * pair, 128 * (pair + 1))
        total = own_ref[:, cols] + a_ref[:, cols].astype(F32) + b_ref[:, cols].astype(F32) + c_ref[:, cols].astype(F32)
        turned = pltpu.roll(total, 64, 1)
        for parity in range(2):
            f = 2 * pair + parity
            rows = jnp.where(low_lane, total, turned) if parity == 0 else jnp.where(low_lane, turned, total)
            target = jnp.broadcast_to(inner[:, f : f + 1], (batch, 128)) - offset
            high = rows.astype(BF16).astype(F32)
            low = rows - high
            spread_high, spread_low = [], []
            for k in range(8):
                mask = target == float(2 * k)
                spread_high.append(jnp.where(mask, high, 0.0).astype(BF16))
                spread_low.append(jnp.where(mask, low, 0.0).astype(BF16))
            values = jnp.concatenate(
                [jnp.concatenate(spread_high, axis=1), jnp.concatenate(spread_low, axis=1)], axis=0
            )
            hot = jnp.concatenate([hots[f], hots[f]], axis=1)
            part = dot_f32(hot, values)
            if f == 0:
                acc_ref[...] = part
            else:
                acc_ref[...] = acc_ref[...] + part
    acc = acc_ref[...]
    out_ref[:, :half_width] = acc[:owners].astype(BF16)
    out_ref[:, half_width:width] = acc[owners:].astype(BF16)
    square = jnp.sum(jnp.sum(acc * acc, axis=1, keepdims=True), axis=0, keepdims=True)
    square = square + dense_ref[0:1, 0:1]
    top = square.astype(BF16).astype(F32)
    mid = (square - top).astype(BF16).astype(F32)
    end = square - top - mid
    ids = ids_ref[...]
    block = ids >> 8
    inside = ids & 255
    tail_lane = iota((owners, 128 - 2 * ids.shape[1]), 1)
    tail = jnp.where(tail_lane == 0, top, jnp.where(tail_lane == 1, mid, jnp.where(tail_lane == 2, end, 0.0)))
    out_ref[:, width:] = jnp.concatenate([block.astype(F32), inside.astype(F32), tail], axis=1).astype(BF16)


def slot_sums(counts, lookups_t, ids, own, pieces, dense_square):
    owners, capacity = ids.shape
    return pl.pallas_call(
        slot_kernel,
        out_shape=jax.ShapeDtypeStruct((owners, capacity * 64 + 128), BF16),
        in_specs=[VM] * 8,
        out_specs=VM,
        scratch_shapes=[pltpu.VMEM((2 * owners, capacity * 32), F32)],
        name="slot_sums",
        compiler_params=pltpu.CompilerParams(vmem_limit_bytes=24 * 2**20),
        cost_estimate=pl.CostEstimate(flops=8 * 10**9, transcendentals=0, bytes_accessed=3 * 10**6),
    )(counts, lookups_t, ids, own, *pieces, dense_square)


def table_kernel(rate, eps, clip, arrived_ref, table_ref, accum_ref, table_out, accum_out, scale_out, acc_ref):
    sources = arrived_ref.shape[0]
    width = arrived_ref.shape[1] - 128
    capacity = width // 64
    rows = table_ref.shape[1]
    blocks = rows // 256
    info = arrived_ref[:, width:].astype(F32).T
    squares = info[2 * capacity : 2 * capacity + 8, :]
    squares = jnp.sum(squares[0:3, :], axis=0, keepdims=True)
    total = jnp.sum(squares, axis=1, keepdims=True)
    scale = clip / jnp.maximum(jnp.sqrt(total), clip)
    scale_out[...] = jnp.broadcast_to(scale, scale_out.shape)
    inside_at = iota((256, sources), 0).astype(F32)
    for pair in range(capacity // 2):
        turned = arrived_ref[:, 128 * pair : 128 * (pair + 1)].astype(F32).T
        spread, hots = [], []
        for parity in range(2):
            c = 2 * pair + parity
            piece = turned[64 * parity : 64 * (parity + 1), :]
            block = info[c : c + 1, :]
            inside = info[capacity + c : capacity + c + 1, :]
            hots.append(jnp.where(inside_at == inside, 1.0, 0.0).astype(BF16))
            spread.append(
                jnp.concatenate([jnp.where(block == float(k), piece, 0.0).astype(BF16) for k in range(blocks)], axis=0)
            )
        part = dot_f32(
            jnp.concatenate(spread, axis=1), jnp.concatenate(hots, axis=1), (((1,), (1,)), ((), ()))
        )
        if pair == 0:
            acc_ref[...] = part
        else:
            acc_ref[...] = acc_ref[...] + part
    for k in range(blocks):
        received = scale * acc_ref[64 * k : 64 * (k + 1), :]
        cols = slice(256 * k, 256 * (k + 1))
        accum = accum_ref[:, cols] + jnp.sum(received * received, axis=0, keepdims=True) * (1.0 / 64.0)
        accum_out[:, cols] = accum
        table_out[:, cols] = table_ref[:, cols] - rate * received / (jnp.sqrt(accum) + eps)


def table_update(arrived, table_t, accum, rate, eps, clip):
    width, rows = table_t.shape
    return pl.pallas_call(
        functools.partial(table_kernel, rate, eps, clip),
        out_shape=(
            jax.ShapeDtypeStruct((width, rows), F32),
            jax.ShapeDtypeStruct((1, rows), F32),
            jax.ShapeDtypeStruct((8, 128), F32),
        ),
        in_specs=[VM] * 3,
        out_specs=(VM, VM, VM),
        scratch_shapes=[pltpu.VMEM((rows // 4, 256), F32)],
        name="table_update",
        compiler_params=pltpu.CompilerParams(vmem_limit_bytes=20 * 2**20),
        cost_estimate=pl.CostEstimate(flops=6 * 10**9, transcendentals=0, bytes_accessed=3 * 10**6),
    )(arrived, table_t, accum)


def footprint(shapes):
    return sum(math.prod(s.shape) * jnp.dtype(s.dtype).itemsize for s in shapes)


def call(kernel, outs, flops, args, scratch=(), spare=8):
    shapes = tuple(jax.ShapeDtypeStruct(s, t) for s, t in outs)
    held = footprint(args) + footprint(shapes) + footprint(scratch)
    res = pl.pallas_call(
        kernel,
        out_shape=shapes,
        in_specs=[VM] * len(args),
        out_specs=tuple(VM for _ in shapes),
        scratch_shapes=list(scratch),
        compiler_params=pltpu.CompilerParams(vmem_limit_bytes=held + spare * 2**20),
        cost_estimate=pl.CostEstimate(flops=flops, transcendentals=0, bytes_accessed=2 * 10**6),
    )(*args)
    return res


SHIFTS = (1, 3, 2)


def spot(axis, shift):
    return lax.rem(lax.axis_index(axis) + shift, 4)


def sigmoid(x):
    return 0.5 * jnp.tanh(0.5 * x) + 0.5


def forward_kernel(chunks, *refs):
    ins, (w_ref, bias_ref, out_w_ref) = refs[:chunks], refs[chunks : chunks + 3]
    slope_ref, hidden_ref, logit_ref, turned_ref = refs[chunks + 3 :]
    rows = ins[0].shape[0]
    width = w_ref.shape[1]
    for k in range(chunks):
        turned_ref[:, rows * k : rows * (k + 1)] = ins[k][...].T

    def columns(n, carry):
        cols = pl.ds(pl.multiple_of(n * 256, 256), 256)
        w = w_ref[:, cols]
        out_w = out_w_ref[:, cols].astype(F32)
        for k in range(chunks):
            act = dot_f32(ins[k][...], w) + bias_ref[:, cols]
            sigma = sigmoid(act)
            hidden_ref[rows * k : rows * (k + 1), cols] = (act * sigma).astype(BF16)
            slope_ref[rows * k : rows * (k + 1), cols] = out_w * sigma * (1.0 + act * (1.0 - sigma))
        return carry

    lax.fori_loop(0, width // 256, columns, 0)
    out_w = jnp.broadcast_to(out_w_ref[...], (16, width))
    for k in range(chunks):
        part = dot_f32(out_w, hidden_ref[rows * k : rows * (k + 1), :], (((1,), (1,)), ((), ())))
        at = rows * k
        logit_ref[at // 256 : at // 256 + 1, at % 256 : at % 256 + rows] = part[0:1, :]


def forward(chunks, w, bias, out_w):
    rows, depth = chunks[0].shape
    width = w.shape[1]
    n = len(chunks)
    total = n * rows
    outs = [((total, width), F32), ((total, width), BF16), ((total // 256, 256), F32), ((depth, total), BF16)]
    return call(functools.partial(forward_kernel, n), outs, total * 10**7, (*chunks, w, bias, out_w))


ORDER = (0, 3, 1, 2)
PARTNERS = ((0, 1, 2, 3), (2, 0, 3, 1), (1, 3, 0, 2), (3, 2, 1, 0))


def slope_kernel(*refs):
    slopes, hiddens = refs[0:3], refs[3:6]
    own_ref, prev_ref, next_ref, far_ref, labels_ref, weight_ref = refs[6:12]
    dact_ref, other_ref, sums_mine_ref, sums_other_ref, sums_ref = refs[12:]
    rows, width = slopes[0].shape
    spans = ((0, 0), (1, 0), (1, rows), (2, 0))
    half = width // 2
    core = lax.axis_index("dp_2")
    dlogits = []
    for k in range(4):
        at = spot("mp", ORDER[k])
        logit = (own_ref[k : k + 1, :] + far_ref[PARTNERS[3][k] : PARTNERS[3][k] + 1, :]) + (
            prev_ref[PARTNERS[1][k] : PARTNERS[1][k] + 1, :] + next_ref[PARTNERS[2][k] : PARTNERS[2][k] + 1, :]
        )
        label = labels_ref[pl.ds(at, 1), :].astype(F32)
        dlogits.append(weight_ref[pl.ds(at, 1), :] * (sigmoid(logit) - label))
    rows_form = jnp.concatenate(dlogits + [jnp.zeros((4, rows), F32)], axis=0)
    cols_form = rows_form.T
    for k in range(4):
        which, start = spans[k]
        col = cols_form[:, k : k + 1]
        dact_ref[rows * k : rows * (k + 1), :] = (slopes[which][start : start + rows, :] * col).astype(BF16)
    other_ref[...] = dact_ref[:, pl.ds(pl.multiple_of((1 - core) * half, half), half)]
    ones = jnp.ones((16, rows), BF16)
    bias_sum = jnp.zeros((16, width), F32)
    out_sum = jnp.zeros((16, width), F32)
    for k in range(4):
        bias_sum = bias_sum + dot_f32(ones, dact_ref[rows * k : rows * (k + 1), :])
        d = dlogits[k]
        top = d.astype(BF16)
        rest = (d - top.astype(F32)).astype(BF16)
        pick = iota((16, rows), 0)
        left = jnp.where(pick == 0, top.astype(F32), jnp.where(pick == 1, rest.astype(F32), 0.0)).astype(BF16)
        which, start = spans[k]
        out_sum = out_sum + dot_f32(left, hiddens[which][start : start + rows, :])
    pick = iota((16, width), 0)
    total = jnp.sum(out_sum, axis=0, keepdims=True)
    sums_ref[...] = jnp.where(pick == 0, bias_sum, jnp.where(pick == 1, total, 0.0))
    sums_mine_ref[...] = sums_ref[:, pl.ds(pl.multiple_of(core * half, half), half)]
    sums_other_ref[...] = sums_ref[:, pl.ds(pl.multiple_of((1 - core) * half, half), half)]


def back_kernel(first, count, dact_ref, w_ref, *outs):
    rows = outs[0].shape[0]
    for k in range(count):
        start = rows * (first + k)
        part = dot_f32(dact_ref[start : start + rows, :], w_ref[...], (((1,), (1,)), ((), ())))
        outs[k][...] = part.astype(outs[k].dtype)


def grad_kernel(second, *refs):
    turned, (dact_ref, far_dact_ref, sums_a_ref, sums_b_ref) = refs[0:6], refs[6:10]
    outs, own_ref, acc_ref = refs[10:13], refs[13], refs[14]
    depth = turned[0].shape[0]
    half = far_dact_ref.shape[1]
    quarter = half // 2
    core = lax.axis_index("dp_2")
    spans = ((0, 256), (256, 512), (768, 256))
    start = pl.multiple_of(core * half + second * quarter, quarter)
    local = dact_ref[:, pl.ds(start, quarter)]
    remote = far_dact_ref[:, second * quarter : (second + 1) * quarter]
    extra = sums_a_ref[:, second * quarter : (second + 1) * quarter] + sums_b_ref[:, second * quarter : (second + 1) * quarter]

    def block(row):
        part = None
        for i, (s, n) in enumerate(spans):
            for source, d in ((turned[i], local), (turned[i + 3], remote)):
                p = dot_f32(source[pl.ds(row, 256), :], d[s : s + n, :])
                part = p if part is None else part + p
        return part

    def rows(x, carry):
        at = pl.multiple_of(x * 256, 256)
        acc_ref[pl.ds(at, 256), :] = block(at)
        return carry

    lax.fori_loop(0, depth // 256, rows, 0)
    for k, shift in enumerate((*SHIFTS, 0)):
        target = (*outs, own_ref)[k]
        if second:
            for x in range(4):
                at = pl.multiple_of(spot("dp_1", shift) * 64 + 256 * x, 64)
                target[64 * x : 64 * (x + 1), :] = acc_ref[pl.ds(at, 64), :].astype(target.dtype)
        else:
            at = pl.multiple_of(spot("dp_0", shift) * 256, 256)
            target[0:256, :] = acc_ref[pl.ds(at, 256), :].astype(target.dtype)
    for k in range(3):
        outs[k][256:272, :] = extra.astype(BF16)
    own_ref[256:272, :] = extra


def middle_kernel(*refs):
    ins, outs = refs[:8], refs[8:16]
    acc_ref = refs[16]
    for part, axis in enumerate(("dp_1", "dp_0")):
        own, a, b, c = ins[4 * part : 4 * part + 4]
        send, keep = outs[4 * part : 4 * part + 3], outs[4 * part + 3]
        acc_ref[...] = own[...] + a[...].astype(F32) + b[...].astype(F32) + c[...].astype(F32)
        extra = acc_ref[256:272, :]
        for k, shift in enumerate(SHIFTS):
            send[k][0:64, :] = acc_ref[pl.ds(pl.multiple_of(spot(axis, shift) * 64, 64), 64), :].astype(BF16)
            send[k][64:80, :] = extra.astype(BF16)
        keep[0:64, :] = acc_ref[pl.ds(pl.multiple_of(spot(axis, 0) * 64, 64), 64), :]
        keep[64:80, :] = extra


def last_kernel(*refs):
    ins = refs[:8]
    first_ref, second_ref, mine_ref, other_ref, square_ref, full_ref = refs[8:]
    core = lax.axis_index("dp_2")
    lead = jnp.where((lax.axis_index("dp_0") == 0) & (lax.axis_index("dp_1") == 0), 1.0, 0.0)
    square = jnp.zeros((1, 1), F32)
    for part in range(2):
        own, a, b, c = ins[4 * part : 4 * part + 4]
        total = own[...] + a[...].astype(F32) + b[...].astype(F32) + c[...].astype(F32)
        grad = total[0:64, :]
        extra = total[64:80, :]
        (first_ref, second_ref)[part][...] = grad.astype(BF16)
        full_ref[:, 512 * part : 512 * (part + 1)] = grad
        square = square + jnp.sum(jnp.sum(grad * grad, axis=1, keepdims=True), axis=0, keepdims=True)
        square = square + lead * jnp.sum(jnp.sum(extra * extra, axis=1, keepdims=True), axis=0, keepdims=True)
    mine_ref[...] = full_ref[pl.ds(pl.multiple_of(core * 32, 32), 32), :]
    other_ref[...] = full_ref[pl.ds(pl.multiple_of((1 - core) * 32, 32), 32), :]
    square_ref[...] = jnp.broadcast_to(square, square_ref.shape)


def weight_kernel(*refs):
    scale_ref, w_ref, accum_mine_ref, accum_theirs_ref, rows_accum_ref, mine_ref, theirs_ref = refs[:7]
    stacks = refs[7:23]
    w_out_ref, accum_out_ref = refs[23:]
    core = lax.axis_index("dp_2")
    scale = scale_ref[0:1, 0:1]
    half = mine_ref.shape[1]
    quarter = half // 2
    for side in range(2):
        shift = pl.multiple_of((core if side == 0 else 1 - core) * half, half)
        for part in range(2):
            axes = ("dp_0", "dp_1") if part == 0 else ("dp_1", "dp_0")
            start = pl.multiple_of(shift + part * quarter, quarter)
            for i in range(4):
                stack = stacks[8 * side + 4 * part + i]
                outer = spot(axes[0], ORDER[i])
                for j in range(4):
                    inner = spot(axes[1], ORDER[j])
                    at = outer * 4 + inner if part == 0 else inner * 4 + outer
                    where = (pl.ds(pl.multiple_of(at * 64, 64), 64), pl.ds(start, quarter))
                    grad = scale * stack[64 * j : 64 * (j + 1), :].astype(F32)
                    held = (accum_mine_ref, accum_theirs_ref)[side][where[0], quarter * part : quarter * (part + 1)]
                    accum = held.astype(F32) + grad * grad
                    w = w_ref[where].astype(F32)
                    w_out_ref[where] = (w - dense_rate * grad / (jnp.sqrt(accum) + adagrad_eps)).astype(BF16)
        grad = scale * (mine_ref if side == 0 else theirs_ref)[...]
        where = (slice(None), pl.ds(shift, half))
        accum_out_ref[where] = rows_accum_ref[where] + grad * grad


def send(x, axis, shift):
    n = lax.axis_size(axis)
    return lax.ppermute(x, axis, [(i, (i + shift) % n) for i in range(n)])


def exchange(pieces, axis):
    return [send(p, axis, s) for p, s in zip(pieces, SHIFTS)]


def around(x, axis):
    return [send(x, axis, s) for s in SHIFTS]


def inner(
    slab_values,
    row_ids,
    peer_counts,
    lookup_slots,
    labels,
    sample_weight,
    weight_in,
    bias_in,
    weight_out,
    dense_accum,
    table_rows,
    table_accum,
):
    batch, _ = lookup_slots.shape
    depth, width = weight_in.shape
    half = width // 2
    quarter = half // 2
    lookups_t = lookup_slots.T
    pooled = gather_rows(peer_counts, lookups_t, slab_values[0])
    before, after = send(pooled, "mp", 1), send(pooled, "mp", 3)
    core = lax.axis_index("dp_2")
    narrow = jnp.stack([dense_accum[:, :half], dense_accum[:, half:]]).astype(BF16)
    keep = lax.dynamic_index_in_dim(narrow, core, 0, False)
    give = send(lax.dynamic_index_in_dim(narrow, 1 - core, 0, False), "dp_2", 1)
    both = jnp.where(core == 0, jnp.concatenate([keep, give], 0), jnp.concatenate([give, keep], 0))
    spread = jnp.broadcast_to(both[None], (16, *both.shape))
    accum_mine = lax.all_to_all(spread, ("dp_0", "dp_1"), 0, 0, tiled=True).reshape(depth, half)
    accum_theirs = send(accum_mine, "dp_2", 1)
    bias = bias_in.reshape(1, width)
    out_w = weight_out.reshape(1, width)
    far_low, far_high = send(before[: batch // 2], "mp", 1), send(after[batch // 2 :], "mp", 3)
    slope_0, hidden_0, logit_0, turned_0 = forward([pooled], weight_in, bias, out_w)
    slope_1, hidden_1, logit_1, turned_1 = forward([before, after], weight_in, bias, out_w)
    slope_2, hidden_2, logit_2, turned_2 = forward([far_low, far_high], weight_in, bias, out_w)
    turned = [turned_0, turned_1, turned_2]
    turned = turned + [send(t, "dp_2", 1) for t in turned]
    logits = jnp.concatenate([logit_0, logit_1, logit_2], axis=0)
    logit_before, logit_after, logit_far = around(logits, "mp")
    dact, other, sums_mine, sums_other = call(
        slope_kernel,
        [((4 * batch, width), BF16), ((4 * batch, half), BF16), ((16, half), F32), ((16, half), F32)],
        2 * 10**9,
        (
            slope_0,
            slope_1,
            slope_2,
            hidden_0,
            hidden_1,
            hidden_2,
            logits,
            logit_before,
            logit_after,
            logit_far,
            labels.reshape(4, batch),
            sample_weight.reshape(4, batch),
        ),
        [pltpu.VMEM((16, width), F32)],
    )
    far_dact = send(other, "dp_2", 1)
    far_sums = send(sums_other, "dp_2", 1)

    def back(first, count, kind):
        return call(
            functools.partial(back_kernel, first, count),
            [((batch, depth), kind)] * count,
            count * 10**9,
            (dact, weight_in),
        )

    (to_far,) = back(3, 1, BF16)
    from_far = send(to_far, "mp", 2)
    to_before, to_after = back(1, 2, BF16)
    from_after = send(to_before, "mp", 3)
    from_before = send(to_after, "mp", 1)
    stage = [((272, quarter), BF16)] * 3 + [((272, quarter), F32)]
    common = (*turned, dact, far_dact, sums_mine, far_sums)
    scratch = [pltpu.VMEM((depth, quarter), F32)]
    a = call(functools.partial(grad_kernel, 0), stage, 4 * 10**9, common, scratch)
    a_in = exchange(a[:3], "dp_0")
    b = call(functools.partial(grad_kernel, 1), stage, 4 * 10**9, common, scratch)
    b_in = exchange(b[:3], "dp_1")
    (own,) = back(0, 1, F32)
    stage = [((80, quarter), BF16)] * 3 + [((80, quarter), F32)]
    m = call(middle_kernel, stage + stage, 10**8, (a[3], *a_in, b[3], *b_in), [pltpu.VMEM((272, quarter), F32)])
    a_in = exchange(m[0:3], "dp_1")
    b_in = exchange(m[4:7], "dp_0")
    first, second, mine, others, square = call(
        last_kernel,
        [((64, quarter), BF16)] * 2 + [((32, half), F32)] * 2 + [((8, 128), F32)],
        10**8,
        (m[3], *a_in, m[7], *b_in),
        [pltpu.VMEM((64, half), F32)],
    )
    theirs = send(others, "dp_2", 1)
    a_stack = jnp.concatenate([first, *around(first, "dp_1")], axis=0)
    b_stack = jnp.concatenate([second, *around(second, "dp_0")], axis=0)
    stacks = [a_stack, *around(a_stack, "dp_0"), b_stack, *around(b_stack, "dp_1")]
    stacks = stacks + [send(s, "dp_2", 1) for s in stacks]

    outgoing = slot_sums(peer_counts, lookups_t, row_ids[0], own, [from_before, from_after, from_far], square)
    arrived = lax.all_to_all(outgoing, DP_MP, 0, 0, tiled=True)
    table_t, accum_t, scale = table_update(
        arrived, table_rows.T, table_accum.reshape(1, -1), table_rate, adagrad_eps, clip_norm
    )
    weight_new, accum_new = call(
        weight_kernel,
        [((depth, width), BF16), (dense_accum.shape, F32)],
        10**9,
        (scale, weight_in, accum_mine, accum_theirs, dense_accum, mine, theirs, *stacks),
    )
    return (weight_new, accum_new, table_t.T, accum_t.reshape(-1))


def solution(mesh):
    torus = Mesh(mesh.devices.reshape(4, 4, 2, mesh.shape["mp"]), ("dp_0", "dp_1", "dp_2", "mp"))
    placed = (
        P(DP_MP, None, None),
        P(DP_MP, None, None),
        P(DP_MP, None),
        P(DP_MP, None),
        P(DP),
        P(DP),
        P(None, "mp"),
        P("mp"),
        P("mp"),
        P(DP, "mp"),
        P(DP_MP, None),
        P(DP_MP),
    )
    return jax.shard_map(
        inner,
        mesh=torus,
        in_specs=placed,
        out_specs=(P(None, "mp"), P(DP, "mp"), P(DP_MP, None), P(DP_MP)),
        check_vma=False,
    )
```

```python
import functools
import math

import jax
import jax.numpy as jnp
from jax import lax
from jax.experimental import pallas as pl
from jax.experimental.pallas import tpu as pltpu
from jax.sharding import Mesh
from jax.sharding import PartitionSpec as P


DP = ("dp_0", "dp_1", "dp_2")
DP_MP = ("dp_0", "dp_1", "dp_2", "mp")

clip_norm = 1.0
dense_rate = 0.02
table_rate = 0.5
adagrad_eps = 1e-10

F32 = jnp.float32
BF16 = jnp.bfloat16
VM = pl.BlockSpec(memory_space=pltpu.VMEM)


def iota(shape, dim):
    return lax.broadcasted_iota(jnp.int32, shape, dim)


def dot_f32(a, b, dims=(((1,), (0,)), ((), ()))):
    return lax.dot_general(a, b, dims, preferred_element_type=F32)


def hot_rows(counts_ref, lookups_ref):
    owners = counts_ref.shape[1]
    features = lookups_ref.shape[0]
    spread = jnp.broadcast_to(counts_ref[...].astype(F32), (owners, owners))
    at, of = iota((owners, owners), 0), iota((owners, owners), 1)
    ends = jnp.sum(jnp.where(of <= at, spread, 0.0), axis=1, keepdims=True)
    starts = ends - jnp.sum(jnp.where(of == at, spread, 0.0), axis=1, keepdims=True)
    hots, slots = [], []
    for f in range(features):
        q = lookups_ref[f : f + 1, :].astype(F32)
        match = (q >= starts) & (q < ends)
        hots.append(jnp.where(match, 1.0, 0.0))
        slots.append(q - jnp.sum(jnp.where(match, starts, 0.0), axis=0, keepdims=True))
    return hots, slots


def gather_kernel(counts_ref, lookups_ref, slab_ref, out_ref):
    features, batch = lookups_ref.shape
    halfway = slab_ref.shape[1] // 2
    hots, slots = hot_rows(counts_ref, lookups_ref)
    inner = jnp.concatenate([jnp.where(s >= 16.0, s - 16.0, s) for s in slots], axis=0).T
    halves = jnp.concatenate([slab_ref[:, :halfway], slab_ref[:, halfway:]], axis=0)
    low_lane = iota((batch, 128), 1) < 64
    for pair in range(features // 2):
        both = []
        for parity in range(2):
            f = 2 * pair + parity
            upper = slots[f] >= 16.0
            hot = jnp.concatenate(
                [jnp.where(upper, 0.0, hots[f]), jnp.where(upper, hots[f], 0.0)], axis=0
            ).astype(BF16)
            rows = dot_f32(hot, halves, (((0,), (0,)), ((), ())))
            place = jnp.broadcast_to(inner[:, f : f + 1], (batch, 128))
            block = jnp.floor(place * 0.5)
            found = rows[:, :128]
            for k in range(1, 8):
                found = jnp.where(block == float(k), rows[:, 128 * k : 128 * (k + 1)], found)
            swap = place - 2.0 * block != float(parity)
            both.append(jnp.where(swap, pltpu.roll(found, 64, 1), found))
        out_ref[:, 128 * pair : 128 * (pair + 1)] = jnp.where(low_lane, both[0], both[1]).astype(BF16)


def gather_rows(counts, lookups_t, slab):
    features, batch = lookups_t.shape
    return pl.pallas_call(
        gather_kernel,
        out_shape=jax.ShapeDtypeStruct((batch, features * 64), BF16),
        in_specs=[VM, VM, VM],
        out_specs=VM,
        name="gather_rows",
        compiler_params=pltpu.CompilerParams(vmem_limit_bytes=16 * 2**20),
        cost_estimate=pl.CostEstimate(flops=6 * 10**9, transcendentals=0, bytes_accessed=2 * 10**6),
    )(counts, lookups_t, slab)


def slot_kernel(
    counts_ref, lookups_ref, ids_ref, own_ref, a_ref, b_ref, c_ref, dense_ref, out_ref, value_ref, at_ref
):
    owners = counts_ref.shape[1]
    capacity = ids_ref.shape[1]
    features, batch = lookups_ref.shape
    spread = jnp.broadcast_to(counts_ref[...].astype(F32), (owners, owners))
    at, of = iota((owners, owners), 0), iota((owners, owners), 1)
    ends = jnp.sum(jnp.where(of <= at, spread, 0.0), axis=1, keepdims=True)
    starts = ends - jnp.sum(jnp.where(of == at, spread, 0.0), axis=1, keepdims=True)
    moves = iota((owners, 1), 0).astype(F32) * float(capacity) - starts
    indices = []
    for f in range(features):
        q = lookups_ref[f : f + 1, :].astype(F32)
        match = (q >= starts) & (q < ends)
        indices.append(q + jnp.sum(jnp.where(match, moves, 0.0), axis=0, keepdims=True))
        at_ref[0:1, batch * f : batch * (f + 1)] = jnp.floor(indices[f] * 0.5)
    index = jnp.concatenate(indices, axis=0)
    odd = (index - 2.0 * jnp.floor(index * 0.5)).T
    low_lane = iota((batch, 128), 1) < 64
    lane_odd = jnp.where(low_lane, 0.0, 1.0)
    for pair in range(features // 2):
        cols = slice(128 * pair, 128 * (pair + 1))
        total = own_ref[:, cols]
        for piece_ref in (a_ref, b_ref, c_ref):
            total = total + piece_ref[:, cols].astype(F32)
        turned = pltpu.roll(total, 64, 1)
        for parity in range(2):
            f = 2 * pair + parity
            rows = jnp.where(low_lane, total, turned) if parity == 0 else jnp.where(low_lane, turned, total)
            rows = jnp.where(jnp.broadcast_to(odd[:, f : f + 1], (batch, 128)) == lane_odd, rows, 0.0)
            high = rows.astype(BF16)
            value_ref[batch * f : batch * (f + 1), 0:128] = high
            value_ref[batch * f : batch * (f + 1), 128:256] = (rows - high.astype(F32)).astype(BF16)
    block = 512
    each = block * 2 // capacity
    where = jnp.broadcast_to(at_ref[...], (block, features * batch))
    lines = iota((block, features * batch), 0).astype(F32)

    def part(m, square):
        hot = jnp.where(lines == where - (m * block).astype(F32), 1.0, 0.0).astype(BF16)
        both = dot_f32(hot, value_ref[...])
        sums = both[:, 0:128] + both[:, 128:256]
        first = pl.multiple_of(m * each, each)
        out_ref[pl.ds(first, each), 0 : capacity // 2, :] = sums.astype(BF16).reshape(each, capacity // 2, 128)
        return square + jnp.sum(jnp.sum(sums * sums, axis=1, keepdims=True), axis=0, keepdims=True)

    square = lax.fori_loop(0, owners // each, part, dense_ref[0:1, 0:1])
    top = square.astype(BF16).astype(F32)
    mid = (square - top).astype(BF16).astype(F32)
    end = square - top - mid
    ids = ids_ref[...]
    lane = iota((owners, 128 - 2 * capacity), 1)
    tail = jnp.where(lane == 0, top, jnp.where(lane == 1, mid, jnp.where(lane == 2, end, 0.0)))
    info = jnp.concatenate([(ids >> 8).astype(F32), (ids & 255).astype(F32), tail], axis=1)
    out_ref[:, capacity // 2 :, :] = jnp.broadcast_to(info[:, None, :], (owners, 8, 128)).astype(BF16)


def table_kernel(rate, eps, clip, arrived_ref, table_ref, accum_ref, table_out, accum_out, scale_out, acc_ref):
    sources, lines, _ = arrived_ref.shape
    half = lines - 8
    capacity = 2 * half
    rows = table_ref.shape[1]
    blocks = rows // 256
    every = sources * half
    info = arrived_ref[:, half:, :].reshape(sources * 8, 128)
    squares = jnp.sum(info.astype(F32)[:, 2 * capacity : 2 * capacity + 3], axis=0, keepdims=True)
    total = jnp.sum(squares, axis=1, keepdims=True) * 0.125
    scale = clip / jnp.maximum(jnp.sqrt(total), clip)
    scale_out[...] = jnp.broadcast_to(scale, scale_out.shape)
    share = jnp.where(iota((sources * 8, every), 0) >> 3 == iota((sources * 8, every), 1) // half, 0.125, 0.0)
    spread_info = dot_f32(info, share.astype(BF16), (((0,), (0,)), ((), ())))
    slot = iota((capacity, every), 0)
    line = iota((capacity, every), 1) & (half - 1)
    inside_at = iota((256, every), 0).astype(F32)
    turned = arrived_ref[:, :half, :].reshape(every, 128).astype(F32).T
    acc = None
    for parity in range(2):
        mine = slot == 2 * line + parity
        block = jnp.sum(jnp.where(mine, spread_info[0:capacity], 0.0), axis=0, keepdims=True)
        inside = jnp.sum(jnp.where(mine, spread_info[capacity : 2 * capacity], 0.0), axis=0, keepdims=True)
        piece = turned[64 * parity : 64 * (parity + 1), :]
        hot = jnp.where(inside_at == inside, 1.0, 0.0).astype(BF16)
        spread = jnp.concatenate([jnp.where(block == float(k), piece, 0.0).astype(BF16) for k in range(blocks)], axis=0)
        part = dot_f32(spread, hot, (((1,), (1,)), ((), ())))
        acc = part if acc is None else acc + part
    acc_ref[...] = acc
    for k in range(blocks):
        received = scale * acc_ref[64 * k : 64 * (k + 1), :]
        cols = slice(256 * k, 256 * (k + 1))
        accum = accum_ref[:, cols] + jnp.sum(received * received, axis=0, keepdims=True) * (1.0 / 64.0)
        accum_out[:, cols] = accum
        table_out[:, cols] = table_ref[:, cols] - rate * received / (jnp.sqrt(accum) + eps)


def footprint(shapes):
    return sum(math.prod(s.shape) * jnp.dtype(s.dtype).itemsize for s in shapes)


def call(kernel, outs, flops, args, scratch=(), spare=8):
    shapes = tuple(jax.ShapeDtypeStruct(s, t) for s, t in outs)
    held = footprint(args) + footprint(shapes) + footprint(scratch)
    res = pl.pallas_call(
        kernel,
        out_shape=shapes,
        in_specs=[VM] * len(args),
        out_specs=tuple(VM for _ in shapes),
        scratch_shapes=list(scratch),
        compiler_params=pltpu.CompilerParams(vmem_limit_bytes=held + spare * 2**20),
        cost_estimate=pl.CostEstimate(flops=flops, transcendentals=0, bytes_accessed=2 * 10**6),
    )(*args)
    return res


SHIFTS = (1, 3, 2)


def spot(axis, shift):
    return lax.rem(lax.axis_index(axis) + shift, 4)


def sigmoid(x):
    return 0.5 * jnp.tanh(0.5 * x) + 0.5


def forward_kernel(chunks, *refs):
    ins, (w_ref, bias_ref, out_w_ref) = refs[:chunks], refs[chunks : chunks + 3]
    slope_ref, hidden_ref, logit_ref, turned_ref = refs[chunks + 3 :]
    rows = ins[0].shape[0]
    width = w_ref.shape[1]
    for k in range(chunks):
        turned_ref[:, rows * k : rows * (k + 1)] = ins[k][...].T

    def columns(n, carry):
        cols = pl.ds(pl.multiple_of(n * 256, 256), 256)
        w = w_ref[:, cols]
        out_w = out_w_ref[:, cols].astype(F32)
        for k in range(chunks):
            act = dot_f32(ins[k][...], w) + bias_ref[:, cols]
            sigma = sigmoid(act)
            hidden_ref[rows * k : rows * (k + 1), cols] = (act * sigma).astype(BF16)
            slope_ref[rows * k : rows * (k + 1), cols] = out_w * sigma * (1.0 + act * (1.0 - sigma))
        return carry

    lax.fori_loop(0, width // 256, columns, 0)
    out_w = jnp.broadcast_to(out_w_ref[...], (16, width))
    for k in range(chunks):
        part = dot_f32(out_w, hidden_ref[rows * k : rows * (k + 1), :], (((1,), (1,)), ((), ())))
        at = rows * k
        logit_ref[at // 256 : at // 256 + 1, at % 256 : at % 256 + rows] = part[0:1, :]


def forward(chunks, w, bias, out_w):
    rows, depth = chunks[0].shape
    width = w.shape[1]
    n = len(chunks)
    total = n * rows
    outs = [((total, width), F32), ((total, width), BF16), ((total // 256, 256), F32), ((depth, total), BF16)]
    return call(functools.partial(forward_kernel, n), outs, total * 10**7, (*chunks, w, bias, out_w))


ORDER = (0, 3, 1, 2)
PARTNERS = ((0, 1, 2, 3), (2, 0, 3, 1), (1, 3, 0, 2), (3, 2, 1, 0))


def slope_kernel(*refs):
    slopes, hiddens = refs[0:3], refs[3:6]
    own_ref, prev_ref, next_ref, far_ref, labels_ref, weight_ref = refs[6:12]
    dact_ref, other_ref, sums_ref = refs[12:]
    rows, width = slopes[0].shape
    spans = ((0, 0), (1, 0), (1, rows), (2, 0))
    half = width // 2
    core = lax.axis_index("dp_2")
    dlogits = []
    for k in range(4):
        at = spot("mp", ORDER[k])
        logit = (own_ref[k : k + 1, :] + far_ref[PARTNERS[3][k] : PARTNERS[3][k] + 1, :]) + (
            prev_ref[PARTNERS[1][k] : PARTNERS[1][k] + 1, :] + next_ref[PARTNERS[2][k] : PARTNERS[2][k] + 1, :]
        )
        label = labels_ref[pl.ds(at, 1), :].astype(F32)
        dlogits.append(weight_ref[pl.ds(at, 1), :] * (sigmoid(logit) - label))
    rows_form = jnp.concatenate(dlogits + [jnp.zeros((4, rows), F32)], axis=0)
    cols_form = rows_form.T
    for k in range(4):
        which, start = spans[k]
        col = cols_form[:, k : k + 1]
        dact_ref[rows * k : rows * (k + 1), :] = (slopes[which][start : start + rows, :] * col).astype(BF16)
    other_ref[...] = dact_ref[:, pl.ds(pl.multiple_of((1 - core) * half, half), half)]
    ones = jnp.ones((16, rows), BF16)
    bias_sum = jnp.zeros((16, width), F32)
    out_sum = jnp.zeros((16, width), F32)
    for k in range(4):
        bias_sum = bias_sum + dot_f32(ones, dact_ref[rows * k : rows * (k + 1), :])
        d = dlogits[k]
        top = d.astype(BF16)
        rest = (d - top.astype(F32)).astype(BF16)
        pick = iota((16, rows), 0)
        left = jnp.where(pick == 0, top.astype(F32), jnp.where(pick == 1, rest.astype(F32), 0.0)).astype(BF16)
        which, start = spans[k]
        out_sum = out_sum + dot_f32(left, hiddens[which][start : start + rows, :])
    total = jnp.sum(out_sum, axis=0, keepdims=True)
    sums_ref[...] = jnp.concatenate([bias_sum[0:1, :], total], axis=0)


def back_kernel(dact_ref, w_ref, own_ref, *outs):
    rows = own_ref.shape[0]
    for k, target in enumerate((own_ref, *outs)):
        part = dot_f32(dact_ref[rows * k : rows * (k + 1), :], w_ref[...], (((1,), (1,)), ((), ())))
        target[...] = part.astype(target.dtype)


def spot_on(first, core, shift):
    x, y = lax.axis_index("dp_0"), lax.axis_index("dp_1")
    along = x * (1 - core) + y * core if first else y * (1 - core) + x * core
    return lax.rem(along + shift, 4)


def chip_rows(core, outer, inner, size):
    return pl.multiple_of((outer * (4 - 3 * core) + inner * (1 + 3 * core)) * size, size)


def grad_kernel(*refs):
    turned, (dact_ref, far_dact_ref) = refs[0:6], refs[6:8]
    outs, acc_ref = refs[8:12], refs[12]
    depth = turned[0].shape[0]
    half = far_dact_ref.shape[1]
    spans = ((0, 256), (256, 512), (768, 256))
    core = lax.axis_index("dp_2")
    local = pl.ds(pl.multiple_of(core * half, half), half)

    def rows(x, carry):
        at = pl.ds(pl.multiple_of(x * 256, 256), 256)
        part = None
        for i, (s, n) in enumerate(spans):
            p = dot_f32(turned[i][at, :], dact_ref[s : s + n, local])
            p = p + dot_f32(turned[i + 3][at, :], far_dact_ref[s : s + n, :])
            part = p if part is None else part + p
        acc_ref[at, :] = part
        return carry

    lax.fori_loop(0, depth // 256, rows, 0)
    size = depth // 16
    for target, shift in zip(outs, (0, *SHIFTS)):
        for t in range(4):
            at = chip_rows(core, spot_on(True, core, shift), t, size)
            target[size * t : size * (t + 1), :] = acc_ref[pl.ds(at, size), :].astype(target.dtype)


def middle_kernel(own_ref, a_ref, b_ref, c_ref, *refs):
    outs, acc_ref = refs[:4], refs[4]
    size = outs[0].shape[0]
    core = lax.axis_index("dp_2")
    acc_ref[...] = own_ref[...] + a_ref[...].astype(F32) + b_ref[...].astype(F32) + c_ref[...].astype(F32)
    for target, shift in zip(outs, (0, *SHIFTS)):
        at = pl.multiple_of(spot_on(False, core, shift) * size, size)
        target[...] = acc_ref[pl.ds(at, size), :].astype(target.dtype)


def last_kernel(own_ref, a_ref, b_ref, c_ref, sums_ref, narrow_ref, mine_ref, other_ref, square_ref, full_ref):
    core = lax.axis_index("dp_2")
    total = own_ref[...] + a_ref[...].astype(F32) + b_ref[...].astype(F32) + c_ref[...].astype(F32)
    extra = jnp.sum(sums_ref[...], axis=0, keepdims=True)
    square = jnp.sum(jnp.sum(total * total, axis=1, keepdims=True), axis=0, keepdims=True)
    square = square + jnp.sum(extra * extra, axis=1, keepdims=True)
    square_ref[...] = jnp.broadcast_to(square, square_ref.shape)
    full_ref[...] = total
    narrow_ref[...] = total.astype(BF16)
    per = total.shape[0] // 2
    mine_ref[...] = full_ref[pl.ds(pl.multiple_of(core * per, per), per), :]
    other_ref[...] = full_ref[pl.ds(pl.multiple_of((1 - core) * per, per), per), :]


def pack_kernel(*refs):
    rows = refs[0].shape[0]
    for k in range(4):
        refs[4][rows * k : rows * (k + 1), :] = refs[k][...]


def weight_kernel(scale_ref, w_ref, near_ref, far_ref, rows_ref, mine_ref, theirs_ref, *refs):
    stacks, (w_out_ref, accum_ref) = refs[:8], refs[8:]
    core = lax.axis_index("dp_2")
    scale = scale_ref[0:1, 0:1]
    _, per, _ = near_ref.shape
    half = stacks[0].shape[1]
    for side, c in ((0, core), (1, 1 - core)):
        cols = pl.ds(pl.multiple_of(c * half, half), half)
        for i in range(4):
            outer = spot_on(True, c, (4 - i) % 4)

            def chip(j, carry, stack=stacks[4 * side + i], outer=outer, c=c, cols=cols):
                inner = spot_on(False, c, lax.rem(4 - j, 4))
                at = chip_rows(c, outer, inner, 1)
                for held_ref, r in ((near_ref, core), (far_ref, 1 - core)):
                    rows = pl.ds(pl.multiple_of((at * 2 + r) * per, per), per)
                    grad = scale * stack[pl.ds(pl.multiple_of((j * 2 + r) * per, per), per), :].astype(F32)
                    accum = held_ref[at, :, cols].astype(F32) + grad * grad
                    w = w_ref[rows, cols].astype(F32)
                    w_out_ref[rows, cols] = (w - dense_rate * grad / (jnp.sqrt(accum) + adagrad_eps)).astype(BF16)
                return carry

            lax.fori_loop(0, 4, chip, 0)
        grad = scale * (mine_ref, theirs_ref)[side][...]
        accum_ref[:, cols] = rows_ref[:, cols] + grad * grad


def cross(x, first, shift):
    moves = []
    for i in range(32):
        a, b, c = i // 8, i // 2 % 4, i % 2
        a, b = ((a + shift) % 4, b) if (c == 0) == first else (a, (b + shift) % 4)
        moves.append((i, a * 8 + b * 2 + c))
    return lax.ppermute(x, DP, moves)


def send(x, axis, shift):
    n = lax.axis_size(axis)
    return lax.ppermute(x, axis, [(i, (i + shift) % n) for i in range(n)])


def around(x, axis):
    return [send(x, axis, s) for s in SHIFTS]


def inner(
    slab_values,
    row_ids,
    peer_counts,
    lookup_slots,
    labels,
    sample_weight,
    weight_in,
    bias_in,
    weight_out,
    dense_accum,
    table_rows,
    table_accum,
):
    batch, features = lookup_slots.shape
    depth, width = weight_in.shape
    half = width // 2
    lookups_t = lookup_slots.T
    pooled = gather_rows(peer_counts, lookups_t, slab_values[0])
    before, after = send(pooled, "mp", 1), send(pooled, "mp", 3)
    chips = ("dp_0", "dp_1")
    narrow = dense_accum.astype(BF16)
    near = lax.all_to_all(jnp.broadcast_to(narrow[None], (16, *narrow.shape)), chips, 0, 0, tiled=True)
    distant = send(near, "dp_2", 1)
    bias = bias_in.reshape(1, width)
    out_w = weight_out.reshape(1, width)
    far_low, far_high = send(before[: batch // 2], "mp", 1), send(after[batch // 2 :], "mp", 3)
    slope_0, hidden_0, logit_0, turned_0 = forward([pooled], weight_in, bias, out_w)
    slope_1, hidden_1, logit_1, turned_1 = forward([before, after], weight_in, bias, out_w)
    slope_2, hidden_2, logit_2, turned_2 = forward([far_low, far_high], weight_in, bias, out_w)
    turned = [turned_0, turned_1, turned_2]
    turned = turned + [send(t, "dp_2", 1) for t in turned]
    logits = jnp.concatenate([logit_0, logit_1, logit_2], axis=0)
    logit_before, logit_after, logit_far = around(logits, "mp")
    dact, other, sums = call(
        slope_kernel,
        [((4 * batch, width), BF16), ((4 * batch, half), BF16), ((2, width), F32)],
        2 * 10**9,
        (
            slope_0,
            slope_1,
            slope_2,
            hidden_0,
            hidden_1,
            hidden_2,
            logits,
            logit_before,
            logit_after,
            logit_far,
            labels.reshape(4, batch),
            sample_weight.reshape(4, batch),
        ),
    )
    far_dact = send(other, "dp_2", 1)
    own, to_before, to_after, to_far = call(
        back_kernel, [((batch, depth), F32)] + [((batch, depth), BF16)] * 3, 4 * 10**9, (dact, weight_in)
    )
    from_after, from_before, from_far = send(to_before, "mp", 3), send(to_after, "mp", 1), send(to_far, "mp", 2)
    stage = [((depth // 4, half), F32)] + [((depth // 4, half), BF16)] * 3
    keep, *give = call(grad_kernel, stage, 8 * 10**9, (*turned, dact, far_dact), [pltpu.VMEM((depth, half), F32)])
    got = [cross(g, True, s) for g, s in zip(give, SHIFTS)]
    stage = [((depth // 16, half), F32)] + [((depth // 16, half), BF16)] * 3
    keep, *give = call(middle_kernel, stage, 10**8, (keep, *got), [pltpu.VMEM((depth // 4, half), F32)])
    got = [cross(g, False, s) for g, s in zip(give, SHIFTS)]
    sums = lax.all_to_all(sums.reshape(32, 1, 2 * width // 32), DP, 0, 0, tiled=True).reshape(32, -1)
    narrow, mine, others, square = call(
        last_kernel,
        [((depth // 16, half), BF16)] + [((depth // 32, half), F32)] * 2 + [((8, 128), F32)],
        10**8,
        (keep, *got, sums),
        [pltpu.VMEM((depth // 16, half), F32)],
    )
    theirs = send(others, "dp_2", 1)
    parts = {s: cross(narrow, False, s) for s in SHIFTS}
    pack = call(pack_kernel, [((depth // 4, half), BF16)], 10**8, (narrow, parts[1], parts[2], parts[3]))[0]
    stacks = {s: cross(pack, True, s) for s in SHIFTS}
    stacks = [pack, stacks[1], stacks[2], stacks[3]]
    stacks = stacks + [send(g, "dp_2", 1) for g in stacks]
    peers, capacity = row_ids.shape[1:]
    outgoing = call(
        slot_kernel,
        [((peers, capacity // 2 + 8, 128), BF16)],
        8 * 10**9,
        (peer_counts, lookups_t, row_ids[0], own, from_before, from_after, from_far, square),
        [pltpu.VMEM((features * batch, 256), BF16), pltpu.VMEM((1, features * batch), F32)],
        24,
    )[0]
    arrived = lax.all_to_all(outgoing, DP_MP, 0, 0, tiled=True)
    table_t, accum_t, scale = call(
        functools.partial(table_kernel, table_rate, adagrad_eps, clip_norm),
        [(table_rows.shape[::-1], F32), ((1, table_rows.shape[0]), F32), ((8, 128), F32)],
        6 * 10**9,
        (arrived, table_rows.T, table_accum.reshape(1, -1)),
        [pltpu.VMEM((table_rows.shape[0] // 4, 256), F32)],
        32,
    )
    weight_new, accum_new = call(
        weight_kernel,
        [((depth, width), BF16), (dense_accum.shape, F32)],
        10**9,
        (scale, weight_in, near, distant, dense_accum, mine, theirs, *stacks),
    )
    return (weight_new, accum_new, table_t.T, accum_t.reshape(-1))


def solution(mesh):
    torus = Mesh(mesh.devices.reshape(4, 4, 2, mesh.shape["mp"]), ("dp_0", "dp_1", "dp_2", "mp"))
    placed = (
        P(DP_MP, None, None),
        P(DP_MP, None, None),
        P(DP_MP, None),
        P(DP_MP, None),
        P(DP),
        P(DP),
        P(None, "mp"),
        P("mp"),
        P("mp"),
        P(DP, "mp"),
        P(DP_MP, None),
        P(DP_MP),
    )
    return jax.shard_map(
        inner,
        mesh=torus,
        in_specs=placed,
        out_specs=(P(None, "mp"), P(DP, "mp"), P(DP_MP, None), P(DP_MP)),
        check_vma=False,
    )
```

```python
import functools
import math

import jax
import jax.numpy as jnp
from jax import lax
from jax.experimental import pallas as pl
from jax.experimental.pallas import tpu as pltpu
from jax.sharding import Mesh
from jax.sharding import PartitionSpec as P


DP = ("dp_0", "dp_1", "dp_2")
DP_MP = ("dp_0", "dp_1", "dp_2", "mp")

clip_norm = 1.0
dense_rate = 0.02
table_rate = 0.5
adagrad_eps = 1e-10

F32 = jnp.float32
BF16 = jnp.bfloat16
VM = pl.BlockSpec(memory_space=pltpu.VMEM)


def iota(shape, dim):
    return lax.broadcasted_iota(jnp.int32, shape, dim)


def dot_f32(a, b, dims=(((1,), (0,)), ((), ()))):
    return lax.dot_general(a, b, dims, preferred_element_type=F32)


def hot_rows(counts_ref, lookups_ref):
    owners = counts_ref.shape[1]
    features = lookups_ref.shape[0]
    spread = jnp.broadcast_to(counts_ref[...].astype(F32), (owners, owners))
    at, of = iota((owners, owners), 0), iota((owners, owners), 1)
    ends = jnp.sum(jnp.where(of <= at, spread, 0.0), axis=1, keepdims=True)
    starts = ends - jnp.sum(jnp.where(of == at, spread, 0.0), axis=1, keepdims=True)
    hots, slots = [], []
    for f in range(features):
        q = lookups_ref[f : f + 1, :].astype(F32)
        match = (q >= starts) & (q < ends)
        hots.append(jnp.where(match, 1.0, 0.0))
        slots.append(q - jnp.sum(jnp.where(match, starts, 0.0), axis=0, keepdims=True))
    return hots, slots


def gather_kernel(counts_ref, lookups_ref, slab_ref, out_ref):
    features, batch = lookups_ref.shape
    halfway = slab_ref.shape[1] // 2
    hots, slots = hot_rows(counts_ref, lookups_ref)
    inner = jnp.concatenate([jnp.where(s >= 16.0, s - 16.0, s) for s in slots], axis=0).T
    halves = jnp.concatenate([slab_ref[:, :halfway], slab_ref[:, halfway:]], axis=0)
    low_lane = iota((batch, 128), 1) < 64
    for pair in range(features // 2):
        both = []
        for parity in range(2):
            f = 2 * pair + parity
            upper = slots[f] >= 16.0
            hot = jnp.concatenate(
                [jnp.where(upper, 0.0, hots[f]), jnp.where(upper, hots[f], 0.0)], axis=0
            ).astype(BF16)
            rows = dot_f32(hot, halves, (((0,), (0,)), ((), ())))
            place = jnp.broadcast_to(inner[:, f : f + 1], (batch, 128))
            block = jnp.floor(place * 0.5)
            found = rows[:, :128]
            for k in range(1, 8):
                found = jnp.where(block == float(k), rows[:, 128 * k : 128 * (k + 1)], found)
            swap = place - 2.0 * block != float(parity)
            both.append(jnp.where(swap, pltpu.roll(found, 64, 1), found))
        out_ref[:, 128 * pair : 128 * (pair + 1)] = jnp.where(low_lane, both[0], both[1]).astype(BF16)


def gather_rows(counts, lookups_t, slab):
    features, batch = lookups_t.shape
    return pl.pallas_call(
        gather_kernel,
        out_shape=jax.ShapeDtypeStruct((batch, features * 64), BF16),
        in_specs=[VM, VM, VM],
        out_specs=VM,
        name="gather_rows",
        compiler_params=pltpu.CompilerParams(vmem_limit_bytes=16 * 2**20),
        cost_estimate=pl.CostEstimate(flops=6 * 10**9, transcendentals=0, bytes_accessed=2 * 10**6),
    )(counts, lookups_t, slab)


def slot_kernel(
    capacity, counts_ref, lookups_ref, own_ref, a_ref, b_ref, c_ref, out_ref, square_ref, value_ref, at_ref
):
    owners = counts_ref.shape[1]
    features, batch = lookups_ref.shape
    spread = jnp.broadcast_to(counts_ref[...].astype(F32), (owners, owners))
    at, of = iota((owners, owners), 0), iota((owners, owners), 1)
    ends = jnp.sum(jnp.where(of <= at, spread, 0.0), axis=1, keepdims=True)
    starts = ends - jnp.sum(jnp.where(of == at, spread, 0.0), axis=1, keepdims=True)
    moves = iota((owners, 1), 0).astype(F32) * float(capacity) - starts
    indices = []
    for f in range(features):
        q = lookups_ref[f : f + 1, :].astype(F32)
        match = (q >= starts) & (q < ends)
        indices.append(q + jnp.sum(jnp.where(match, moves, 0.0), axis=0, keepdims=True))
        at_ref[0:1, batch * f : batch * (f + 1)] = jnp.floor(indices[f] * 0.5)
    index = jnp.concatenate(indices, axis=0)
    odd = (index - 2.0 * jnp.floor(index * 0.5)).T
    low_lane = iota((batch, 128), 1) < 64
    lane_odd = jnp.where(low_lane, 0.0, 1.0)
    for pair in range(features // 2):
        cols = slice(128 * pair, 128 * (pair + 1))
        total = own_ref[:, cols]
        for piece_ref in (a_ref, b_ref, c_ref):
            total = total + piece_ref[:, cols].astype(F32)
        turned = pltpu.roll(total, 64, 1)
        for parity in range(2):
            f = 2 * pair + parity
            rows = jnp.where(low_lane, total, turned) if parity == 0 else jnp.where(low_lane, turned, total)
            rows = jnp.where(jnp.broadcast_to(odd[:, f : f + 1], (batch, 128)) == lane_odd, rows, 0.0)
            high = rows.astype(BF16)
            value_ref[batch * f : batch * (f + 1), 0:128] = high
            value_ref[batch * f : batch * (f + 1), 128:256] = (rows - high.astype(F32)).astype(BF16)
    block = 512
    each = block * 2 // capacity
    where = jnp.broadcast_to(at_ref[...], (block, features * batch))
    lines = iota((block, features * batch), 0).astype(F32)

    def part(m, square):
        hot = jnp.where(lines == where - (m * block).astype(F32), 1.0, 0.0).astype(BF16)
        both = dot_f32(hot, value_ref[...])
        sums = both[:, 0:128] + both[:, 128:256]
        first = pl.multiple_of(m * each, each)
        out_ref[pl.ds(first, each), :, :] = sums.astype(BF16).reshape(each, capacity // 2, 128)
        return square + jnp.sum(jnp.sum(sums * sums, axis=1, keepdims=True), axis=0, keepdims=True)

    square = lax.fori_loop(0, owners // each, part, jnp.zeros((1, 1), F32))
    square_ref[...] = jnp.broadcast_to(square, square_ref.shape)


def stamp_kernel(sums_ref, ids_ref, slot_square_ref, dense_square_ref, extra_ref, out_ref):
    owners, capacity = ids_ref.shape
    half = capacity // 2
    extra = jnp.sum(extra_ref[...], axis=0, keepdims=True)
    square = slot_square_ref[0:1, 0:1] + dense_square_ref[0:1, 0:1] + jnp.sum(extra * extra, axis=1, keepdims=True)
    top = square.astype(BF16).astype(F32)
    mid = (square - top).astype(BF16).astype(F32)
    end = square - top - mid
    ids = ids_ref[...]
    lane = iota((owners, 128 - 2 * capacity), 1)
    tail = jnp.where(lane == 0, top, jnp.where(lane == 1, mid, jnp.where(lane == 2, end, 0.0)))
    info = jnp.concatenate([(ids >> 8).astype(F32), (ids & 255).astype(F32), tail], axis=1)
    out_ref[:, :half, :] = sums_ref[...]
    out_ref[:, half:, :] = jnp.broadcast_to(info[:, None, :], (owners, 8, 128)).astype(BF16)


def table_kernel(rate, eps, clip, arrived_ref, table_ref, accum_ref, table_out, accum_out, scale_out, acc_ref):
    sources, lines, _ = arrived_ref.shape
    half = lines - 8
    capacity = 2 * half
    rows = table_ref.shape[1]
    blocks = rows // 256
    every = sources * half
    info = arrived_ref[:, half:, :].reshape(sources * 8, 128)
    squares = jnp.sum(info.astype(F32)[:, 2 * capacity : 2 * capacity + 3], axis=0, keepdims=True)
    total = jnp.sum(squares, axis=1, keepdims=True) * 0.125
    scale = clip / jnp.maximum(jnp.sqrt(total), clip)
    scale_out[...] = jnp.broadcast_to(scale, scale_out.shape)
    share = jnp.where(iota((sources * 8, every), 0) >> 3 == iota((sources * 8, every), 1) // half, 0.125, 0.0)
    spread_info = dot_f32(info, share.astype(BF16), (((0,), (0,)), ((), ())))
    slot = iota((capacity, every), 0)
    line = iota((capacity, every), 1) & (half - 1)
    inside_at = iota((256, every), 0).astype(F32)
    turned = arrived_ref[:, :half, :].reshape(every, 128).astype(F32).T
    acc = None
    for parity in range(2):
        mine = slot == 2 * line + parity
        block = jnp.sum(jnp.where(mine, spread_info[0:capacity], 0.0), axis=0, keepdims=True)
        inside = jnp.sum(jnp.where(mine, spread_info[capacity : 2 * capacity], 0.0), axis=0, keepdims=True)
        piece = turned[64 * parity : 64 * (parity + 1), :]
        hot = jnp.where(inside_at == inside, 1.0, 0.0).astype(BF16)
        spread = jnp.concatenate([jnp.where(block == float(k), piece, 0.0).astype(BF16) for k in range(blocks)], axis=0)
        part = dot_f32(spread, hot, (((1,), (1,)), ((), ())))
        acc = part if acc is None else acc + part
    acc_ref[...] = acc
    for k in range(blocks):
        received = scale * acc_ref[64 * k : 64 * (k + 1), :]
        cols = slice(256 * k, 256 * (k + 1))
        accum = accum_ref[:, cols] + jnp.sum(received * received, axis=0, keepdims=True) * (1.0 / 64.0)
        accum_out[:, cols] = accum
        table_out[:, cols] = table_ref[:, cols] - rate * received / (jnp.sqrt(accum) + eps)


def footprint(shapes):
    return sum(math.prod(s.shape) * jnp.dtype(s.dtype).itemsize for s in shapes)


def call(kernel, outs, flops, args, scratch=(), spare=8):
    shapes = tuple(jax.ShapeDtypeStruct(s, t) for s, t in outs)
    return pl.pallas_call(
        kernel,
        out_shape=shapes,
        in_specs=[VM] * len(args),
        out_specs=tuple(VM for _ in shapes),
        scratch_shapes=list(scratch),
        compiler_params=pltpu.CompilerParams(vmem_limit_bytes=footprint(scratch) + spare * 2**20),
        cost_estimate=pl.CostEstimate(flops=flops, transcendentals=0, bytes_accessed=2 * 10**6),
    )(*args)


SHIFTS = (1, 3, 2)


def spot(axis, shift):
    return lax.rem(lax.axis_index(axis) + shift, 4)


def sigmoid(x):
    return 0.5 * jnp.tanh(0.5 * x) + 0.5


def forward_kernel(chunks, *refs):
    ins, (w_ref, bias_ref, out_w_ref) = refs[:chunks], refs[chunks : chunks + 3]
    slope_ref, hidden_ref, logit_ref, turned_ref, rows_ref = refs[chunks + 3 :]
    rows = ins[0].shape[0]
    width = w_ref.shape[1]
    for k in range(chunks):
        rows_ref[rows * k : rows * (k + 1), :] = ins[k][...]
        turned_ref[:, rows * k : rows * (k + 1)] = ins[k][...].T

    def columns(n, carry):
        cols = pl.ds(pl.multiple_of(n * 256, 256), 256)
        act = dot_f32(rows_ref[...], w_ref[:, cols]) + bias_ref[:, cols]
        sigma = sigmoid(act)
        hidden_ref[:, cols] = (act * sigma).astype(BF16)
        slope_ref[:, cols] = out_w_ref[:, cols].astype(F32) * sigma * (1.0 + act * (1.0 - sigma))
        return carry

    lax.fori_loop(0, width // 256, columns, 0)
    out_w = jnp.broadcast_to(out_w_ref[...], (16, width))
    for k in range(logit_ref.shape[0]):
        part = dot_f32(out_w, hidden_ref[256 * k : 256 * (k + 1), :], (((1,), (1,)), ((), ())))
        logit_ref[k : k + 1, :] = part[0:1, :]


def forward(chunks, w, bias, out_w):
    rows, depth = chunks[0].shape
    width = w.shape[1]
    n = len(chunks)
    total = n * rows
    outs = [((total, width), F32), ((total, width), BF16), ((total // 256, 256), F32), ((depth, total), BF16)]
    return call(
        functools.partial(forward_kernel, n),
        outs,
        total * 10**7,
        (*chunks, w, bias, out_w),
        [pltpu.VMEM((total, depth), BF16)],
    )


ORDER = (0, 3, 1, 2)
PARTNERS = ((0, 1, 2, 3), (2, 0, 3, 1), (1, 3, 0, 2), (3, 2, 1, 0))


def slope_kernel(*refs):
    slopes, hiddens = refs[0:3], refs[3:6]
    own_ref, prev_ref, next_ref, far_ref, labels_ref, weight_ref = refs[6:12]
    dact_ref, other_ref, sums_ref = refs[12:]
    rows, width = slopes[0].shape
    spans = ((0, 0), (1, 0), (1, rows), (2, 0))
    half = width // 2
    core = lax.axis_index("dp_2")
    dlogits = []
    for k in range(4):
        at = spot("mp", ORDER[k])
        logit = (own_ref[k : k + 1, :] + far_ref[PARTNERS[3][k] : PARTNERS[3][k] + 1, :]) + (
            prev_ref[PARTNERS[1][k] : PARTNERS[1][k] + 1, :] + next_ref[PARTNERS[2][k] : PARTNERS[2][k] + 1, :]
        )
        here = pl.ds(pl.multiple_of(at * rows, rows), rows)
        label = labels_ref[:, here].astype(F32)
        dlogits.append(weight_ref[:, here] * (sigmoid(logit) - label))
    rows_form = jnp.concatenate(dlogits + [jnp.zeros((4, rows), F32)], axis=0)
    cols_form = rows_form.T
    for k in range(4):
        which, start = spans[k]
        col = cols_form[:, k : k + 1]
        dact_ref[rows * k : rows * (k + 1), :] = (slopes[which][start : start + rows, :] * col).astype(BF16)
    other_ref[...] = dact_ref[:, pl.ds(pl.multiple_of((1 - core) * half, half), half)]
    ones = jnp.ones((16, rows), BF16)
    bias_sum = jnp.zeros((16, width), F32)
    out_sum = jnp.zeros((16, width), F32)
    for k in range(4):
        bias_sum = bias_sum + dot_f32(ones, dact_ref[rows * k : rows * (k + 1), :])
        d = dlogits[k]
        top = d.astype(BF16)
        rest = (d - top.astype(F32)).astype(BF16)
        pick = iota((16, rows), 0)
        left = jnp.where(pick == 0, top.astype(F32), jnp.where(pick == 1, rest.astype(F32), 0.0)).astype(BF16)
        which, start = spans[k]
        out_sum = out_sum + dot_f32(left, hiddens[which][start : start + rows, :])
    total = jnp.sum(out_sum, axis=0, keepdims=True)
    sums_ref[...] = jnp.concatenate([bias_sum[0:1, :], total], axis=0)


def back_kernel(dact_ref, w_ref, own_ref, *outs):
    rows = own_ref.shape[0]
    for k, target in enumerate((own_ref, *outs)):
        part = dot_f32(dact_ref[rows * k : rows * (k + 1), :], w_ref[...], (((1,), (1,)), ((), ())))
        target[...] = part.astype(target.dtype)


def spot_on(first, core, shift):
    x, y = lax.axis_index("dp_0"), lax.axis_index("dp_1")
    along = x * (1 - core) + y * core if first else y * (1 - core) + x * core
    return lax.rem(along + shift, 4)


def chip_rows(core, outer, inner, size):
    return pl.multiple_of((outer * (4 - 3 * core) + inner * (1 + 3 * core)) * size, size)


def grad_kernel(*refs):
    turned, (dact_ref, far_dact_ref) = refs[0:6], refs[6:8]
    outs, acc_ref = refs[8:12], refs[12]
    depth = turned[0].shape[0]
    half = far_dact_ref.shape[1]
    spans = ((0, 256), (256, 512), (768, 256))
    core = lax.axis_index("dp_2")
    local = pl.ds(pl.multiple_of(core * half, half), half)

    def rows(x, carry):
        at = pl.ds(pl.multiple_of(x * 256, 256), 256)
        part = None
        for i, (s, n) in enumerate(spans):
            p = dot_f32(turned[i][at, :], dact_ref[s : s + n, local])
            p = p + dot_f32(turned[i + 3][at, :], far_dact_ref[s : s + n, :])
            part = p if part is None else part + p
        acc_ref[at, :] = part
        return carry

    lax.fori_loop(0, depth // 256, rows, 0)
    size = depth // 16
    for target, shift in zip(outs, (0, *SHIFTS)):
        for t in range(4):
            at = chip_rows(core, spot_on(True, core, shift), t, size)
            target[size * t : size * (t + 1), :] = acc_ref[pl.ds(at, size), :].astype(target.dtype)


def middle_kernel(own_ref, a_ref, b_ref, c_ref, *refs):
    outs, acc_ref = refs[:4], refs[4]
    size = outs[0].shape[0]
    core = lax.axis_index("dp_2")
    acc_ref[...] = own_ref[...] + a_ref[...].astype(F32) + b_ref[...].astype(F32) + c_ref[...].astype(F32)
    for target, shift in zip(outs, (0, *SHIFTS)):
        at = pl.multiple_of(spot_on(False, core, shift) * size, size)
        target[...] = acc_ref[pl.ds(at, size), :].astype(target.dtype)


def last_kernel(own_ref, a_ref, b_ref, c_ref, narrow_ref, mine_ref, other_ref, square_ref, full_ref):
    core = lax.axis_index("dp_2")
    total = own_ref[...] + a_ref[...].astype(F32) + b_ref[...].astype(F32) + c_ref[...].astype(F32)
    square = jnp.sum(jnp.sum(total * total, axis=1, keepdims=True), axis=0, keepdims=True)
    square_ref[...] = jnp.broadcast_to(square, square_ref.shape)
    full_ref[...] = total
    narrow_ref[...] = total.astype(BF16)
    per = total.shape[0] // 2
    mine_ref[...] = full_ref[pl.ds(pl.multiple_of(core * per, per), per), :]
    other_ref[...] = full_ref[pl.ds(pl.multiple_of((1 - core) * per, per), per), :]


def pack_kernel(*refs):
    rows = refs[0].shape[0]
    for k in range(4):
        refs[4][rows * k : rows * (k + 1), :] = refs[k][...]


def merge_kernel(*refs):
    stacks, out_ref = refs[:8], refs[8]
    core = lax.axis_index("dp_2")
    per = stacks[0].shape[0] // 4
    for side, c in ((0, core), (1, 1 - core)):
        for i in range(4):
            for j in range(4):
                at = chip_rows(c, spot_on(True, c, (4 - i) % 4), spot_on(False, c, (4 - j) % 4), 1)
                rows = pl.ds(pl.multiple_of((at * 2 + c) * per, per), per)
                out_ref[rows, :] = stacks[4 * side + i][per * j : per * (j + 1), :]


def weight_kernel(scale_ref, w_ref, held_ref, rows_ref, mine_ref, theirs_ref, *refs):
    stacks, (w_out_ref, accum_ref) = refs[:8], refs[8:]
    core = lax.axis_index("dp_2")
    scale = scale_ref[0:1, 0:1]
    half = stacks[0].shape[1]
    size = stacks[0].shape[0] // 4
    for side, c in ((0, core), (1, 1 - core)):
        cols = pl.ds(pl.multiple_of(c * half, half), half)
        for i in range(4):
            outer = spot_on(True, c, (4 - i) % 4)

            def chip(j, carry, stack=stacks[4 * side + i], outer=outer, c=c, cols=cols):
                inner = spot_on(False, c, lax.rem(4 - j, 4))
                rows = pl.ds(chip_rows(c, outer, inner, size), size)
                grad = scale * stack[pl.ds(pl.multiple_of(j * size, size), size), :].astype(F32)
                accum = held_ref[rows, cols].astype(F32) + grad * grad
                w = w_ref[rows, cols].astype(F32)
                w_out_ref[rows, cols] = (w - dense_rate * grad / (jnp.sqrt(accum) + adagrad_eps)).astype(BF16)
                return carry

            lax.fori_loop(0, 4, chip, 0)
        grad = scale * (mine_ref, theirs_ref)[side][...]
        accum_ref[:, cols] = rows_ref[:, cols] + grad * grad


def cross(x, first, shift):
    moves = []
    for i in range(32):
        a, b, c = i // 8, i // 2 % 4, i % 2
        a, b = ((a + shift) % 4, b) if (c == 0) == first else (a, (b + shift) % 4)
        moves.append((i, a * 8 + b * 2 + c))
    return lax.ppermute(x, DP, moves)


def send(x, axis, shift):
    n = lax.axis_size(axis)
    return lax.ppermute(x, axis, [(i, (i + shift) % n) for i in range(n)])


def around(x, axis):
    return [send(x, axis, s) for s in SHIFTS]


def inner(
    slab_values,
    row_ids,
    peer_counts,
    lookup_slots,
    labels,
    sample_weight,
    weight_in,
    bias_in,
    weight_out,
    dense_accum,
    table_rows,
    table_accum,
):
    batch, features = lookup_slots.shape
    depth, width = weight_in.shape
    half = width // 2
    lookups_t = lookup_slots.T
    pooled = gather_rows(peer_counts, lookups_t, slab_values[0])
    before, after = send(pooled, "mp", 1), send(pooled, "mp", 3)
    narrow = dense_accum.astype(BF16)
    parts = {s: cross(narrow, False, s) for s in SHIFTS}
    block = (depth // 8, width)
    near = call(pack_kernel, [(block, BF16)], 10**8, (narrow, parts[1], parts[2], parts[3]))[0]
    stacks = {s: cross(near, True, s) for s in SHIFTS}
    stacks = [near, stacks[1], stacks[2], stacks[3]]
    stacks = stacks + [send(g, "dp_2", 1) for g in stacks]
    accum_full = call(merge_kernel, [((depth, width), BF16)], 10**8, stacks)[0]
    bias = bias_in.reshape(1, width)
    out_w = weight_out.reshape(1, width)
    far_low, far_high = send(before[: batch // 2], "mp", 1), send(after[batch // 2 :], "mp", 3)
    slope_0, hidden_0, logit_0, turned_0 = forward([pooled], weight_in, bias, out_w)
    slope_1, hidden_1, logit_1, turned_1 = forward([before, after], weight_in, bias, out_w)
    slope_2, hidden_2, logit_2, turned_2 = forward([far_low, far_high], weight_in, bias, out_w)
    turned = [turned_0, turned_1, turned_2]
    turned = turned + [send(t, "dp_2", 1) for t in turned]
    logits = jnp.concatenate([logit_0, logit_1, logit_2], axis=0)
    logit_before, logit_after, logit_far = around(logits, "mp")
    dact, other, sums = call(
        slope_kernel,
        [((4 * batch, width), BF16), ((4 * batch, half), BF16), ((2, width), F32)],
        2 * 10**9,
        (
            slope_0,
            slope_1,
            slope_2,
            hidden_0,
            hidden_1,
            hidden_2,
            logits,
            logit_before,
            logit_after,
            logit_far,
            labels.reshape(1, -1),
            sample_weight.reshape(1, -1),
        ),
    )
    far_dact = send(other, "dp_2", 1)
    own, to_before, to_after, to_far = call(
        back_kernel, [((batch, depth), F32)] + [((batch, depth), BF16)] * 3, 4 * 10**9, (dact, weight_in)
    )
    from_after, from_before, from_far = send(to_before, "mp", 3), send(to_after, "mp", 1), send(to_far, "mp", 2)
    stage = [((depth // 4, half), F32)] + [((depth // 4, half), BF16)] * 3
    keep, *give = call(grad_kernel, stage, 8 * 10**9, (*turned, dact, far_dact), [pltpu.VMEM((depth, half), F32)])
    got = [cross(g, True, s) for g, s in zip(give, SHIFTS)]
    stage = [((depth // 16, half), F32)] + [((depth // 16, half), BF16)] * 3
    keep, *give = call(middle_kernel, stage, 10**8, (keep, *got), [pltpu.VMEM((depth // 4, half), F32)])
    got = [cross(g, False, s) for g, s in zip(give, SHIFTS)]
    sums = lax.all_to_all(sums.reshape(32, 1, 2 * width // 32), DP, 0, 0, tiled=True).reshape(32, -1)
    narrow, mine, others, square = call(
        last_kernel,
        [((depth // 16, half), BF16)] + [((depth // 32, half), F32)] * 2 + [((8, 128), F32)],
        10**8,
        (keep, *got),
        [pltpu.VMEM((depth // 16, half), F32)],
    )
    theirs = send(others, "dp_2", 1)
    parts = {s: cross(narrow, False, s) for s in SHIFTS}
    pack = call(pack_kernel, [((depth // 4, half), BF16)], 10**8, (narrow, parts[1], parts[2], parts[3]))[0]
    stacks = {s: cross(pack, True, s) for s in SHIFTS}
    stacks = [pack, stacks[1], stacks[2], stacks[3]]
    stacks = stacks + [send(g, "dp_2", 1) for g in stacks]
    peers, capacity = row_ids.shape[1:]
    slot_sums, slot_square = call(
        functools.partial(slot_kernel, capacity),
        [((peers, capacity // 2, 128), BF16), ((8, 128), F32)],
        8 * 10**9,
        (peer_counts, lookups_t, own, from_before, from_after, from_far),
        [pltpu.VMEM((features * batch, 256), BF16), pltpu.VMEM((1, features * batch), F32)],
        24,
    )
    outgoing = call(
        stamp_kernel,
        [((peers, capacity // 2 + 8, 128), BF16)],
        10**8,
        (slot_sums, row_ids[0], slot_square, square, sums),
    )[0]
    arrived = lax.all_to_all(outgoing, DP_MP, 0, 0, tiled=True)
    table_t, accum_t, scale = call(
        functools.partial(table_kernel, table_rate, adagrad_eps, clip_norm),
        [(table_rows.shape[::-1], F32), ((1, table_rows.shape[0]), F32), ((8, 128), F32)],
        6 * 10**9,
        (arrived, table_rows.T, table_accum.reshape(1, -1)),
        [pltpu.VMEM((table_rows.shape[0] // 4, 256), F32)],
        32,
    )
    weight_new, accum_new = call(
        weight_kernel,
        [((depth, width), BF16), (dense_accum.shape, F32)],
        10**9,
        (scale, weight_in, accum_full, dense_accum, mine, theirs, *stacks),
        (),
        16,
    )
    return (weight_new, accum_new, table_t.T, accum_t.reshape(-1))


def solution(mesh):
    torus = Mesh(mesh.devices.reshape(4, 4, 2, mesh.shape["mp"]), ("dp_0", "dp_1", "dp_2", "mp"))
    placed = (
        P(DP_MP, None, None),
        P(DP_MP, None, None),
        P(DP_MP, None),
        P(DP_MP, None),
        P(DP),
        P(DP),
        P(None, "mp"),
        P("mp"),
        P("mp"),
        P(DP, "mp"),
        P(DP_MP, None),
        P(DP_MP),
    )
    return jax.shard_map(
        inner,
        mesh=torus,
        in_specs=placed,
        out_specs=(P(None, "mp"), P(DP, "mp"), P(DP_MP, None), P(DP_MP)),
        check_vma=False,
    )
```

```python
import functools
import math

import jax
import jax.numpy as jnp
from jax import lax
from jax.experimental import pallas as pl
from jax.experimental.pallas import tpu as pltpu
from jax.sharding import Mesh
from jax.sharding import PartitionSpec as P


DP = ("dp_0", "dp_1", "dp_2")
DP_MP = ("dp_0", "dp_1", "dp_2", "mp")

clip_norm = 1.0
dense_rate = 0.02
table_rate = 0.5
adagrad_eps = 1e-10

F32 = jnp.float32
BF16 = jnp.bfloat16
VM = pl.BlockSpec(memory_space=pltpu.VMEM)
HBM = pl.BlockSpec(memory_space=pltpu.MemorySpace.HBM)


def iota(shape, dim):
    return lax.broadcasted_iota(jnp.int32, shape, dim)


def dot_f32(a, b, dims=(((1,), (0,)), ((), ()))):
    return lax.dot_general(a, b, dims, preferred_element_type=F32)


def spans_of(counts_ref):
    owners = counts_ref.shape[1]
    spread = jnp.broadcast_to(counts_ref[...].astype(F32), (owners, owners))
    at, of = iota((owners, owners), 0), iota((owners, owners), 1)
    ends = jnp.sum(jnp.where(of <= at, spread, 0.0), axis=1, keepdims=True)
    return ends - jnp.sum(jnp.where(of == at, spread, 0.0), axis=1, keepdims=True), ends


def gather_kernel(counts_hbm, lookups_hbm, slab_hbm, out_ref, counts_ref, lookups_ref, slab_ref, sems):
    copies = [
        pltpu.make_async_copy(a, b, sems.at[k])
        for k, (a, b) in enumerate(
            ((counts_hbm, counts_ref), (lookups_hbm, lookups_ref), (slab_hbm, slab_ref))
        )
    ]
    for copy in copies:
        copy.start()
    features, batch = lookups_ref.shape
    copies[0].wait()
    copies[1].wait()
    halfway = slab_ref.shape[1] // 2
    starts, ends = spans_of(counts_ref)
    copies[2].wait()
    halves = jnp.concatenate([slab_ref[:, :halfway], slab_ref[:, halfway:]], axis=0)
    low_lane = iota((batch, 128), 1) < 64

    def pair(p, carry):
        hots, inners = [], []
        for parity in range(2):
            q = lookups_ref[pl.ds(2 * p + parity, 1), :].astype(F32)
            match = (q >= starts) & (q < ends)
            slot = q - jnp.sum(jnp.where(match, starts, 0.0), axis=0, keepdims=True)
            upper = slot >= 16.0
            hot = jnp.where(match, 1.0, 0.0)
            hots.append(
                jnp.concatenate([jnp.where(upper, 0.0, hot), jnp.where(upper, hot, 0.0)], axis=0).astype(BF16)
            )
            inners.append(jnp.where(upper, slot - 16.0, slot))
        inner = jnp.concatenate([*inners, jnp.zeros((6, batch), F32)], axis=0).T
        both = []
        for parity in range(2):
            rows = dot_f32(hots[parity], halves, (((0,), (0,)), ((), ())))
            place = jnp.broadcast_to(inner[:, parity : parity + 1], (batch, 128))
            block = jnp.floor(place * 0.5)
            found = rows[:, :128]
            for k in range(1, 8):
                found = jnp.where(block == float(k), rows[:, 128 * k : 128 * (k + 1)], found)
            swap = place - 2.0 * block != float(parity)
            both.append(jnp.where(swap, pltpu.roll(found, 64, 1), found))
        out_ref[:, pl.ds(pl.multiple_of(p * 128, 128), 128)] = jnp.where(low_lane, both[0], both[1]).astype(BF16)
        return carry

    lax.fori_loop(0, features // 2, pair, 0, unroll=4)


def gather_rows(counts, lookups_t, slab):
    features, batch = lookups_t.shape
    return pl.pallas_call(
        gather_kernel,
        out_shape=jax.ShapeDtypeStruct((batch, features * 64), BF16),
        in_specs=[HBM, HBM, HBM],
        out_specs=VM,
        scratch_shapes=[
            pltpu.VMEM(counts.shape, counts.dtype),
            pltpu.VMEM(lookups_t.shape, lookups_t.dtype),
            pltpu.VMEM(slab.shape, slab.dtype),
            pltpu.SemaphoreType.DMA((3,)),
        ],
        name="gather_rows",
        compiler_params=pltpu.CompilerParams(vmem_limit_bytes=16 * 2**20),
        cost_estimate=pl.CostEstimate(flops=6 * 10**9, transcendentals=0, bytes_accessed=2 * 10**6),
    )(counts, lookups_t, slab)


def slot_kernel(
    capacity, counts_ref, lookups_ref, own_ref, a_ref, b_ref, c_ref, out_ref, square_ref, value_ref, at_ref
):
    owners = counts_ref.shape[1]
    features, batch = lookups_ref.shape
    spread = jnp.broadcast_to(counts_ref[...].astype(F32), (owners, owners))
    at, of = iota((owners, owners), 0), iota((owners, owners), 1)
    ends = jnp.sum(jnp.where(of <= at, spread, 0.0), axis=1, keepdims=True)
    starts = ends - jnp.sum(jnp.where(of == at, spread, 0.0), axis=1, keepdims=True)
    moves = iota((owners, 1), 0).astype(F32) * float(capacity) - starts
    indices = []
    for f in range(features):
        q = lookups_ref[f : f + 1, :].astype(F32)
        match = (q >= starts) & (q < ends)
        indices.append(q + jnp.sum(jnp.where(match, moves, 0.0), axis=0, keepdims=True))
        at_ref[0:1, batch * f : batch * (f + 1)] = jnp.floor(indices[f] * 0.5)
    index = jnp.concatenate(indices, axis=0)
    odd = (index - 2.0 * jnp.floor(index * 0.5)).T
    low_lane = iota((batch, 128), 1) < 64
    lane_odd = jnp.where(low_lane, 0.0, 1.0)
    for pair in range(features // 2):
        cols = slice(128 * pair, 128 * (pair + 1))
        total = own_ref[:, cols]
        for piece_ref in (a_ref, b_ref, c_ref):
            total = total + piece_ref[:, cols].astype(F32)
        turned = pltpu.roll(total, 64, 1)
        for parity in range(2):
            f = 2 * pair + parity
            rows = jnp.where(low_lane, total, turned) if parity == 0 else jnp.where(low_lane, turned, total)
            rows = jnp.where(jnp.broadcast_to(odd[:, f : f + 1], (batch, 128)) == lane_odd, rows, 0.0)
            high = rows.astype(BF16)
            value_ref[batch * f : batch * (f + 1), 0:128] = high
            value_ref[batch * f : batch * (f + 1), 128:256] = (rows - high.astype(F32)).astype(BF16)
    block = 512
    each = block * 2 // capacity
    where = jnp.broadcast_to(at_ref[...], (block, features * batch))
    lines = iota((block, features * batch), 0).astype(F32)

    def part(m, square):
        hot = jnp.where(lines == where - (m * block).astype(F32), 1.0, 0.0).astype(BF16)
        both = dot_f32(hot, value_ref[...])
        sums = both[:, 0:128] + both[:, 128:256]
        first = pl.multiple_of(m * each, each)
        out_ref[pl.ds(first, each), :, :] = sums.astype(BF16).reshape(each, capacity // 2, 128)
        return square + jnp.sum(jnp.sum(sums * sums, axis=1, keepdims=True), axis=0, keepdims=True)

    square = lax.fori_loop(0, owners // each, part, jnp.zeros((1, 1), F32))
    square_ref[...] = jnp.broadcast_to(square, square_ref.shape)


def final_kernel(
    rates,
    arrived_ref,
    rows_ref,
    mine_ref,
    theirs_ref,
    table_hbm,
    accum_hbm,
    w_hbm,
    held_hbm,
    grad_hbm,
    table_out,
    accum_out,
    w_out_hbm,
    dense_out,
    acc_ref,
    table_ref,
    accum_ref,
    w_ref,
    held_ref,
    grad_ref,
    sems,
    in_sems,
    out_sems,
):
    rate, dense, eps, clip = rates
    size = 64
    count = w_ref.shape[0] // size
    copies = [
        pltpu.make_async_copy(a, b, sems.at[k])
        for k, (a, b) in enumerate(((table_hbm, table_ref), (accum_hbm, accum_ref)))
    ]
    for copy in copies:
        copy.start()
    sides = ((w_hbm, w_ref), (held_hbm, held_ref), (grad_hbm, grad_ref))

    def fetch(k):
        at = pl.ds(pl.multiple_of(k * size, size), size)
        return [pltpu.make_async_copy(a.at[at, :], b.at[at, :], in_sems.at[m, k]) for m, (a, b) in enumerate(sides)]

    def begin(k, carry):
        for copy in fetch(k):
            copy.start()
        return carry

    lax.fori_loop(0, count, begin, 0)
    sources, lines, _ = arrived_ref.shape
    half = lines - 8
    capacity = 2 * half
    rows = table_ref.shape[1]
    blocks = rows // 256
    every = sources * half
    info = arrived_ref[:, half:, :].reshape(sources * 8, 128)
    squares = jnp.sum(info.astype(F32)[:, 2 * capacity : 2 * capacity + 3], axis=0, keepdims=True)
    total = jnp.sum(squares, axis=1, keepdims=True) * 0.125
    scale = clip / jnp.maximum(jnp.sqrt(total), clip)
    share = jnp.where(iota((sources * 8, every), 0) >> 3 == iota((sources * 8, every), 1) // half, 0.125, 0.0)
    spread_info = dot_f32(info, share.astype(BF16), (((0,), (0,)), ((), ())))
    slot = iota((capacity, every), 0)
    line = iota((capacity, every), 1) & (half - 1)
    inside_at = iota((256, every), 0).astype(F32)
    turned = arrived_ref[:, :half, :].reshape(every, 128).astype(F32).T
    acc = None
    for parity in range(2):
        mine = slot == 2 * line + parity
        block = jnp.sum(jnp.where(mine, spread_info[0:capacity], 0.0), axis=0, keepdims=True)
        inside = jnp.sum(jnp.where(mine, spread_info[capacity : 2 * capacity], 0.0), axis=0, keepdims=True)
        piece = turned[64 * parity : 64 * (parity + 1), :]
        hot = jnp.where(inside_at == inside, 1.0, 0.0).astype(BF16)
        spread = jnp.concatenate([jnp.where(block == float(k), piece, 0.0).astype(BF16) for k in range(blocks)], axis=0)
        part = dot_f32(spread, hot, (((1,), (1,)), ((), ())))
        acc = part if acc is None else acc + part
    acc_ref[...] = acc
    for copy in copies:
        copy.wait()

    def finish(k, carry):
        received = scale * acc_ref[pl.ds(pl.multiple_of(64 * k, 64), 64), :]
        cols = pl.ds(pl.multiple_of(256 * k, 256), 256)
        accum = accum_ref[:, cols] + jnp.sum(received * received, axis=0, keepdims=True) * (1.0 / 64.0)
        accum_out[:, cols] = accum
        table_out[:, cols] = table_ref[:, cols] - rate * received / (accum * lax.rsqrt(accum) + eps)
        return carry

    lax.fori_loop(0, blocks, finish, 0, unroll=2)

    def update(k, carry):
        for copy in fetch(k):
            copy.wait()
        at = pl.ds(pl.multiple_of(k * size, size), size)
        grad = scale * grad_ref[at, :].astype(F32)
        accum = held_ref[at, :].astype(F32) + grad * grad
        step = dense * grad / (accum * lax.rsqrt(accum) + eps)
        w_ref[at, :] = (w_ref[at, :].astype(F32) - step).astype(BF16)
        pltpu.make_async_copy(w_ref.at[at, :], w_out_hbm.at[at, :], out_sems.at[k]).start()
        return carry

    lax.fori_loop(0, count, update, 0)
    core = lax.axis_index("dp_2")
    half = mine_ref.shape[1]
    for grad, c in ((mine_ref[...], core), (theirs_ref[...], 1 - core)):
        cols = pl.ds(pl.multiple_of(c * half, half), half)
        grad = scale * grad
        dense_out[:, cols] = rows_ref[:, cols] + grad * grad

    def drain(k, carry):
        at = pl.ds(pl.multiple_of(k * size, size), size)
        pltpu.make_async_copy(w_ref.at[at, :], w_out_hbm.at[at, :], out_sems.at[k]).wait()
        return carry

    lax.fori_loop(0, count, drain, 0)


def footprint(shapes):
    return sum(math.prod(s.shape) * 4 for s in shapes)


def call(kernel, outs, flops, args, scratch=(), spare=8, far=(), far_out=(), aliases=None):
    shapes = tuple(jax.ShapeDtypeStruct(s, t) for s, t in outs)
    return pl.pallas_call(
        kernel,
        out_shape=shapes,
        in_specs=[HBM if k in far else VM for k in range(len(args))],
        out_specs=tuple(HBM if k in far_out else VM for k in range(len(shapes))),
        scratch_shapes=list(scratch),
        input_output_aliases=aliases or {},
        compiler_params=pltpu.CompilerParams(vmem_limit_bytes=footprint(scratch) + spare * 2**20),
        cost_estimate=pl.CostEstimate(flops=flops, transcendentals=0, bytes_accessed=2 * 10**6),
    )(*args)


SHIFTS = (1, 3, 2)


def spot(axis, shift):
    return lax.rem(lax.axis_index(axis) + shift, 4)


def sigmoid(x):
    return 0.5 * jnp.tanh(0.5 * x) + 0.5


def forward_kernel(chunks, *refs):
    ins, (w_ref, bias_ref, out_w_ref) = refs[:chunks], refs[chunks : chunks + 3]
    slope_ref, hidden_ref, logit_ref, turned_ref, rows_ref = refs[chunks + 3 :]
    rows = ins[0].shape[0]
    width = w_ref.shape[1]
    for k in range(chunks):
        rows_ref[rows * k : rows * (k + 1), :] = ins[k][...]
        turned_ref[:, rows * k : rows * (k + 1)] = ins[k][...].T

    def columns(n, carry):
        cols = pl.ds(pl.multiple_of(n * 256, 256), 256)
        act = dot_f32(rows_ref[...], w_ref[:, cols]) + bias_ref[:, cols]
        sigma = sigmoid(act)
        hidden_ref[:, cols] = (act * sigma).astype(BF16)
        slope_ref[:, cols] = out_w_ref[:, cols].astype(F32) * sigma * (1.0 + act * (1.0 - sigma))
        return carry

    lax.fori_loop(0, width // 256, columns, 0, unroll=8)
    out_w = jnp.broadcast_to(out_w_ref[...], (16, width))
    for k in range(logit_ref.shape[0]):
        part = dot_f32(out_w, hidden_ref[256 * k : 256 * (k + 1), :], (((1,), (1,)), ((), ())))
        logit_ref[k : k + 1, :] = part[0:1, :]


def forward(chunks, w, bias, out_w):
    rows, depth = chunks[0].shape
    width = w.shape[1]
    n = len(chunks)
    total = n * rows
    outs = [((total, width), F32), ((total, width), BF16), ((total // 256, 256), F32), ((depth, total), BF16)]
    return call(
        functools.partial(forward_kernel, n),
        outs,
        total * 10**7,
        (*chunks, w, bias, out_w),
        [pltpu.VMEM((total, depth), BF16)],
    )


ORDER = (0, 3, 1, 2)
PARTNERS = ((0, 1, 2, 3), (2, 0, 3, 1), (1, 3, 0, 2), (3, 2, 1, 0))


def slope_kernel(*refs):
    slopes, hiddens = refs[0:3], refs[3:6]
    own_ref, prev_ref, next_ref, far_ref, labels_ref, weight_ref = refs[6:12]
    dact_ref, other_ref, sums_mine_ref, sums_other_ref, sums_ref = refs[12:]
    rows, width = slopes[0].shape
    spans = ((0, 0), (1, 0), (1, rows), (2, 0))
    half = width // 2
    core = lax.axis_index("dp_2")
    dlogits = []
    for k in range(4):
        at = spot("mp", ORDER[k])
        logit = (own_ref[k : k + 1, :] + far_ref[PARTNERS[3][k] : PARTNERS[3][k] + 1, :]) + (
            prev_ref[PARTNERS[1][k] : PARTNERS[1][k] + 1, :] + next_ref[PARTNERS[2][k] : PARTNERS[2][k] + 1, :]
        )
        here = pl.ds(pl.multiple_of(at * rows, rows), rows)
        label = labels_ref[:, here].astype(F32)
        dlogits.append(weight_ref[:, here] * (sigmoid(logit) - label))
    rows_form = jnp.concatenate(dlogits + [jnp.zeros((4, rows), F32)], axis=0)
    cols_form = rows_form.T
    pick = iota((16, rows), 0)
    ones = jnp.ones((16, rows), BF16)
    cols, lefts = [], []
    for k in range(4):
        cols.append(cols_form[:, k : k + 1])
        top = dlogits[k].astype(BF16).astype(F32)
        rest = dlogits[k] - top
        lefts.append(jnp.where(pick == 0, top, jnp.where(pick == 1, rest, 0.0)).astype(BF16))
    block = 256
    line = iota((16, block), 0)

    def columns(n, carry):
        span = pl.ds(pl.multiple_of(n * block, block), block)
        bias_sum = out_sum = jnp.zeros((16, block), F32)
        for k in range(4):
            which, start = spans[k]
            part = (slopes[which][start : start + rows, span] * cols[k]).astype(BF16)
            dact_ref[rows * k : rows * (k + 1), span] = part
            bias_sum = bias_sum + dot_f32(ones, part)
            out_sum = out_sum + dot_f32(lefts[k], hiddens[which][start : start + rows, span])
        total = jnp.sum(out_sum, axis=0, keepdims=True)
        sums_ref[:, span] = jnp.where(line == 0, bias_sum, jnp.where(line == 1, total, 0.0))
        return carry

    lax.fori_loop(0, width // block, columns, 0)
    other_ref[...] = dact_ref[:, pl.ds(pl.multiple_of((1 - core) * half, half), half)]
    sums_mine_ref[...] = sums_ref[:, pl.ds(pl.multiple_of(core * half, half), half)]
    sums_other_ref[...] = sums_ref[:, pl.ds(pl.multiple_of((1 - core) * half, half), half)]


def back_kernel(dact_ref, w_ref, own_ref, *outs):
    rows, depth = own_ref.shape
    block = 512

    def columns(n, carry):
        span = pl.ds(pl.multiple_of(n * block, block), block)
        part = dot_f32(dact_ref[...], w_ref[span, :], (((1,), (1,)), ((), ())))
        for k, target in enumerate((own_ref, *outs)):
            target[:, span] = part[rows * k : rows * (k + 1), :].astype(target.dtype)
        return carry

    lax.fori_loop(0, depth // block, columns, 0)


def spot_on(first, core, shift):
    x, y = lax.axis_index("dp_0"), lax.axis_index("dp_1")
    along = x * (1 - core) + y * core if first else y * (1 - core) + x * core
    return lax.rem(along + shift, 4)


def chip_rows(core, outer, inner, size):
    return pl.multiple_of((outer * (4 - 3 * core) + inner * (1 + 3 * core)) * size, size)


def grad_kernel(shifts, *refs):
    turned, (dact_ref, far_dact_ref, sums_ref, far_sums_ref), outs = refs[0:6], refs[6:10], refs[10:]
    size = turned[0].shape[0] // 16
    half = far_dact_ref.shape[1]
    spans = ((0, 256), (256, 512), (768, 256))
    core = lax.axis_index("dp_2")
    local = pl.ds(pl.multiple_of(core * half, half), half)
    for target, shift in zip(outs, shifts):
        at = [pl.ds(chip_rows(core, spot_on(True, core, shift), t, size), size) for t in range(4)]
        part = None
        for i, (s, n) in enumerate(spans):
            near = jnp.concatenate([turned[i][a, :] for a in at], axis=0)
            away = jnp.concatenate([turned[i + 3][a, :] for a in at], axis=0)
            p = dot_f32(near, dact_ref[s : s + n, local]) + dot_f32(away, far_dact_ref[s : s + n, :])
            part = p if part is None else part + p
        target[0:256, :] = part.astype(target.dtype)
        target[256:272, :] = split_rows(sums_ref[...] + far_sums_ref[...]).astype(target.dtype)


def split_rows(sums):
    top = sums.astype(BF16).astype(F32)
    return jnp.concatenate([top[0:8], (sums - top)[0:8]], axis=0)


def joined_rows(rows):
    return jnp.concatenate([rows[0:8] + rows[8:16], jnp.zeros_like(rows[0:8])], axis=0)


def middle_kernel(own_ref, a_ref, b_ref, c_ref, out_ref):
    total = own_ref[...] + a_ref[...].astype(F32) + b_ref[...].astype(F32) + c_ref[...].astype(F32)
    out_ref[0:256, :] = total[0:256].astype(BF16)
    out_ref[256:272, :] = split_rows(joined_rows(total[256:272])).astype(BF16)


def last_kernel(
    own_ref,
    before_ref,
    after_ref,
    far_ref,
    sums_ref,
    ids_ref,
    slot_square_ref,
    narrow_ref,
    mine_ref,
    other_ref,
    out_ref,
    full_ref,
):
    core = lax.axis_index("dp_2")
    at = spot_on(False, core, 0)
    even = lax.rem(at, 2) == 0
    before, after = before_ref[...].astype(F32), after_ref[...].astype(F32)
    partner, other = jnp.where(even, after, before), jnp.where(even, before, after)
    total = (own_ref[...].astype(F32) + partner) + (other + far_ref[...].astype(F32))
    count = narrow_ref.shape[0]
    extra = joined_rows(total[count:])
    full_ref[...] = total[:count]
    narrow_ref[...] = total[:count].astype(BF16)
    size = count // 4
    per = size // 2
    chunk = full_ref[pl.ds(pl.multiple_of(at * size, size), size), :]
    mine_ref[...] = full_ref[pl.ds(pl.multiple_of(at * size + core * per, per), per), :]
    other_ref[...] = full_ref[pl.ds(pl.multiple_of(at * size + (1 - core) * per, per), per), :]
    lead = jnp.where((lax.axis_index("dp_0") == 0) & (lax.axis_index("dp_1") == 0), 1.0, 0.0)
    square = slot_square_ref[0:1, 0:1] + jnp.sum(jnp.sum(chunk * chunk, axis=1, keepdims=True), axis=0, keepdims=True)
    square = square + lead * jnp.sum(jnp.sum(extra * extra, axis=1, keepdims=True), axis=0, keepdims=True)
    owners, capacity = ids_ref.shape
    lines = capacity // 2
    top = square.astype(BF16).astype(F32)
    mid = (square - top).astype(BF16).astype(F32)
    end = square - top - mid
    ids = ids_ref[...]
    lane = iota((owners, 128 - 2 * capacity), 1)
    tail = jnp.where(lane == 0, top, jnp.where(lane == 1, mid, jnp.where(lane == 2, end, 0.0)))
    info = jnp.concatenate([(ids >> 8).astype(F32), (ids & 255).astype(F32), tail], axis=1)
    out_ref[:, :lines, :] = sums_ref[...]
    out_ref[:, lines:, :] = jnp.broadcast_to(info[:, None, :], (owners, 8, 128)).astype(BF16)


def pack_kernel(*refs):
    rows = refs[0].shape[0]
    for k in range(4):
        refs[4][rows * k : rows * (k + 1), :] = refs[k][...]


def merge_kernel(*refs):
    stacks, out_ref = refs[:8], refs[8]
    core = lax.axis_index("dp_2")
    per = stacks[0].shape[0] // 4
    for side, c in ((0, core), (1, 1 - core)):
        for i in range(4):
            for j in range(4):
                at = chip_rows(c, spot_on(True, c, (4 - i) % 4), spot_on(False, c, (4 - j) % 4), 1)
                rows = pl.ds(pl.multiple_of((at * 2 + c) * per, per), per)
                out_ref[rows, :] = stacks[4 * side + i][per * j : per * (j + 1), :]


def grad_merge_kernel(*refs):
    stacks, out_ref = refs[:8], refs[8]
    core = lax.axis_index("dp_2")
    size = stacks[0].shape[0] // 4
    half = stacks[0].shape[1]
    for side, c in ((0, core), (1, 1 - core)):
        cols = pl.ds(pl.multiple_of(c * half, half), half)
        for i in range(4):
            outer = spot_on(True, c, (4 - i) % 4)
            for j in range(4):
                out_ref[pl.ds(chip_rows(c, outer, j, size), size), cols] = stacks[4 * side + i][size * j : size * (j + 1), :]


def cross(x, first, shift):
    moves = []
    for i in range(32):
        a, b, c = i // 8, i // 2 % 4, i % 2
        a, b = ((a + shift) % 4, b) if (c == 0) == first else (a, (b + shift) % 4)
        moves.append((i, a * 8 + b * 2 + c))
    return lax.ppermute(x, DP, moves)


def send(x, axis, shift):
    n = lax.axis_size(axis)
    return lax.ppermute(x, axis, [(i, (i + shift) % n) for i in range(n)])


def around(x, axis):
    return [send(x, axis, s) for s in SHIFTS]


def inner(
    slab_values,
    row_ids,
    peer_counts,
    lookup_slots,
    labels,
    sample_weight,
    weight_in,
    bias_in,
    weight_out,
    dense_accum,
    table_rows,
    table_accum,
):
    batch, features = lookup_slots.shape
    depth, width = weight_in.shape
    half = width // 2
    lookups_t = lookup_slots.T
    pooled = gather_rows(peer_counts, lookups_t, slab_values[0])
    before, after = send(pooled, "mp", 1), send(pooled, "mp", 3)
    narrow = dense_accum.astype(BF16)
    parts = {s: cross(narrow, False, s) for s in SHIFTS}
    block = (depth // 8, width)
    near = call(pack_kernel, [(block, BF16)], 10**8, (narrow, parts[1], parts[2], parts[3]))[0]
    stacks = {s: cross(near, True, s) for s in SHIFTS}
    stacks = [near, stacks[1], stacks[2], stacks[3]]
    stacks = stacks + [send(g, "dp_2", 1) for g in stacks]
    accum_full = call(merge_kernel, [((depth, width), BF16)], 10**8, stacks)[0]
    bias = bias_in.reshape(1, width)
    out_w = weight_out.reshape(1, width)
    far_low, far_high = send(before[: batch // 2], "mp", 1), send(after[batch // 2 :], "mp", 3)
    slope_0, hidden_0, logit_0, turned_0 = forward([pooled], weight_in, bias, out_w)
    slope_1, hidden_1, logit_1, turned_1 = forward([before, after], weight_in, bias, out_w)
    slope_2, hidden_2, logit_2, turned_2 = forward([far_low, far_high], weight_in, bias, out_w)
    turned = [turned_0, turned_1, turned_2]
    turned = turned + [send(t, "dp_2", 1) for t in turned]
    logits = jnp.concatenate([logit_0, logit_1, logit_2], axis=0)
    logit_before, logit_after, logit_far = around(logits, "mp")
    dact, other, sums_mine, sums_other = call(
        slope_kernel,
        [((4 * batch, width), BF16), ((4 * batch, half), BF16), ((16, half), F32), ((16, half), F32)],
        2 * 10**9,
        (
            slope_0,
            slope_1,
            slope_2,
            hidden_0,
            hidden_1,
            hidden_2,
            logits,
            logit_before,
            logit_after,
            logit_far,
            labels.reshape(1, -1),
            sample_weight.reshape(1, -1),
        ),
        [pltpu.VMEM((16, width), F32)],
    )
    far_dact = send(other, "dp_2", 1)
    far_sums = send(sums_other, "dp_2", 1)
    own, to_before, to_after, to_far = call(
        back_kernel, [((batch, depth), F32)] + [((batch, depth), BF16)] * 3, 4 * 10**9, (dact, weight_in)
    )
    from_after, from_before, from_far = send(to_before, "mp", 3), send(to_after, "mp", 1), send(to_far, "mp", 2)
    held = (*turned, dact, far_dact, sums_mine, far_sums)
    block = (depth // 4 + 16, half)
    to_next, to_prev = call(functools.partial(grad_kernel, SHIFTS[:2]), [(block, BF16)] * 2, 4 * 10**9, held)
    from_prev, from_next = cross(to_next, True, 1), cross(to_prev, True, 3)
    to_far, keep = call(functools.partial(grad_kernel, (2, 0)), [(block, BF16), (block, F32)], 4 * 10**9, held)
    distant = cross(to_far, True, 2)
    keep = call(middle_kernel, [(block, BF16)], 10**8, (keep, from_prev, from_next, distant))[0]
    got = [cross(keep, False, s) for s in SHIFTS]
    peers, capacity = row_ids.shape[1:]
    slot_sums, slot_square = call(
        functools.partial(slot_kernel, capacity),
        [((peers, capacity // 2, 128), BF16), ((8, 128), F32)],
        8 * 10**9,
        (peer_counts, lookups_t, own, from_before, from_after, from_far),
        [pltpu.VMEM((features * batch, 256), BF16), pltpu.VMEM((1, features * batch), F32)],
        24,
    )
    narrow, mine, others, outgoing = call(
        last_kernel,
        [((depth // 4, half), BF16)] + [((depth // 32, half), F32)] * 2 + [((peers, capacity // 2 + 8, 128), BF16)],
        10**8,
        (keep, *got, slot_sums, row_ids[0], slot_square),
        [pltpu.VMEM((depth // 4, half), F32)],
    )
    theirs = send(others, "dp_2", 1)
    stacks = {s: cross(narrow, True, s) for s in SHIFTS}
    stacks = [narrow, stacks[1], stacks[2], stacks[3]]
    stacks = stacks + [send(g, "dp_2", 1) for g in stacks]
    arrived = lax.all_to_all(outgoing, DP_MP, 0, 0, tiled=True)
    grad_full = call(grad_merge_kernel, [((depth, width), BF16)], 10**8, stacks)[0]
    size = depth // 64
    table_t, accum_t, weight_new, accum_new = call(
        functools.partial(final_kernel, (table_rate, dense_rate, adagrad_eps, clip_norm)),
        [
            (table_rows.shape[::-1], F32),
            ((1, table_rows.shape[0]), F32),
            ((depth, width), BF16),
            (dense_accum.shape, F32),
        ],
        8 * 10**9,
        (
            arrived,
            dense_accum,
            mine,
            theirs,
            table_rows.T,
            table_accum.reshape(1, -1),
            weight_in,
            accum_full,
            grad_full,
        ),
        [
            pltpu.VMEM((table_rows.shape[0] // 4, 256), F32),
            pltpu.VMEM(table_rows.shape[::-1], F32),
            pltpu.VMEM((1, table_rows.shape[0]), F32),
            pltpu.VMEM((depth, width), BF16),
            pltpu.VMEM((depth, width), BF16),
            pltpu.VMEM((depth, width), BF16),
            pltpu.SemaphoreType.DMA((2,)),
            pltpu.SemaphoreType.DMA((3, size)),
            pltpu.SemaphoreType.DMA((size,)),
        ],
        33,
        (4, 5, 6, 7, 8),
        (2,),
    )
    return (weight_new, accum_new, table_t.T, accum_t.reshape(-1))


def solution(mesh):
    torus = Mesh(mesh.devices.reshape(4, 4, 2, mesh.shape["mp"]), ("dp_0", "dp_1", "dp_2", "mp"))
    placed = (
        P(DP_MP, None, None),
        P(DP_MP, None, None),
        P(DP_MP, None),
        P(DP_MP, None),
        P(DP),
        P(DP),
        P(None, "mp"),
        P("mp"),
        P("mp"),
        P(DP, "mp"),
        P(DP_MP, None),
        P(DP_MP),
    )
    return jax.shard_map(
        inner,
        mesh=torus,
        in_specs=placed,
        out_specs=(P(None, "mp"), P(DP, "mp"), P(DP_MP, None), P(DP_MP)),
        check_vma=False,
    )
```

```python
import functools
import math

import jax
import jax.numpy as jnp
from jax import lax
from jax.experimental import pallas as pl
from jax.experimental.pallas import tpu as pltpu
from jax.sharding import Mesh
from jax.sharding import PartitionSpec as P


DP = ("dp_0", "dp_1", "dp_2")
DP_MP = ("dp_0", "dp_1", "dp_2", "mp")

clip_norm = 1.0
dense_rate = 0.02
table_rate = 0.5
adagrad_eps = 1e-10

F32 = jnp.float32
BF16 = jnp.bfloat16
VM = pl.BlockSpec(memory_space=pltpu.VMEM)
HBM = pl.BlockSpec(memory_space=pltpu.MemorySpace.HBM)


def iota(shape, dim):
    return lax.broadcasted_iota(jnp.int32, shape, dim)


def dot_f32(a, b, dims=(((1,), (0,)), ((), ()))):
    return lax.dot_general(a, b, dims, preferred_element_type=F32)


def spans_of(counts_ref):
    owners = counts_ref.shape[1]
    spread = jnp.broadcast_to(counts_ref[...].astype(F32), (owners, owners))
    at, of = iota((owners, owners), 0), iota((owners, owners), 1)
    ends = jnp.sum(jnp.where(of <= at, spread, 0.0), axis=1, keepdims=True)
    return ends - jnp.sum(jnp.where(of == at, spread, 0.0), axis=1, keepdims=True), ends


def gather_kernel(counts_hbm, lookups_hbm, slab_hbm, low_ref, high_ref, counts_ref, lookups_ref, slab_ref, sems):
    copies = [
        pltpu.make_async_copy(a, b, sems.at[k])
        for k, (a, b) in enumerate(
            ((counts_hbm, counts_ref), (lookups_hbm, lookups_ref), (slab_hbm, slab_ref))
        )
    ]
    for copy in copies:
        copy.start()
    features, batch = lookups_ref.shape
    copies[0].wait()
    copies[1].wait()
    halfway = slab_ref.shape[1] // 2
    starts, ends = spans_of(counts_ref)
    copies[2].wait()
    halves = jnp.concatenate([slab_ref[:, :halfway], slab_ref[:, halfway:]], axis=0)
    low_lane = iota((batch, 128), 1) < 64

    def pair(p, carry):
        hots, inners = [], []
        for parity in range(2):
            q = lookups_ref[pl.ds(2 * p + parity, 1), :].astype(F32)
            match = (q >= starts) & (q < ends)
            slot = q - jnp.sum(jnp.where(match, starts, 0.0), axis=0, keepdims=True)
            upper = slot >= 16.0
            hot = jnp.where(match, 1.0, 0.0)
            hots.append(
                jnp.concatenate([jnp.where(upper, 0.0, hot), jnp.where(upper, hot, 0.0)], axis=0).astype(BF16)
            )
            inners.append(jnp.where(upper, slot - 16.0, slot))
        inner = jnp.concatenate([*inners, jnp.zeros((6, batch), F32)], axis=0).T
        both = []
        for parity in range(2):
            rows = dot_f32(hots[parity], halves, (((0,), (0,)), ((), ())))
            place = jnp.broadcast_to(inner[:, parity : parity + 1], (batch, 128))
            block = jnp.floor(place * 0.5)
            found = rows[:, :128]
            for k in range(1, 8):
                found = jnp.where(block == float(k), rows[:, 128 * k : 128 * (k + 1)], found)
            swap = place - 2.0 * block != float(parity)
            both.append(jnp.where(swap, pltpu.roll(found, 64, 1), found))
        pooled = jnp.where(low_lane, both[0], both[1]).astype(BF16)
        cols = pl.ds(pl.multiple_of(p * 128, 128), 128)
        low_ref[:, cols] = pooled[: batch // 2]
        high_ref[:, cols] = pooled[batch // 2 :]
        return carry

    lax.fori_loop(0, features // 2, pair, 0, unroll=4)


def gather_rows(counts, lookups_t, slab):
    features, batch = lookups_t.shape
    return pl.pallas_call(
        gather_kernel,
        out_shape=(jax.ShapeDtypeStruct((batch // 2, features * 64), BF16),) * 2,
        in_specs=[HBM, HBM, HBM],
        out_specs=(VM, VM),
        scratch_shapes=[
            pltpu.VMEM(counts.shape, counts.dtype),
            pltpu.VMEM(lookups_t.shape, lookups_t.dtype),
            pltpu.VMEM(slab.shape, slab.dtype),
            pltpu.SemaphoreType.DMA((3,)),
        ],
        name="gather_rows",
        compiler_params=pltpu.CompilerParams(vmem_limit_bytes=16 * 2**20),
        cost_estimate=pl.CostEstimate(flops=6 * 10**9, transcendentals=0, bytes_accessed=2 * 10**6),
    )(counts, lookups_t, slab)


def slot_kernel(
    capacity, counts_ref, lookups_ref, own_ref, a_ref, b_ref, c_ref, out_ref, square_ref, value_ref, at_ref
):
    owners = counts_ref.shape[1]
    features, batch = lookups_ref.shape
    spread = jnp.broadcast_to(counts_ref[...].astype(F32), (owners, owners))
    at, of = iota((owners, owners), 0), iota((owners, owners), 1)
    ends = jnp.sum(jnp.where(of <= at, spread, 0.0), axis=1, keepdims=True)
    starts = ends - jnp.sum(jnp.where(of == at, spread, 0.0), axis=1, keepdims=True)
    moves = iota((owners, 1), 0).astype(F32) * float(capacity) - starts
    indices = []
    for f in range(features):
        q = lookups_ref[f : f + 1, :].astype(F32)
        match = (q >= starts) & (q < ends)
        indices.append(q + jnp.sum(jnp.where(match, moves, 0.0), axis=0, keepdims=True))
        at_ref[0:1, batch * f : batch * (f + 1)] = jnp.floor(indices[f] * 0.5)
    index = jnp.concatenate(indices, axis=0)
    odd = (index - 2.0 * jnp.floor(index * 0.5)).T
    low_lane = iota((batch, 128), 1) < 64
    lane_odd = jnp.where(low_lane, 0.0, 1.0)
    for pair in range(features // 2):
        cols = slice(128 * pair, 128 * (pair + 1))
        total = own_ref[:, cols]
        for piece_ref in (a_ref, b_ref, c_ref):
            total = total + piece_ref[:, cols].astype(F32)
        turned = pltpu.roll(total, 64, 1)
        for parity in range(2):
            f = 2 * pair + parity
            rows = jnp.where(low_lane, total, turned) if parity == 0 else jnp.where(low_lane, turned, total)
            rows = jnp.where(jnp.broadcast_to(odd[:, f : f + 1], (batch, 128)) == lane_odd, rows, 0.0)
            high = rows.astype(BF16)
            value_ref[batch * f : batch * (f + 1), 0:128] = high
            value_ref[batch * f : batch * (f + 1), 128:256] = (rows - high.astype(F32)).astype(BF16)
    block = 512
    each = block * 2 // capacity
    where = jnp.broadcast_to(at_ref[...], (block, features * batch))
    lines = iota((block, features * batch), 0).astype(F32)

    def part(m, square):
        hot = jnp.where(lines == where - (m * block).astype(F32), 1.0, 0.0).astype(BF16)
        both = dot_f32(hot, value_ref[...])
        sums = both[:, 0:128] + both[:, 128:256]
        first = pl.multiple_of(m * each, each)
        out_ref[pl.ds(first, each), :, :] = sums.astype(BF16).reshape(each, capacity // 2, 128)
        return square + jnp.sum(jnp.sum(sums * sums, axis=1, keepdims=True), axis=0, keepdims=True)

    square = lax.fori_loop(0, owners // each, part, jnp.zeros((1, 1), F32))
    square_ref[...] = jnp.broadcast_to(square, square_ref.shape)


def final_kernel(
    rates,
    arrived_ref,
    rows_ref,
    mine_ref,
    theirs_ref,
    table_hbm,
    accum_hbm,
    w_hbm,
    held_hbm,
    grad_hbm,
    table_out,
    accum_out,
    w_out_hbm,
    dense_out,
    acc_ref,
    table_ref,
    accum_ref,
    w_ref,
    held_ref,
    grad_ref,
    sems,
    in_sems,
    out_sems,
):
    rate, dense, eps, clip = rates
    size = 64
    count = w_ref.shape[0] // size
    copies = [
        pltpu.make_async_copy(a, b, sems.at[k])
        for k, (a, b) in enumerate(((table_hbm, table_ref), (accum_hbm, accum_ref)))
    ]
    for copy in copies:
        copy.start()
    sides = ((w_hbm, w_ref), (held_hbm, held_ref), (grad_hbm, grad_ref))

    def fetch(k):
        at = pl.ds(pl.multiple_of(k * size, size), size)
        return [pltpu.make_async_copy(a.at[at, :], b.at[at, :], in_sems.at[m, k]) for m, (a, b) in enumerate(sides)]

    def begin(k, carry):
        for copy in fetch(k):
            copy.start()
        return carry

    lax.fori_loop(0, count, begin, 0)
    sources, lines, _ = arrived_ref.shape
    half = lines - 8
    capacity = 2 * half
    rows = table_ref.shape[1]
    blocks = rows // 256
    every = sources * half
    info = arrived_ref[:, half:, :].reshape(sources * 8, 128)
    squares = jnp.sum(info.astype(F32)[:, 2 * capacity : 2 * capacity + 3], axis=0, keepdims=True)
    total = jnp.sum(squares, axis=1, keepdims=True) * 0.125
    scale = clip / jnp.maximum(jnp.sqrt(total), clip)
    share = jnp.where(iota((sources * 8, every), 0) >> 3 == iota((sources * 8, every), 1) // half, 0.125, 0.0)
    spread_info = dot_f32(info, share.astype(BF16), (((0,), (0,)), ((), ())))
    slot = iota((capacity, every), 0)
    line = iota((capacity, every), 1) & (half - 1)
    inside_at = iota((256, every), 0).astype(F32)
    turned = arrived_ref[:, :half, :].reshape(every, 128).astype(F32).T
    acc = None
    for parity in range(2):
        mine = slot == 2 * line + parity
        block = jnp.sum(jnp.where(mine, spread_info[0:capacity], 0.0), axis=0, keepdims=True)
        inside = jnp.sum(jnp.where(mine, spread_info[capacity : 2 * capacity], 0.0), axis=0, keepdims=True)
        piece = turned[64 * parity : 64 * (parity + 1), :]
        hot = jnp.where(inside_at == inside, 1.0, 0.0).astype(BF16)
        spread = jnp.concatenate([jnp.where(block == float(k), piece, 0.0).astype(BF16) for k in range(blocks)], axis=0)
        part = dot_f32(spread, hot, (((1,), (1,)), ((), ())))
        acc = part if acc is None else acc + part
    acc_ref[...] = acc
    for copy in copies:
        copy.wait()

    def finish(k, carry):
        received = scale * acc_ref[pl.ds(pl.multiple_of(64 * k, 64), 64), :]
        cols = pl.ds(pl.multiple_of(256 * k, 256), 256)
        accum = accum_ref[:, cols] + jnp.sum(received * received, axis=0, keepdims=True) * (1.0 / 64.0)
        accum_out[:, cols] = accum
        table_out[:, cols] = table_ref[:, cols] - rate * received / (accum * lax.rsqrt(accum) + eps)
        return carry

    lax.fori_loop(0, blocks, finish, 0, unroll=2)

    def update(k, carry):
        for copy in fetch(k):
            copy.wait()
        at = pl.ds(pl.multiple_of(k * size, size), size)
        grad = scale * grad_ref[at, :].astype(F32)
        accum = held_ref[at, :].astype(F32) + grad * grad
        seed = lax.rsqrt(accum)
        inverse = seed * (2.0 - (accum * seed + eps) * seed)
        w_ref[at, :] = (w_ref[at, :].astype(F32) - (dense * grad) * inverse).astype(BF16)
        pltpu.make_async_copy(w_ref.at[at, :], w_out_hbm.at[at, :], out_sems.at[k]).start()
        return carry

    lax.fori_loop(0, count, update, 0)
    core = lax.axis_index("dp_2")
    half = mine_ref.shape[1]
    for grad, c in ((mine_ref[...], core), (theirs_ref[...], 1 - core)):
        cols = pl.ds(pl.multiple_of(c * half, half), half)
        grad = scale * grad
        dense_out[:, cols] = rows_ref[:, cols] + grad * grad

    def drain(k, carry):
        at = pl.ds(pl.multiple_of(k * size, size), size)
        pltpu.make_async_copy(w_ref.at[at, :], w_out_hbm.at[at, :], out_sems.at[k]).wait()
        return carry

    lax.fori_loop(0, count, drain, 0)


def footprint(shapes):
    return sum(math.prod(s.shape) * 4 for s in shapes)


def call(kernel, outs, flops, args, scratch=(), spare=8, far=(), far_out=(), aliases=None):
    shapes = tuple(jax.ShapeDtypeStruct(s, t) for s, t in outs)
    return pl.pallas_call(
        kernel,
        out_shape=shapes,
        in_specs=[HBM if k in far else VM for k in range(len(args))],
        out_specs=tuple(HBM if k in far_out else VM for k in range(len(shapes))),
        scratch_shapes=list(scratch),
        input_output_aliases=aliases or {},
        compiler_params=pltpu.CompilerParams(vmem_limit_bytes=footprint(scratch) + spare * 2**20),
        cost_estimate=pl.CostEstimate(flops=flops, transcendentals=0, bytes_accessed=2 * 10**6),
    )(*args)


SHIFTS = (1, 3, 2)


def spot(axis, shift):
    return lax.rem(lax.axis_index(axis) + shift, 4)


def sigmoid(x):
    return 0.5 * jnp.tanh(0.5 * x) + 0.5


def forward_kernel(chunks, *refs):
    ins, (w_ref, bias_ref, out_w_ref) = refs[:chunks], refs[chunks : chunks + 3]
    slope_ref, hidden_ref, logit_ref, turned_ref, rows_ref = refs[chunks + 3 :]
    rows = ins[0].shape[0]
    width = w_ref.shape[1]
    for k in range(chunks):
        rows_ref[rows * k : rows * (k + 1), :] = ins[k][...]
        turned_ref[:, rows * k : rows * (k + 1)] = ins[k][...].T

    def columns(n, carry):
        cols = pl.ds(pl.multiple_of(n * 256, 256), 256)
        act = dot_f32(rows_ref[...], w_ref[:, cols]) + bias_ref[:, cols]
        sigma = sigmoid(act)
        hidden_ref[:, cols] = (act * sigma).astype(BF16)
        slope_ref[:, cols] = out_w_ref[:, cols].astype(F32) * sigma * (1.0 + act * (1.0 - sigma))
        return carry

    lax.fori_loop(0, width // 256, columns, 0, unroll=8)
    out_w = jnp.broadcast_to(out_w_ref[...], (16, width))
    for k in range(logit_ref.shape[0]):
        part = dot_f32(out_w, hidden_ref[256 * k : 256 * (k + 1), :], (((1,), (1,)), ((), ())))
        logit_ref[k : k + 1, :] = part[0:1, :]


def forward(chunks, w, bias, out_w):
    rows, depth = chunks[0].shape
    width = w.shape[1]
    n = len(chunks)
    total = n * rows
    outs = [((total, width), F32), ((total, width), BF16), ((total // 256, 256), F32), ((depth, total), BF16)]
    return call(
        functools.partial(forward_kernel, n),
        outs,
        total * 10**7,
        (*chunks, w, bias, out_w),
        [pltpu.VMEM((total, depth), BF16)],
    )


ORDER = (0, 3, 1, 2)
PARTNERS = ((0, 1, 2, 3), (2, 0, 3, 1), (1, 3, 0, 2), (3, 2, 1, 0))


def slope_kernel(*refs):
    slopes, hiddens = refs[0:3], refs[3:6]
    own_ref, prev_ref, next_ref, far_ref, labels_ref, weight_ref = refs[6:12]
    dact_ref, other_ref, sums_mine_ref, sums_other_ref, sums_ref = refs[12:]
    rows, width = slopes[0].shape
    spans = ((0, 0), (1, 0), (1, rows), (2, 0))
    half = width // 2
    core = lax.axis_index("dp_2")
    dlogits = []
    for k in range(4):
        at = spot("mp", ORDER[k])
        logit = (own_ref[k : k + 1, :] + far_ref[PARTNERS[3][k] : PARTNERS[3][k] + 1, :]) + (
            prev_ref[PARTNERS[1][k] : PARTNERS[1][k] + 1, :] + next_ref[PARTNERS[2][k] : PARTNERS[2][k] + 1, :]
        )
        here = pl.ds(pl.multiple_of(at * rows, rows), rows)
        label = labels_ref[:, here].astype(F32)
        dlogits.append(weight_ref[:, here] * (sigmoid(logit) - label))
    rows_form = jnp.concatenate(dlogits + [jnp.zeros((4, rows), F32)], axis=0)
    cols_form = rows_form.T
    pick = iota((16, rows), 0)
    ones = jnp.ones((16, rows), BF16)
    cols, lefts = [], []
    for k in range(4):
        cols.append(cols_form[:, k : k + 1])
        top = dlogits[k].astype(BF16).astype(F32)
        rest = dlogits[k] - top
        lefts.append(jnp.where(pick == 0, top, jnp.where(pick == 1, rest, 0.0)).astype(BF16))
    block = 256
    line = iota((16, block), 0)

    def columns(n, carry):
        span = pl.ds(pl.multiple_of(n * block, block), block)
        bias_sum = out_sum = jnp.zeros((16, block), F32)
        for k in range(4):
            which, start = spans[k]
            part = (slopes[which][start : start + rows, span] * cols[k]).astype(BF16)
            dact_ref[rows * k : rows * (k + 1), span] = part
            bias_sum = bias_sum + dot_f32(ones, part)
            out_sum = out_sum + dot_f32(lefts[k], hiddens[which][start : start + rows, span])
        total = jnp.sum(out_sum, axis=0, keepdims=True)
        sums_ref[:, span] = jnp.where(line == 0, bias_sum, jnp.where(line == 1, total, 0.0))
        return carry

    lax.fori_loop(0, width // block, columns, 0)
    other_ref[...] = dact_ref[:, pl.ds(pl.multiple_of((1 - core) * half, half), half)]
    sums_mine_ref[...] = sums_ref[:, pl.ds(pl.multiple_of(core * half, half), half)]
    sums_other_ref[...] = sums_ref[:, pl.ds(pl.multiple_of((1 - core) * half, half), half)]


def back_kernel(dact_ref, w_ref, own_ref, *outs):
    rows, depth = own_ref.shape
    block = 512

    def columns(n, carry):
        span = pl.ds(pl.multiple_of(n * block, block), block)
        part = dot_f32(dact_ref[...], w_ref[span, :], (((1,), (1,)), ((), ())))
        for k, target in enumerate((own_ref, *outs)):
            target[:, span] = part[rows * k : rows * (k + 1), :].astype(target.dtype)
        return carry

    lax.fori_loop(0, depth // block, columns, 0)


def spot_on(first, core, shift):
    x, y = lax.axis_index("dp_0"), lax.axis_index("dp_1")
    along = x * (1 - core) + y * core if first else y * (1 - core) + x * core
    return lax.rem(along + shift, 4)


def chip_rows(core, outer, inner, size):
    return pl.multiple_of((outer * (4 - 3 * core) + inner * (1 + 3 * core)) * size, size)


def grad_kernel(shifts, *refs):
    turned, (dact_ref, far_dact_ref, sums_ref, far_sums_ref), outs = refs[0:6], refs[6:10], refs[10:]
    size = turned[0].shape[0] // 16
    half = far_dact_ref.shape[1]
    spans = ((0, 256), (256, 512), (768, 256))
    core = lax.axis_index("dp_2")
    local = pl.ds(pl.multiple_of(core * half, half), half)
    for target, shift in zip(outs, shifts):
        at = [pl.ds(chip_rows(core, spot_on(True, core, shift), t, size), size) for t in range(4)]
        part = None
        for i, (s, n) in enumerate(spans):
            near = jnp.concatenate([turned[i][a, :] for a in at], axis=0)
            away = jnp.concatenate([turned[i + 3][a, :] for a in at], axis=0)
            p = dot_f32(near, dact_ref[s : s + n, local]) + dot_f32(away, far_dact_ref[s : s + n, :])
            part = p if part is None else part + p
        target[0:256, :] = part.astype(target.dtype)
        target[256:272, :] = split_rows(sums_ref[...] + far_sums_ref[...]).astype(target.dtype)


def split_rows(sums):
    top = sums.astype(BF16).astype(F32)
    return jnp.concatenate([top[0:8], (sums - top)[0:8]], axis=0)


def joined_rows(rows):
    return jnp.concatenate([rows[0:8] + rows[8:16], jnp.zeros_like(rows[0:8])], axis=0)


def middle_kernel(own_ref, a_ref, b_ref, c_ref, out_ref):
    total = own_ref[...] + a_ref[...].astype(F32) + b_ref[...].astype(F32) + c_ref[...].astype(F32)
    out_ref[0:256, :] = total[0:256].astype(BF16)
    out_ref[256:272, :] = split_rows(joined_rows(total[256:272])).astype(BF16)


def last_kernel(
    own_ref,
    before_ref,
    after_ref,
    far_ref,
    sums_ref,
    ids_ref,
    slot_square_ref,
    narrow_ref,
    mine_ref,
    other_ref,
    out_ref,
    full_ref,
):
    core = lax.axis_index("dp_2")
    at = spot_on(False, core, 0)
    even = lax.rem(at, 2) == 0
    before, after = before_ref[...].astype(F32), after_ref[...].astype(F32)
    partner, other = jnp.where(even, after, before), jnp.where(even, before, after)
    total = (own_ref[...].astype(F32) + partner) + (other + far_ref[...].astype(F32))
    count = narrow_ref.shape[0]
    extra = joined_rows(total[count:])
    full_ref[...] = total[:count]
    narrow_ref[...] = total[:count].astype(BF16)
    size = count // 4
    per = size // 2
    chunk = full_ref[pl.ds(pl.multiple_of(at * size, size), size), :]
    mine_ref[...] = full_ref[pl.ds(pl.multiple_of(at * size + core * per, per), per), :]
    other_ref[...] = full_ref[pl.ds(pl.multiple_of(at * size + (1 - core) * per, per), per), :]
    lead = jnp.where((lax.axis_index("dp_0") == 0) & (lax.axis_index("dp_1") == 0), 1.0, 0.0)
    square = slot_square_ref[0:1, 0:1] + jnp.sum(jnp.sum(chunk * chunk, axis=1, keepdims=True), axis=0, keepdims=True)
    square = square + lead * jnp.sum(jnp.sum(extra * extra, axis=1, keepdims=True), axis=0, keepdims=True)
    owners, capacity = ids_ref.shape
    lines = capacity // 2
    top = square.astype(BF16).astype(F32)
    mid = (square - top).astype(BF16).astype(F32)
    end = square - top - mid
    ids = ids_ref[...]
    lane = iota((owners, 128 - 2 * capacity), 1)
    tail = jnp.where(lane == 0, top, jnp.where(lane == 1, mid, jnp.where(lane == 2, end, 0.0)))
    info = jnp.concatenate([(ids >> 8).astype(F32), (ids & 255).astype(F32), tail], axis=1)
    out_ref[:, :lines, :] = sums_ref[...]
    out_ref[:, lines:, :] = jnp.broadcast_to(info[:, None, :], (owners, 8, 128)).astype(BF16)


def pack_kernel(*refs):
    rows = refs[0].shape[0]
    for k in range(4):
        refs[4][rows * k : rows * (k + 1), :] = refs[k][...]


def merge_kernel(*refs):
    stacks, out_ref = refs[:8], refs[8]
    core = lax.axis_index("dp_2")
    per = stacks[0].shape[0] // 4
    for side, c in ((0, core), (1, 1 - core)):
        for i in range(4):
            for j in range(4):
                at = chip_rows(c, spot_on(True, c, (4 - i) % 4), spot_on(False, c, (4 - j) % 4), 1)
                rows = pl.ds(pl.multiple_of((at * 2 + c) * per, per), per)
                out_ref[rows, :] = stacks[4 * side + i][per * j : per * (j + 1), :]


def grad_merge_kernel(*refs):
    stacks, out_ref = refs[:8], refs[8]
    core = lax.axis_index("dp_2")
    size = stacks[0].shape[0] // 4
    half = stacks[0].shape[1]
    for side, c in ((0, core), (1, 1 - core)):
        cols = pl.ds(pl.multiple_of(c * half, half), half)
        for i in range(4):
            outer = spot_on(True, c, (4 - i) % 4)
            for j in range(4):
                out_ref[pl.ds(chip_rows(c, outer, j, size), size), cols] = stacks[4 * side + i][size * j : size * (j + 1), :]


def cross(x, first, shift):
    moves = []
    for i in range(32):
        a, b, c = i // 8, i // 2 % 4, i % 2
        a, b = ((a + shift) % 4, b) if (c == 0) == first else (a, (b + shift) % 4)
        moves.append((i, a * 8 + b * 2 + c))
    return lax.ppermute(x, DP, moves)


def send(x, axis, shift):
    n = lax.axis_size(axis)
    return lax.ppermute(x, axis, [(i, (i + shift) % n) for i in range(n)])


def around(x, axis):
    return [send(x, axis, s) for s in SHIFTS]


def inner(
    slab_values,
    row_ids,
    peer_counts,
    lookup_slots,
    labels,
    sample_weight,
    weight_in,
    bias_in,
    weight_out,
    dense_accum,
    table_rows,
    table_accum,
):
    batch, features = lookup_slots.shape
    depth, width = weight_in.shape
    half = width // 2
    lookups_t = lookup_slots.T
    low, high = gather_rows(peer_counts, lookups_t, slab_values[0])
    before_low, after_high = send(low, "mp", 1), send(high, "mp", 3)
    before_high, after_low = send(high, "mp", 1), send(low, "mp", 3)
    narrow = dense_accum.astype(BF16)
    parts = {s: cross(narrow, False, s) for s in SHIFTS}
    block = (depth // 8, width)
    near = call(pack_kernel, [(block, BF16)], 10**8, (narrow, parts[1], parts[2], parts[3]))[0]
    stacks = {s: cross(near, True, s) for s in SHIFTS}
    stacks = [near, stacks[1], stacks[2], stacks[3]]
    stacks = stacks + [send(g, "dp_2", 1) for g in stacks]
    accum_full = call(merge_kernel, [((depth, width), BF16)], 10**8, stacks)[0]
    bias = bias_in.reshape(1, width)
    out_w = weight_out.reshape(1, width)
    far_low, far_high = send(before_low, "mp", 1), send(after_high, "mp", 3)
    slope_0, hidden_0, logit_0, turned_0 = forward([low, high], weight_in, bias, out_w)
    slope_1, hidden_1, logit_1, turned_1 = forward(
        [before_low, before_high, after_low, after_high], weight_in, bias, out_w
    )
    slope_2, hidden_2, logit_2, turned_2 = forward([far_low, far_high], weight_in, bias, out_w)
    turned = [turned_0, turned_1, turned_2]
    turned = turned + [send(t, "dp_2", 1) for t in turned]
    logits = jnp.concatenate([logit_0, logit_1, logit_2], axis=0)
    logit_before, logit_after, logit_far = around(logits, "mp")
    dact, other, sums_mine, sums_other = call(
        slope_kernel,
        [((4 * batch, width), BF16), ((4 * batch, half), BF16), ((16, half), F32), ((16, half), F32)],
        2 * 10**9,
        (
            slope_0,
            slope_1,
            slope_2,
            hidden_0,
            hidden_1,
            hidden_2,
            logits,
            logit_before,
            logit_after,
            logit_far,
            labels.reshape(1, -1),
            sample_weight.reshape(1, -1),
        ),
        [pltpu.VMEM((16, width), F32)],
    )
    far_dact = send(other, "dp_2", 1)
    far_sums = send(sums_other, "dp_2", 1)
    own, to_before, to_after, to_far = call(
        back_kernel, [((batch, depth), F32)] + [((batch, depth), BF16)] * 3, 4 * 10**9, (dact, weight_in)
    )
    from_after, from_before, from_far = send(to_before, "mp", 3), send(to_after, "mp", 1), send(to_far, "mp", 2)
    held = (*turned, dact, far_dact, sums_mine, far_sums)
    block = (depth // 4 + 16, half)
    to_far, to_next = call(functools.partial(grad_kernel, (2, 1)), [(block, BF16)] * 2, 4 * 10**9, held)
    distant, from_prev = cross(to_far, True, 2), cross(to_next, True, 1)
    to_prev, keep = call(functools.partial(grad_kernel, (3, 0)), [(block, BF16), (block, F32)], 4 * 10**9, held)
    from_next = cross(to_prev, True, 3)
    keep = call(middle_kernel, [(block, BF16)], 10**8, (keep, from_prev, from_next, distant))[0]
    got = [cross(keep, False, s) for s in SHIFTS]
    peers, capacity = row_ids.shape[1:]
    slot_sums, slot_square = call(
        functools.partial(slot_kernel, capacity),
        [((peers, capacity // 2, 128), BF16), ((8, 128), F32)],
        8 * 10**9,
        (peer_counts, lookups_t, own, from_before, from_after, from_far),
        [pltpu.VMEM((features * batch, 256), BF16), pltpu.VMEM((1, features * batch), F32)],
        24,
    )
    narrow, mine, others, outgoing = call(
        last_kernel,
        [((depth // 4, half), BF16)] + [((depth // 32, half), F32)] * 2 + [((peers, capacity // 2 + 8, 128), BF16)],
        10**8,
        (keep, *got, slot_sums, row_ids[0], slot_square),
        [pltpu.VMEM((depth // 4, half), F32)],
    )
    theirs = send(others, "dp_2", 1)
    stacks = {s: cross(narrow, True, s) for s in SHIFTS}
    stacks = [narrow, stacks[1], stacks[2], stacks[3]]
    stacks = stacks + [send(g, "dp_2", 1) for g in stacks]
    arrived = lax.all_to_all(outgoing, DP_MP, 0, 0, tiled=True)
    grad_full = call(grad_merge_kernel, [((depth, width), BF16)], 10**8, stacks)[0]
    size = depth // 64
    table_t, accum_t, weight_new, accum_new = call(
        functools.partial(final_kernel, (table_rate, dense_rate, adagrad_eps, clip_norm)),
        [
            (table_rows.shape[::-1], F32),
            ((1, table_rows.shape[0]), F32),
            ((depth, width), BF16),
            (dense_accum.shape, F32),
        ],
        8 * 10**9,
        (
            arrived,
            dense_accum,
            mine,
            theirs,
            table_rows.T,
            table_accum.reshape(1, -1),
            weight_in,
            accum_full,
            grad_full,
        ),
        [
            pltpu.VMEM((table_rows.shape[0] // 4, 256), F32),
            pltpu.VMEM(table_rows.shape[::-1], F32),
            pltpu.VMEM((1, table_rows.shape[0]), F32),
            pltpu.VMEM((depth, width), BF16),
            pltpu.VMEM((depth, width), BF16),
            pltpu.VMEM((depth, width), BF16),
            pltpu.SemaphoreType.DMA((2,)),
            pltpu.SemaphoreType.DMA((3, size)),
            pltpu.SemaphoreType.DMA((size,)),
        ],
        33,
        (4, 5, 6, 7, 8),
        (2,),
    )
    return (weight_new, accum_new, table_t.T, accum_t.reshape(-1))


def solution(mesh):
    torus = Mesh(mesh.devices.reshape(4, 4, 2, mesh.shape["mp"]), ("dp_0", "dp_1", "dp_2", "mp"))
    placed = (
        P(DP_MP, None, None),
        P(DP_MP, None, None),
        P(DP_MP, None),
        P(DP_MP, None),
        P(DP),
        P(DP),
        P(None, "mp"),
        P("mp"),
        P("mp"),
        P(DP, "mp"),
        P(DP_MP, None),
        P(DP_MP),
    )
    return jax.shard_map(
        inner,
        mesh=torus,
        in_specs=placed,
        out_specs=(P(None, "mp"), P(DP, "mp"), P(DP_MP, None), P(DP_MP)),
        check_vma=False,
    )
```

```python
import functools
import math

import jax
import jax.numpy as jnp
from jax import lax
from jax.experimental import pallas as pl
from jax.experimental.pallas import tpu as pltpu
from jax.sharding import Mesh
from jax.sharding import PartitionSpec as P


DP = ("dp_0", "dp_1", "dp_2")
DP_MP = ("dp_0", "dp_1", "dp_2", "mp")

clip_norm = 1.0
dense_rate = 0.02
table_rate = 0.5
adagrad_eps = 1e-10

F32 = jnp.float32
BF16 = jnp.bfloat16
VM = pl.BlockSpec(memory_space=pltpu.VMEM)
HBM = pl.BlockSpec(memory_space=pltpu.MemorySpace.HBM)


def iota(shape, dim):
    return lax.broadcasted_iota(jnp.int32, shape, dim)


def dot_f32(a, b, dims=(((1,), (0,)), ((), ()))):
    return lax.dot_general(a, b, dims, preferred_element_type=F32)


def spans_of(counts_ref):
    owners = counts_ref.shape[1]
    spread = jnp.broadcast_to(counts_ref[...].astype(F32), (owners, owners))
    at, of = iota((owners, owners), 0), iota((owners, owners), 1)
    ends = jnp.sum(jnp.where(of <= at, spread, 0.0), axis=1, keepdims=True)
    return ends - jnp.sum(jnp.where(of == at, spread, 0.0), axis=1, keepdims=True), ends


def gather_kernel(counts_hbm, lookups_hbm, slab_hbm, low_ref, high_ref, counts_ref, lookups_ref, slab_ref, sems):
    copies = [
        pltpu.make_async_copy(a, b, sems.at[k])
        for k, (a, b) in enumerate(
            ((counts_hbm, counts_ref), (lookups_hbm, lookups_ref), (slab_hbm, slab_ref))
        )
    ]
    for copy in copies:
        copy.start()
    features, batch = lookups_ref.shape
    copies[0].wait()
    copies[1].wait()
    halfway = slab_ref.shape[1] // 2
    starts, ends = spans_of(counts_ref)
    copies[2].wait()
    halves = jnp.concatenate([slab_ref[:, :halfway], slab_ref[:, halfway:]], axis=0)
    low_lane = iota((batch, 128), 1) < 64

    def pair(p, carry):
        hots, inners = [], []
        for parity in range(2):
            q = lookups_ref[pl.ds(2 * p + parity, 1), :].astype(F32)
            match = (q >= starts) & (q < ends)
            slot = q - jnp.sum(jnp.where(match, starts, 0.0), axis=0, keepdims=True)
            upper = slot >= 16.0
            hot = jnp.where(match, 1.0, 0.0)
            hots.append(
                jnp.concatenate([jnp.where(upper, 0.0, hot), jnp.where(upper, hot, 0.0)], axis=0).astype(BF16)
            )
            inners.append(jnp.where(upper, slot - 16.0, slot))
        inner = jnp.concatenate([*inners, jnp.zeros((6, batch), F32)], axis=0).T
        both = []
        for parity in range(2):
            rows = dot_f32(hots[parity], halves, (((0,), (0,)), ((), ())))
            place = jnp.broadcast_to(inner[:, parity : parity + 1], (batch, 128))
            block = jnp.floor(place * 0.5)
            found = rows[:, :128]
            for k in range(1, 8):
                found = jnp.where(block == float(k), rows[:, 128 * k : 128 * (k + 1)], found)
            swap = place - 2.0 * block != float(parity)
            both.append(jnp.where(swap, pltpu.roll(found, 64, 1), found))
        pooled = jnp.where(low_lane, both[0], both[1]).astype(BF16)
        cols = pl.ds(pl.multiple_of(p * 128, 128), 128)
        low_ref[:, cols] = pooled[: batch // 2]
        high_ref[:, cols] = pooled[batch // 2 :]
        return carry

    lax.fori_loop(0, features // 2, pair, 0, unroll=4)


def gather_rows(counts, lookups_t, slab):
    features, batch = lookups_t.shape
    return pl.pallas_call(
        gather_kernel,
        out_shape=(jax.ShapeDtypeStruct((batch // 2, features * 64), BF16),) * 2,
        in_specs=[HBM, HBM, HBM],
        out_specs=(VM, VM),
        scratch_shapes=[
            pltpu.VMEM(counts.shape, counts.dtype),
            pltpu.VMEM(lookups_t.shape, lookups_t.dtype),
            pltpu.VMEM(slab.shape, slab.dtype),
            pltpu.SemaphoreType.DMA((3,)),
        ],
        name="gather_rows",
        compiler_params=pltpu.CompilerParams(vmem_limit_bytes=16 * 2**20),
        cost_estimate=pl.CostEstimate(flops=6 * 10**9, transcendentals=0, bytes_accessed=2 * 10**6),
    )(counts, lookups_t, slab)


def slot_kernel(
    capacity, counts_ref, lookups_ref, own_ref, a_ref, b_ref, c_ref, out_ref, square_ref, value_ref, at_ref
):
    owners = counts_ref.shape[1]
    features, batch = lookups_ref.shape
    spread = jnp.broadcast_to(counts_ref[...].astype(F32), (owners, owners))
    at, of = iota((owners, owners), 0), iota((owners, owners), 1)
    ends = jnp.sum(jnp.where(of <= at, spread, 0.0), axis=1, keepdims=True)
    starts = ends - jnp.sum(jnp.where(of == at, spread, 0.0), axis=1, keepdims=True)
    moves = iota((owners, 1), 0).astype(F32) * float(capacity) - starts
    indices = []
    for f in range(features):
        q = lookups_ref[f : f + 1, :].astype(F32)
        match = (q >= starts) & (q < ends)
        indices.append(q + jnp.sum(jnp.where(match, moves, 0.0), axis=0, keepdims=True))
        at_ref[0:1, batch * f : batch * (f + 1)] = jnp.floor(indices[f] * 0.5)
    index = jnp.concatenate(indices, axis=0)
    odd = (index - 2.0 * jnp.floor(index * 0.5)).T
    low_lane = iota((batch, 128), 1) < 64
    lane_odd = jnp.where(low_lane, 0.0, 1.0)
    for pair in range(features // 2):
        cols = slice(128 * pair, 128 * (pair + 1))
        total = own_ref[:, cols]
        for piece_ref in (a_ref, b_ref, c_ref):
            total = total + piece_ref[:, cols].astype(F32)
        turned = pltpu.roll(total, 64, 1)
        for parity in range(2):
            f = 2 * pair + parity
            rows = jnp.where(low_lane, total, turned) if parity == 0 else jnp.where(low_lane, turned, total)
            rows = jnp.where(jnp.broadcast_to(odd[:, f : f + 1], (batch, 128)) == lane_odd, rows, 0.0)
            high = rows.astype(BF16)
            value_ref[batch * f : batch * (f + 1), 0:128] = high
            value_ref[batch * f : batch * (f + 1), 128:256] = (rows - high.astype(F32)).astype(BF16)
    block = 512
    each = block * 2 // capacity
    where = jnp.broadcast_to(at_ref[...], (block, features * batch))
    lines = iota((block, features * batch), 0).astype(F32)

    def part(m, square):
        hot = jnp.where(lines == where - (m * block).astype(F32), 1.0, 0.0).astype(BF16)
        both = dot_f32(hot, value_ref[...])
        sums = both[:, 0:128] + both[:, 128:256]
        first = pl.multiple_of(m * each, each)
        out_ref[pl.ds(first, each), :, :] = sums.astype(BF16).reshape(each, capacity // 2, 128)
        return square + jnp.sum(jnp.sum(sums * sums, axis=1, keepdims=True), axis=0, keepdims=True)

    square = lax.fori_loop(0, owners // each, part, jnp.zeros((1, 1), F32))
    square_ref[...] = jnp.broadcast_to(square, square_ref.shape)


def final_kernel(
    rates,
    arrived_ref,
    rows_ref,
    mine_ref,
    theirs_ref,
    table_hbm,
    accum_hbm,
    w_hbm,
    held_hbm,
    grad_hbm,
    table_out,
    accum_out,
    w_out_hbm,
    dense_out,
    acc_ref,
    table_ref,
    accum_ref,
    w_ref,
    held_ref,
    grad_ref,
    sems,
    in_sems,
    out_sems,
):
    rate, dense, eps, clip = rates
    size = 64
    count = w_ref.shape[0] // size
    copies = [
        pltpu.make_async_copy(a, b, sems.at[k])
        for k, (a, b) in enumerate(((table_hbm, table_ref), (accum_hbm, accum_ref)))
    ]
    for copy in copies:
        copy.start()
    sides = ((w_hbm, w_ref), (held_hbm, held_ref), (grad_hbm, grad_ref))

    def fetch(k):
        at = pl.ds(pl.multiple_of(k * size, size), size)
        return [pltpu.make_async_copy(a.at[at, :], b.at[at, :], in_sems.at[m, k]) for m, (a, b) in enumerate(sides)]

    def begin(k, carry):
        for copy in fetch(k):
            copy.start()
        return carry

    lax.fori_loop(0, count, begin, 0)
    sources, lines, _ = arrived_ref.shape
    half = lines - 8
    capacity = 2 * half
    rows = table_ref.shape[1]
    blocks = rows // 256
    every = sources * half
    info = jnp.sum(arrived_ref[:, half:, :].astype(F32), axis=1) * 0.125
    squares = jnp.sum(info[:, 2 * capacity : 2 * capacity + 3], axis=0, keepdims=True)
    total = jnp.sum(squares, axis=1, keepdims=True)
    scale = clip / jnp.maximum(jnp.sqrt(total), clip)
    share = jnp.where(iota((sources, every), 0) == iota((sources, every), 1) // half, 1.0, 0.0)
    spread_info = dot_f32(info.astype(BF16), share.astype(BF16), (((0,), (0,)), ((), ())))
    slot = iota((capacity, every), 0)
    line = iota((capacity, every), 1) & (half - 1)
    inside_at = iota((256, every), 0).astype(F32)
    turned = arrived_ref[:, :half, :].reshape(every, 128).astype(F32).T
    acc = None
    for parity in range(2):
        mine = slot == 2 * line + parity
        block = jnp.sum(jnp.where(mine, spread_info[0:capacity], 0.0), axis=0, keepdims=True)
        inside = jnp.sum(jnp.where(mine, spread_info[capacity : 2 * capacity], 0.0), axis=0, keepdims=True)
        piece = turned[64 * parity : 64 * (parity + 1), :]
        hot = jnp.where(inside_at == inside, 1.0, 0.0).astype(BF16)
        spread = jnp.concatenate([jnp.where(block == float(k), piece, 0.0).astype(BF16) for k in range(blocks)], axis=0)
        part = dot_f32(spread, hot, (((1,), (1,)), ((), ())))
        acc = part if acc is None else acc + part
    acc_ref[...] = acc
    for copy in copies:
        copy.wait()

    def finish(k, carry):
        received = scale * acc_ref[pl.ds(pl.multiple_of(64 * k, 64), 64), :]
        cols = pl.ds(pl.multiple_of(256 * k, 256), 256)
        accum = accum_ref[:, cols] + jnp.sum(received * received, axis=0, keepdims=True) * (1.0 / 64.0)
        accum_out[:, cols] = accum
        table_out[:, cols] = table_ref[:, cols] - rate * received / (accum * lax.rsqrt(accum) + eps)
        return carry

    lax.fori_loop(0, blocks, finish, 0, unroll=2)

    def update(k, carry):
        for copy in fetch(k):
            copy.wait()
        at = pl.ds(pl.multiple_of(k * size, size), size)
        grad = scale * grad_ref[at, :].astype(F32)
        accum = held_ref[at, :].astype(F32) + grad * grad
        seed = lax.rsqrt(accum)
        inverse = seed * (2.0 - (accum * seed + eps) * seed)
        w_ref[at, :] = (w_ref[at, :].astype(F32) - (dense * grad) * inverse).astype(BF16)
        pltpu.make_async_copy(w_ref.at[at, :], w_out_hbm.at[at, :], out_sems.at[k]).start()
        return carry

    lax.fori_loop(0, count, update, 0)
    core = lax.axis_index("dp_2")
    half = mine_ref.shape[1]
    for grad, c in ((mine_ref[...], core), (theirs_ref[...], 1 - core)):
        cols = pl.ds(pl.multiple_of(c * half, half), half)
        grad = scale * grad
        dense_out[:, cols] = rows_ref[:, cols] + grad * grad

    def drain(k, carry):
        at = pl.ds(pl.multiple_of(k * size, size), size)
        pltpu.make_async_copy(w_ref.at[at, :], w_out_hbm.at[at, :], out_sems.at[k]).wait()
        return carry

    lax.fori_loop(0, count, drain, 0)


def footprint(shapes):
    return sum(math.prod(s.shape) * 4 for s in shapes)


def call(kernel, outs, flops, args, scratch=(), spare=8, far=(), far_out=(), aliases=None):
    shapes = tuple(jax.ShapeDtypeStruct(s, t) for s, t in outs)
    return pl.pallas_call(
        kernel,
        out_shape=shapes,
        in_specs=[HBM if k in far else VM for k in range(len(args))],
        out_specs=tuple(HBM if k in far_out else VM for k in range(len(shapes))),
        scratch_shapes=list(scratch),
        input_output_aliases=aliases or {},
        compiler_params=pltpu.CompilerParams(vmem_limit_bytes=footprint(scratch) + spare * 2**20),
        cost_estimate=pl.CostEstimate(flops=flops, transcendentals=0, bytes_accessed=2 * 10**6),
    )(*args)


SHIFTS = (1, 3, 2)


def spot(axis, shift):
    return lax.rem(lax.axis_index(axis) + shift, 4)


def sigmoid(x):
    return 0.5 * jnp.tanh(0.5 * x) + 0.5


def forward_kernel(chunks, *refs):
    ins, (w_ref, bias_ref, out_w_ref) = refs[:chunks], refs[chunks : chunks + 3]
    slope_ref, hidden_ref, logit_ref, turned_ref, rows_ref = refs[chunks + 3 :]
    rows = ins[0].shape[0]
    width = w_ref.shape[1]
    for k in range(chunks):
        rows_ref[rows * k : rows * (k + 1), :] = ins[k][...]
        turned_ref[:, rows * k : rows * (k + 1)] = ins[k][...].T

    def columns(n, carry):
        cols = pl.ds(pl.multiple_of(n * 256, 256), 256)
        act = dot_f32(rows_ref[...], w_ref[:, cols]) + bias_ref[:, cols]
        sigma = sigmoid(act)
        hidden_ref[:, cols] = (act * sigma).astype(BF16)
        slope_ref[:, cols] = out_w_ref[:, cols].astype(F32) * sigma * (1.0 + act * (1.0 - sigma))
        return carry

    lax.fori_loop(0, width // 256, columns, 0, unroll=8)
    out_w = jnp.broadcast_to(out_w_ref[...], (16, width))
    for k in range(logit_ref.shape[0]):
        part = dot_f32(out_w, hidden_ref[256 * k : 256 * (k + 1), :], (((1,), (1,)), ((), ())))
        logit_ref[k : k + 1, :] = part[0:1, :]


def forward(chunks, w, bias, out_w):
    rows, depth = chunks[0].shape
    width = w.shape[1]
    n = len(chunks)
    total = n * rows
    outs = [((total, width), F32), ((total, width), BF16), ((total // 256, 256), F32), ((depth, total), BF16)]
    return call(
        functools.partial(forward_kernel, n),
        outs,
        total * 10**7,
        (*chunks, w, bias, out_w),
        [pltpu.VMEM((total, depth), BF16)],
    )


ORDER = (0, 3, 1, 2)
PARTNERS = ((0, 1, 2, 3), (2, 0, 3, 1), (1, 3, 0, 2), (3, 2, 1, 0))


def slope_kernel(*refs):
    slopes, hiddens = refs[0:3], refs[3:6]
    own_ref, prev_ref, next_ref, far_ref, labels_ref, weight_ref = refs[6:12]
    dact_ref, other_ref, sums_mine_ref, sums_other_ref, sums_ref = refs[12:]
    rows, width = slopes[0].shape
    spans = ((0, 0), (1, 0), (1, rows), (2, 0))
    half = width // 2
    core = lax.axis_index("dp_2")
    dlogits = []
    for k in range(4):
        at = spot("mp", ORDER[k])
        logit = (own_ref[k : k + 1, :] + far_ref[PARTNERS[3][k] : PARTNERS[3][k] + 1, :]) + (
            prev_ref[PARTNERS[1][k] : PARTNERS[1][k] + 1, :] + next_ref[PARTNERS[2][k] : PARTNERS[2][k] + 1, :]
        )
        here = pl.ds(pl.multiple_of(at * rows, rows), rows)
        label = labels_ref[:, here].astype(F32)
        dlogits.append(weight_ref[:, here] * (sigmoid(logit) - label))
    rows_form = jnp.concatenate(dlogits + [jnp.zeros((4, rows), F32)], axis=0)
    cols_form = rows_form.T
    pick = iota((16, rows), 0)
    ones = jnp.ones((16, rows), BF16)
    cols, lefts = [], []
    for k in range(4):
        cols.append(cols_form[:, k : k + 1])
        top = dlogits[k].astype(BF16).astype(F32)
        rest = dlogits[k] - top
        lefts.append(jnp.where(pick == 0, top, jnp.where(pick == 1, rest, 0.0)).astype(BF16))
    block = 256
    line = iota((16, block), 0)

    def columns(n, carry):
        span = pl.ds(pl.multiple_of(n * block, block), block)
        bias_sum = out_sum = jnp.zeros((16, block), F32)
        for k in range(4):
            which, start = spans[k]
            part = (slopes[which][start : start + rows, span] * cols[k]).astype(BF16)
            dact_ref[rows * k : rows * (k + 1), span] = part
            bias_sum = bias_sum + dot_f32(ones, part)
            out_sum = out_sum + dot_f32(lefts[k], hiddens[which][start : start + rows, span])
        total = jnp.sum(out_sum, axis=0, keepdims=True)
        sums_ref[:, span] = jnp.where(line == 0, bias_sum, jnp.where(line == 1, total, 0.0))
        return carry

    lax.fori_loop(0, width // block, columns, 0)
    other_ref[...] = dact_ref[:, pl.ds(pl.multiple_of((1 - core) * half, half), half)]
    sums_mine_ref[...] = sums_ref[:, pl.ds(pl.multiple_of(core * half, half), half)]
    sums_other_ref[...] = sums_ref[:, pl.ds(pl.multiple_of((1 - core) * half, half), half)]


def back_kernel(dact_ref, w_ref, own_ref, *outs):
    rows, depth = own_ref.shape
    block = 512

    def columns(n, carry):
        span = pl.ds(pl.multiple_of(n * block, block), block)
        part = dot_f32(dact_ref[...], w_ref[span, :], (((1,), (1,)), ((), ())))
        for k, target in enumerate((own_ref, *outs)):
            target[:, span] = part[rows * k : rows * (k + 1), :].astype(target.dtype)
        return carry

    lax.fori_loop(0, depth // block, columns, 0)


def spot_on(first, core, shift):
    x, y = lax.axis_index("dp_0"), lax.axis_index("dp_1")
    along = x * (1 - core) + y * core if first else y * (1 - core) + x * core
    return lax.rem(along + shift, 4)


def chip_rows(core, outer, inner, size):
    return pl.multiple_of((outer * (4 - 3 * core) + inner * (1 + 3 * core)) * size, size)


def grad_kernel(shifts, *refs):
    turned, (dact_ref, far_dact_ref, sums_ref, far_sums_ref), outs = refs[0:6], refs[6:10], refs[10:]
    size = turned[0].shape[0] // 16
    half = far_dact_ref.shape[1]
    spans = ((0, 256), (256, 512), (768, 256))
    core = lax.axis_index("dp_2")
    local = pl.ds(pl.multiple_of(core * half, half), half)
    for target, shift in zip(outs, shifts):
        at = [pl.ds(chip_rows(core, spot_on(True, core, shift), t, size), size) for t in range(4)]
        part = None
        for i, (s, n) in enumerate(spans):
            near = jnp.concatenate([turned[i][a, :] for a in at], axis=0)
            away = jnp.concatenate([turned[i + 3][a, :] for a in at], axis=0)
            p = dot_f32(near, dact_ref[s : s + n, local]) + dot_f32(away, far_dact_ref[s : s + n, :])
            part = p if part is None else part + p
        target[0:256, :] = part.astype(target.dtype)
        target[256:272, :] = split_rows(sums_ref[...] + far_sums_ref[...]).astype(target.dtype)


def split_rows(sums):
    top = sums.astype(BF16).astype(F32)
    return jnp.concatenate([top[0:8], (sums - top)[0:8]], axis=0)


def joined_rows(rows):
    return jnp.concatenate([rows[0:8] + rows[8:16], jnp.zeros_like(rows[0:8])], axis=0)


def middle_kernel(own_ref, a_ref, b_ref, c_ref, out_ref):
    total = own_ref[...] + a_ref[...].astype(F32) + b_ref[...].astype(F32) + c_ref[...].astype(F32)
    out_ref[0:256, :] = total[0:256].astype(BF16)
    out_ref[256:272, :] = split_rows(joined_rows(total[256:272])).astype(BF16)


def last_kernel(
    own_ref,
    before_ref,
    after_ref,
    far_ref,
    sums_ref,
    ids_ref,
    slot_square_ref,
    narrow_ref,
    mine_ref,
    other_ref,
    out_ref,
    full_ref,
):
    core = lax.axis_index("dp_2")
    at = spot_on(False, core, 0)
    even = lax.rem(at, 2) == 0
    before, after = before_ref[...].astype(F32), after_ref[...].astype(F32)
    partner, other = jnp.where(even, after, before), jnp.where(even, before, after)
    total = (own_ref[...].astype(F32) + partner) + (other + far_ref[...].astype(F32))
    count = narrow_ref.shape[0]
    extra = joined_rows(total[count:])
    full_ref[...] = total[:count]
    narrow_ref[...] = total[:count].astype(BF16)
    size = count // 4
    per = size // 2
    chunk = full_ref[pl.ds(pl.multiple_of(at * size, size), size), :]
    mine_ref[...] = full_ref[pl.ds(pl.multiple_of(at * size + core * per, per), per), :]
    other_ref[...] = full_ref[pl.ds(pl.multiple_of(at * size + (1 - core) * per, per), per), :]
    lead = jnp.where((lax.axis_index("dp_0") == 0) & (lax.axis_index("dp_1") == 0), 1.0, 0.0)
    square = slot_square_ref[0:1, 0:1] + jnp.sum(jnp.sum(chunk * chunk, axis=1, keepdims=True), axis=0, keepdims=True)
    square = square + lead * jnp.sum(jnp.sum(extra * extra, axis=1, keepdims=True), axis=0, keepdims=True)
    owners, capacity = ids_ref.shape
    lines = capacity // 2
    top = square.astype(BF16).astype(F32)
    mid = (square - top).astype(BF16).astype(F32)
    end = square - top - mid
    ids = ids_ref[...]
    lane = iota((owners, 128 - 2 * capacity), 1)
    tail = jnp.where(lane == 0, top, jnp.where(lane == 1, mid, jnp.where(lane == 2, end, 0.0)))
    info = jnp.concatenate([(ids >> 8).astype(F32), (ids & 255).astype(F32), tail], axis=1)
    out_ref[:, :lines, :] = sums_ref[...]
    out_ref[:, lines:, :] = jnp.broadcast_to(info[:, None, :], (owners, 8, 128)).astype(BF16)


def pack_kernel(*refs):
    rows = refs[0].shape[0]
    for k in range(4):
        refs[4][rows * k : rows * (k + 1), :] = refs[k][...]


def merge_kernel(*refs):
    stacks, out_ref = refs[:8], refs[8]
    core = lax.axis_index("dp_2")
    per = stacks[0].shape[0] // 4
    for side, c in ((0, core), (1, 1 - core)):
        for i in range(4):
            for j in range(4):
                at = chip_rows(c, spot_on(True, c, (4 - i) % 4), spot_on(False, c, (4 - j) % 4), 1)
                rows = pl.ds(pl.multiple_of((at * 2 + c) * per, per), per)
                out_ref[rows, :] = stacks[4 * side + i][per * j : per * (j + 1), :]


def grad_merge_kernel(*refs):
    stacks, out_ref = refs[:8], refs[8]
    core = lax.axis_index("dp_2")
    size = stacks[0].shape[0] // 4
    half = stacks[0].shape[1]
    for side, c in ((0, core), (1, 1 - core)):
        cols = pl.ds(pl.multiple_of(c * half, half), half)
        for i in range(4):
            outer = spot_on(True, c, (4 - i) % 4)
            for j in range(4):
                out_ref[pl.ds(chip_rows(c, outer, j, size), size), cols] = stacks[4 * side + i][size * j : size * (j + 1), :]


def cross(x, first, shift):
    moves = []
    for i in range(32):
        a, b, c = i // 8, i // 2 % 4, i % 2
        a, b = ((a + shift) % 4, b) if (c == 0) == first else (a, (b + shift) % 4)
        moves.append((i, a * 8 + b * 2 + c))
    return lax.ppermute(x, DP, moves)


def send(x, axis, shift):
    n = lax.axis_size(axis)
    return lax.ppermute(x, axis, [(i, (i + shift) % n) for i in range(n)])


def around(x, axis):
    return [send(x, axis, s) for s in SHIFTS]


def inner(
    slab_values,
    row_ids,
    peer_counts,
    lookup_slots,
    labels,
    sample_weight,
    weight_in,
    bias_in,
    weight_out,
    dense_accum,
    table_rows,
    table_accum,
):
    batch, features = lookup_slots.shape
    depth, width = weight_in.shape
    half = width // 2
    lookups_t = lookup_slots.T
    low, high = gather_rows(peer_counts, lookups_t, slab_values[0])
    before_low, after_high = send(low, "mp", 1), send(high, "mp", 3)
    before_high, after_low = send(high, "mp", 1), send(low, "mp", 3)
    narrow = dense_accum.astype(BF16)
    parts = {s: cross(narrow, False, s) for s in SHIFTS}
    block = (depth // 8, width)
    near = call(pack_kernel, [(block, BF16)], 10**8, (narrow, parts[1], parts[2], parts[3]))[0]
    stacks = {s: cross(near, True, s) for s in SHIFTS}
    stacks = [near, stacks[1], stacks[2], stacks[3]]
    stacks = stacks + [send(g, "dp_2", 1) for g in stacks]
    accum_full = call(merge_kernel, [((depth, width), BF16)], 10**8, stacks)[0]
    bias = bias_in.reshape(1, width)
    out_w = weight_out.reshape(1, width)
    far_low, far_high = send(before_low, "mp", 1), send(after_high, "mp", 3)
    slope_0, hidden_0, logit_0, turned_0 = forward([low, high], weight_in, bias, out_w)
    slope_1, hidden_1, logit_1, turned_1 = forward(
        [before_low, before_high, after_low, after_high], weight_in, bias, out_w
    )
    slope_2, hidden_2, logit_2, turned_2 = forward([far_low, far_high], weight_in, bias, out_w)
    turned = [turned_0, turned_1, turned_2]
    turned = turned + [send(t, "dp_2", 1) for t in turned]
    logits = jnp.concatenate([logit_0, logit_1, logit_2], axis=0)
    logit_before, logit_after, logit_far = around(logits, "mp")
    dact, other, sums_mine, sums_other = call(
        slope_kernel,
        [((4 * batch, width), BF16), ((4 * batch, half), BF16), ((16, half), F32), ((16, half), F32)],
        2 * 10**9,
        (
            slope_0,
            slope_1,
            slope_2,
            hidden_0,
            hidden_1,
            hidden_2,
            logits,
            logit_before,
            logit_after,
            logit_far,
            labels.reshape(1, -1),
            sample_weight.reshape(1, -1),
        ),
        [pltpu.VMEM((16, width), F32)],
    )
    far_dact = send(other, "dp_2", 1)
    far_sums = send(sums_other, "dp_2", 1)
    own, to_before, to_after, to_far = call(
        back_kernel, [((batch, depth), F32)] + [((batch, depth), BF16)] * 3, 4 * 10**9, (dact, weight_in)
    )
    from_after, from_before, from_far = send(to_before, "mp", 3), send(to_after, "mp", 1), send(to_far, "mp", 2)
    held = (*turned, dact, far_dact, sums_mine, far_sums)
    block = (depth // 4 + 16, half)
    to_far, to_next = call(functools.partial(grad_kernel, (2, 1)), [(block, BF16)] * 2, 4 * 10**9, held)
    distant, from_prev = cross(to_far, True, 2), cross(to_next, True, 1)
    to_prev, keep = call(functools.partial(grad_kernel, (3, 0)), [(block, BF16), (block, F32)], 4 * 10**9, held)
    from_next = cross(to_prev, True, 3)
    keep = call(middle_kernel, [(block, BF16)], 10**8, (keep, from_prev, from_next, distant))[0]
    got = [cross(keep, False, s) for s in SHIFTS]
    peers, capacity = row_ids.shape[1:]
    slot_sums, slot_square = call(
        functools.partial(slot_kernel, capacity),
        [((peers, capacity // 2, 128), BF16), ((8, 128), F32)],
        8 * 10**9,
        (peer_counts, lookups_t, own, from_before, from_after, from_far),
        [pltpu.VMEM((features * batch, 256), BF16), pltpu.VMEM((1, features * batch), F32)],
        24,
    )
    narrow, mine, others, outgoing = call(
        last_kernel,
        [((depth // 4, half), BF16)] + [((depth // 32, half), F32)] * 2 + [((peers, capacity // 2 + 8, 128), BF16)],
        10**8,
        (keep, *got, slot_sums, row_ids[0], slot_square),
        [pltpu.VMEM((depth // 4, half), F32)],
    )
    theirs = send(others, "dp_2", 1)
    stacks = {s: cross(narrow, True, s) for s in SHIFTS}
    stacks = [narrow, stacks[1], stacks[2], stacks[3]]
    stacks = stacks + [send(g, "dp_2", 1) for g in stacks]
    arrived = lax.all_to_all(outgoing, DP_MP, 0, 0, tiled=True)
    grad_full = call(grad_merge_kernel, [((depth, width), BF16)], 10**8, stacks)[0]
    size = depth // 64
    table_t, accum_t, weight_new, accum_new = call(
        functools.partial(final_kernel, (table_rate, dense_rate, adagrad_eps, clip_norm)),
        [
            (table_rows.shape[::-1], F32),
            ((1, table_rows.shape[0]), F32),
            ((depth, width), BF16),
            (dense_accum.shape, F32),
        ],
        8 * 10**9,
        (
            arrived,
            dense_accum,
            mine,
            theirs,
            table_rows.T,
            table_accum.reshape(1, -1),
            weight_in,
            accum_full,
            grad_full,
        ),
        [
            pltpu.VMEM((table_rows.shape[0] // 4, 256), F32),
            pltpu.VMEM(table_rows.shape[::-1], F32),
            pltpu.VMEM((1, table_rows.shape[0]), F32),
            pltpu.VMEM((depth, width), BF16),
            pltpu.VMEM((depth, width), BF16),
            pltpu.VMEM((depth, width), BF16),
            pltpu.SemaphoreType.DMA((2,)),
            pltpu.SemaphoreType.DMA((3, size)),
            pltpu.SemaphoreType.DMA((size,)),
        ],
        33,
        (4, 5, 6, 7, 8),
        (2,),
    )
    return (weight_new, accum_new, table_t.T, accum_t.reshape(-1))


def solution(mesh):
    torus = Mesh(mesh.devices.reshape(4, 4, 2, mesh.shape["mp"]), ("dp_0", "dp_1", "dp_2", "mp"))
    placed = (
        P(DP_MP, None, None),
        P(DP_MP, None, None),
        P(DP_MP, None),
        P(DP_MP, None),
        P(DP),
        P(DP),
        P(None, "mp"),
        P("mp"),
        P("mp"),
        P(DP, "mp"),
        P(DP_MP, None),
        P(DP_MP),
    )
    return jax.shard_map(
        inner,
        mesh=torus,
        in_specs=placed,
        out_specs=(P(None, "mp"), P(DP, "mp"), P(DP_MP, None), P(DP_MP)),
        check_vma=False,
    )
```
